32 devices in a mesh: dp: 8 (over z, y), dap: 4 (over x, core).
Axes of the slice: x: 2, y: 2, z: 4, core: 2. Of those that a mesh axis runs over, the one named last changes fastest.
Arguments:
- z_pair: bfloat16 [8, 256, 256, 64], P('dp', 'dap')
- pair_mask: int32 [8, 256, 256], P('dp', 'dap')
- dz_out: bfloat16 [8, 256, 256, 64], P('dp', 'dap')
- ln_in: bfloat16 [2, 2, 64], replicated
- w_proj: bfloat16 [2, 64, 320], replicated
- b_proj: bfloat16 [2, 320], replicated
- ln_mid: bfloat16 [2, 2, 64], replicated
- w_out: bfloat16 [2, 64, 64], replicated
- b_out: bfloat16 [2, 64], replicated
Outputs:
- output 1: bfloat16 [8, 256, 256, 64], P('dp', 'dap')
- output 2: bfloat16 [8, 256, 256, 64], P('dp', 'dap')
- output 3: float32 [2, 2, 64], replicated
- output 4: float32 [2, 64, 320], replicated
- output 5: float32 [2, 320], replicated
- output 6: float32 [2, 2, 64], replicated
- output 7: float32 [2, 64, 64], replicated
- output 8: float32 [2, 64], replicated
All inputs are finite; a program needn't handle non-finite values.
Results may differ from the reference program's by a relative error of at most 0.0115083.
Values are sent between devices in bfloat16 or wider.
A program may use at most 1 GiB of HBM per device.

```python
import jax
import jax.numpy as jnp
from jax import lax

PROTEINS = 8
N_RES = 256
C_Z = 64
C_HID = 64
LN_EPS = 1e-5


def layer_norm(values, ln_gain, ln_bias):
    mean_val = jnp.mean(values, axis=-1, keepdims=True)
    centered = values - mean_val
    variance = jnp.mean(centered * centered, axis=-1, keepdims=True)
    return centered * lax.rsqrt(variance + LN_EPS) * ln_gain + ln_bias


def to_bf16(values):
    return values.astype(jnp.bfloat16).astype(jnp.float32)


def tri_block(z_in, mask_f, weights, incoming):
    ln_in, w_proj, b_proj, ln_mid, w_out, b_out = weights
    z_f32 = z_in.astype(jnp.float32)
    z_hat = to_bf16(layer_norm(z_f32, ln_in[0], ln_in[1]))
    proj_all = jnp.dot(z_hat, w_proj) + b_proj
    a_side = to_bf16(jax.nn.sigmoid(proj_all[..., :C_HID]) * proj_all[..., C_HID:2 * C_HID] * mask_f)
    b_side = to_bf16(jax.nn.sigmoid(proj_all[..., 2 * C_HID:3 * C_HID]) * proj_all[..., 3 * C_HID:4 * C_HID] * mask_f)
    g_side = jax.nn.sigmoid(proj_all[..., 4 * C_HID:])
    if incoming:
        tri_x = jnp.einsum("kic,kjc->ijc", a_side, b_side)
    else:
        tri_x = jnp.einsum("ikc,jkc->ijc", a_side, b_side)
    x_hat = to_bf16(layer_norm(tri_x, ln_mid[0], ln_mid[1]))
    update = jnp.dot(x_hat, w_out) + b_out
    return (z_f32 + g_side * update).astype(jnp.bfloat16)


def protein_grads(z_one, mask_one, dz_one, weights_all):
    mask_f = mask_one.astype(jnp.float32)[:, :, None]

    def forward(z_in, weights):
        first_set = tuple(weight_arr[0] for weight_arr in weights)
        second_set = tuple(weight_arr[1] for weight_arr in weights)
        z_mid = tri_block(z_in, mask_f, first_set, False)
        return tri_block(z_mid, mask_f, second_set, True)

    z_new, pull_back = jax.vjp(forward, z_one, weights_all)
    dz_in, d_weights = pull_back(dz_one)
    return z_new, dz_in, d_weights


def setup_inputs(seed: int = 0) -> dict:
    key_list = jax.random.split(jax.random.key(seed), 12)
    pair_shape = (PROTEINS, N_RES, N_RES, C_Z)
    proj_width = 4 * C_HID + C_Z
    z_pair = jax.random.normal(key_list[0], pair_shape, jnp.float32).astype(jnp.bfloat16)
    lengths = jax.random.randint(key_list[1], (PROTEINS,), N_RES // 2, N_RES + 1)
    positions = jnp.arange(N_RES)
    valid_res = positions[None, :] < lengths[:, None]
    pair_mask = (valid_res[:, :, None] & valid_res[:, None, :]).astype(jnp.int32)
    dz_out = jax.random.normal(key_list[2], pair_shape, jnp.float32).astype(jnp.bfloat16)
    ln_in = jnp.stack([1.0 + 0.3 * jax.random.normal(key_list[3], (2, C_Z), jnp.float32), 0.3 * jax.random.normal(key_list[4], (2, C_Z), jnp.float32)], axis=1).astype(jnp.bfloat16)
    w_proj = (jax.random.normal(key_list[5], (2, C_Z, proj_width), jnp.float32) * C_Z ** -0.5).astype(jnp.bfloat16)
    b_proj = (0.5 * jax.random.normal(key_list[6], (2, proj_width), jnp.float32)).astype(jnp.bfloat16)
    ln_mid = jnp.stack([1.0 + 0.3 * jax.random.normal(key_list[7], (2, C_HID), jnp.float32), 0.3 * jax.random.normal(key_list[8], (2, C_HID), jnp.float32)], axis=1).astype(jnp.bfloat16)
    w_out = (jax.random.normal(key_list[9], (2, C_HID, C_Z), jnp.float32) * C_HID ** -0.5).astype(jnp.bfloat16)
    b_out = (0.5 * jax.random.normal(key_list[10], (2, C_Z), jnp.float32)).astype(jnp.bfloat16)
    return {"z_pair": z_pair, "pair_mask": pair_mask, "dz_out": dz_out, "ln_in": ln_in, "w_proj": w_proj, "b_proj": b_proj, "ln_mid": ln_mid, "w_out": w_out, "b_out": b_out}


def reference(z_pair, pair_mask, dz_out, ln_in, w_proj, b_proj, ln_mid, w_out, b_out):
    weights_all = (ln_in.astype(jnp.float32), w_proj.astype(jnp.float32), b_proj.astype(jnp.float32), ln_mid.astype(jnp.float32), w_out.astype(jnp.float32), b_out.astype(jnp.float32))

    def per_protein(operands):
        z_one, mask_one, dz_one = operands
        return protein_grads(z_one, mask_one, dz_one, weights_all)

    z_new, dz_in, d_weights = lax.map(per_protein, (z_pair, pair_mask, dz_out))
    d_ln_in, d_w_proj, d_b_proj, d_ln_mid, d_w_out, d_b_out = d_weights
    return (z_new, dz_in, jnp.sum(d_ln_in, axis=0), jnp.sum(d_w_proj, axis=0), jnp.sum(d_b_proj, axis=0), jnp.sum(d_ln_mid, axis=0), jnp.sum(d_w_out, axis=0), jnp.sum(d_b_out, axis=0))
```

```python
import functools

import jax
import jax.numpy as jnp
from jax import lax
from jax.experimental import pallas as pl
from jax.experimental.pallas import tpu as pltpu
from jax.sharding import PartitionSpec as P

EPS = 1e-5
F32 = jnp.float32
BF16 = jnp.bfloat16
INTERPRET = False
C = 64
RB = 16
UNROLL = 4
VMEM_LIMIT = 56 * 1024 * 1024


def sigm(v):
    return 0.5 * jnp.tanh(0.5 * v) + 0.5


def dot_nn(a, b):
    return lax.dot_general(a, b, (((1,), (0,)), ((), ())), preferred_element_type=F32)


def dot_nt(a, b):
    return lax.dot_general(a, b, (((1,), (1,)), ((), ())), preferred_element_type=F32)


def dot_tn(a, b):
    return lax.dot_general(a, b, (((0,), (0,)), ((), ())), preferred_element_type=F32)


def norm_rows(zf):
    mean = jnp.mean(zf, axis=0, keepdims=True)
    cen = zf - mean
    var = jnp.mean(cen * cen, axis=0, keepdims=True)
    rstd = lax.rsqrt(var + EPS)
    return cen * rstd, rstd


def fold(v):
    return v[:, :128] + v[:, 128:]


def to_cmajor(perm, src, dst, rows=RB):
    n = src.shape[-1]
    for grp in range(C // 16):
        blk = src[:, grp * 16:(grp + 1) * 16, :].reshape(256, n)
        out = dot_nn(perm, blk)
        dst(grp, out.reshape(16, 16, n))


def to_rows(perm, src, dst):
    n = src.shape[-1]
    for grp in range(C // 16):
        blk = src[grp * 16:(grp + 1) * 16, :, :].reshape(256, n)
        out = dot_nn(perm, blk)
        dst[:, grp * 16:(grp + 1) * 16, :] = out.reshape(16, 16, n).astype(BF16)


def split_cols(v, core):
    lo, hi = v[..., :128], v[..., 128:]
    lane = lax.broadcasted_iota(jnp.int32, lo.shape, lo.ndim - 1)
    axis = lo.ndim - 1
    first = jnp.where(lane < 64, lo, pltpu.roll(hi, 64, axis))
    second = jnp.where(lane < 64, pltpu.roll(lo, 64, axis), hi)
    mine = jnp.where(core == 0, first, second)
    other = jnp.where(core == 0, second, first)
    return mine, other


def pre_fwd_kernel(two, split, ids, zp, zo, mask, wt, bias, gain, lbias, perm, *rest):
    outs, (a_s, b_s) = rest[:-2], rest[-2:]
    step = pl.program_id(0)

    def row(i, carry):
        if two:
            zf = jnp.where(step < 4, zp[i], zo[i]).astype(F32)
        else:
            zf = zp[i].astype(F32)
        zn, _ = norm_rows(zf)
        zh = (zn * gain[...] + lbias[...]).astype(BF16)
        p = dot_nn(wt[...], zh) + bias[...]
        m = mask[pl.ds(i, 1), :]
        a_s[i] = (sigm(p[0:C]) * p[C:2 * C] * m).astype(BF16)
        b_s[i] = (sigm(p[2 * C:3 * C]) * p[3 * C:4 * C] * m).astype(BF16)
        return carry

    lax.fori_loop(0, RB, row, 0, unroll=UNROLL)

    def put_a(grp, v):
        outs[0][grp * 16:(grp + 1) * 16] = v.astype(BF16)
        if split:
            mine, other = split_cols(v, ids[1])
            outs[2][grp * 16:(grp + 1) * 16] = mine.astype(BF16)
            outs[3][grp * 16:(grp + 1) * 16] = other.astype(BF16)

    def put_b(grp, v):
        outs[1][grp * 16:(grp + 1) * 16] = v.astype(BF16)

    to_cmajor(perm[...], a_s, put_a)
    to_cmajor(perm[...], b_s, put_b)


def full_spec(shape):
    return pl.BlockSpec(shape, lambda s: (0,) * len(shape))


SMEM_SPEC = pl.BlockSpec(memory_space=pltpu.SMEM)


def peer_map(s):
    return (jnp.minimum(s, 3), 0, 0)


def own_map(s):
    return (jnp.maximum(s - 4, 0), 0, 0)


def call(kernel, grid, in_specs, out_specs, out_shape, scratch, name, flops, bytes_accessed, trans=0):
    return pl.pallas_call(
        kernel,
        grid=grid,
        in_specs=in_specs,
        out_specs=out_specs,
        out_shape=out_shape,
        scratch_shapes=scratch,
        name=name,
        interpret=INTERPRET,
        cost_estimate=pl.CostEstimate(flops=flops, bytes_accessed=bytes_accessed, transcendentals=trans),
        compiler_params=pltpu.CompilerParams(dimension_semantics=("arbitrary",) * len(grid), vmem_limit_bytes=VMEM_LIMIT),
    )


def pre_forward(ids, z_parts, mask2, par, split, name):
    n = z_parts[0].shape[-1]
    two = len(z_parts) == 2
    rows = 128
    zspec = [pl.BlockSpec((RB, C, n), peer_map), pl.BlockSpec((RB, C, n), own_map)] if two else [pl.BlockSpec((RB, C, n), lambda s: (s, 0, 0)), pl.BlockSpec((1, 8, 128), lambda s: (0, 0, 0))]
    z_args = z_parts if two else (z_parts[0], jnp.zeros((1, 8, 128), F32))
    cspec = pl.BlockSpec((C, RB, n), lambda s: (0, s, 0))
    hspec = pl.BlockSpec((C, RB, 128), lambda s: (0, s, 0))
    out_shape = [jax.ShapeDtypeStruct((C, rows, n), BF16)] * 2
    out_specs = [cspec] * 2
    if split:
        out_shape = out_shape + [jax.ShapeDtypeStruct((C, rows, 128), BF16)] * 2
        out_specs = out_specs + [hspec] * 2
    fn = call(
        functools.partial(pre_fwd_kernel, two, split), (rows // RB,),
        [SMEM_SPEC] + zspec + [pl.BlockSpec((RB, n), lambda s: (s, 0)), full_spec((4 * C, C)), full_spec((4 * C, n)), full_spec((C, n)), full_spec((C, n)), full_spec((256, 256))],
        out_specs, out_shape, [pltpu.VMEM((RB, C, n), BF16)] * 2, name, 4 * 10 ** 9, 16 * 2 ** 20)
    return fn(ids, *z_args, mask2, par["wt_ab"], par["bias_ab"], par["gain"], par["lbias"], par["perm"])


CB = 8


def global_rows(ids, partner):
    x, c = ids[0], ids[1]
    cc = 1 - c if partner else c
    return pl.multiple_of(64 * (2 * (1 - x) + cc), 64), pl.multiple_of(64 * (2 * x + cc), 64)


def place(dst, src_mine, src_other, ids):
    for src, partner in ((src_mine, False), (src_other, True)):
        off_peer, off_own = global_rows(ids, partner)
        dst[pl.ds(off_peer, 64), :] = src[0:64, :]
        dst[pl.ds(off_own, 64), :] = src[64:128, :]


def tri_out_kernel(ids, a, b, bp, x, full):
    for ch in range(CB):
        buf = full.at[ch % 2]
        place(buf, b[ch], bp[ch], ids)
        x[ch] = dot_nt(a[ch], buf[...])


def tri_in_kernel(ids, ak, ar, b, bp, x):
    xx = ids[0]
    for ch in range(CB):
        out = dot_tn(ak[ch], b[ch]) + dot_tn(ar[ch], bp[ch])
        x[ch, pl.ds(pl.multiple_of(64 * (1 - xx), 64), 64), :] = out[0:64]
        x[ch, pl.ds(pl.multiple_of(64 * xx, 64), 64), :] = out[64:128]

def tri_in_bwd_kernel(ids, a, b, dx, dxp, da, db, full):
    for ch in range(CB):
        buf = full.at[ch % 2]
        place(buf, dx[ch], dxp[ch], ids)
        da[ch] = dot_nt(b[ch], buf[...]).astype(BF16)
        db[ch] = dot_nn(a[ch], buf[...]).astype(BF16)


def tri_out_bwd_kernel(ids, dx, b, bp, dxk, dxr, a, ap, da, db, full, tmp):
    xx = ids[0]
    for ch in range(CB):
        buf = full.at[ch % 2]
        place(buf, b[ch], bp[ch], ids)
        da[ch] = dot_nn(dx[ch, 64:128, :], buf[...]).astype(BF16)
        tmp[ch % 2] = dot_tn(dxk[ch], a[ch]) + dot_tn(dxr[ch], ap[ch])
        db[ch] = tmp[ch % 2, pl.ds(pl.multiple_of(64 * xx, 64), 64), :].astype(BF16)


def tri_call(kernel, ids, args, outs, scratch, name, flops):
    def cspec(shape):
        return pl.BlockSpec((CB,) + tuple(shape[1:]), lambda s: (s, 0, 0))
    nbytes = sum(v.size * v.dtype.itemsize for v in args) + sum(o.size * o.dtype.itemsize for o in outs)
    return call(kernel, (C // CB,), [SMEM_SPEC] + [cspec(v.shape) for v in args], [cspec(o.shape) for o in outs], outs, scratch, name, flops, nbytes)(ids, *args)


def mid_norm(x, xh_s, lnmid, keep_r, keep_mean):
    tot = x[0]
    for c in range(1, C):
        tot = tot + x[c]
    mean = tot * (1.0 / C)
    d = x[0] - mean
    sq = d * d
    for c in range(1, C):
        d = x[c] - mean
        sq = sq + d * d
    rstd = lax.rsqrt(sq * (1.0 / C) + EPS)
    keep_mean[...] = mean
    keep_r[...] = rstd
    for c in range(C):
        xh_s[c] = ((x[c] - mean) * rstd * lnmid[0, c] + lnmid[1, c]).astype(BF16)


def post_fwd_kernel(x, zp, zo, wgt, bg, gain, lbias, wot, bo, lnmid, perm, zmid, xh_s, xi_s, r_s, m_s):
    step = pl.program_id(0)
    mid_norm(x, xh_s, lnmid, r_s, m_s)
    to_rows(perm[...], xh_s, xi_s)

    def row(i, carry):
        zf = jnp.where(step < 4, zp[i], zo[i]).astype(F32)
        zn, _ = norm_rows(zf)
        zh = (zn * gain[...] + lbias[...]).astype(BF16)
        g = sigm(dot_nn(wgt[...], zh) + bg[...])
        upd = dot_nn(wot[...], xi_s[i]) + bo[...]
        zmid[i] = (zf + g * upd).astype(BF16)
        return carry

    lax.fori_loop(0, RB, row, 0, unroll=UNROLL)


def post_forward(x0, zp, zo, par):
    n = zp.shape[-1]
    fn = call(
        post_fwd_kernel, (8,),
        [pl.BlockSpec((C, RB, n), lambda s: (0, s, 0)), pl.BlockSpec((RB, C, n), peer_map), pl.BlockSpec((RB, C, n), own_map)] + [full_spec((C, C)), full_spec((C, n)), full_spec((C, n)), full_spec((C, n)), full_spec((C, C)), full_spec((C, n)), SMEM_SPEC, full_spec((256, 256))],
        [pl.BlockSpec((RB, C, n), lambda s: (s, 0, 0))], [jax.ShapeDtypeStruct((128, C, n), BF16)],
        [pltpu.VMEM((C, RB, n), BF16), pltpu.VMEM((RB, C, n), BF16), pltpu.VMEM((RB, n), F32), pltpu.VMEM((RB, n), F32)],
        "post_fwd0", 2 * 10 ** 9, 20 * 2 ** 20)
    return fn(x0, zp, zo, par["wt_g"], par["bias_g"], par["gain"], par["lbias"], par["wo_t"], par["bo"], par["lnmid"], par["perm"])[0]


def post_bwd_kernel(second, ids, x, zp, zo, dzp, dzo, wgt, bg, gain, lbias, wot, wo, bo, lnmid, perm, *rest):
    if second:
        znew, dx, dpg, acc_bg, acc_bo, acc_wo, acc_mg, acc_mb = rest[:8]
    else:
        dx, dxk, dxs, dpg, acc_bg, acc_bo, acc_wo, acc_mg, acc_mb = rest[:9]
    xh_s, xi_s, dxi_s, dxc_s, r_s, m_s = rest[-6:]
    step = pl.program_id(0)

    @pl.when(step == 0)
    def _():
        for acc in (acc_bg, acc_bo, acc_wo, acc_mg, acc_mb):
            acc[...] = jnp.zeros_like(acc)

    mid_norm(x, xh_s, lnmid, r_s, m_s)
    to_rows(perm[...], xh_s, xi_s)

    def row(i, carry):
        if second:
            zf = zp[i].astype(F32)
            dz = jnp.where(step < 4, dzp[i], dzo[i]).astype(F32)
        else:
            zf = jnp.where(step < 4, zp[i], zo[i]).astype(F32)
            dz = dzp[i].astype(F32)
        zn, _ = norm_rows(zf)
        zh = (zn * gain[...] + lbias[...]).astype(BF16)
        g = sigm(dot_nn(wgt[...], zh) + bg[...])
        xi = xi_s[i]
        upd = dot_nn(wot[...], xi) + bo[...]
        if second:
            znew[i] = (zf + g * upd).astype(BF16)
        d_pg = dz * upd * (g * (1.0 - g))
        d_upd = dz * g
        dpg[i] = d_pg.astype(BF16)
        dub = d_upd.astype(BF16)
        acc_bg[...] += fold(d_pg)
        acc_bo[...] += fold(d_upd)
        acc_wo[...] += dot_nt(dub, xi)
        dxi_s[i] = dot_nn(wo[...], dub).astype(BF16)
        return carry

    lax.fori_loop(0, RB, row, 0, unroll=UNROLL)

    def put(grp, v):
        dxc_s[grp * 16:(grp + 1) * 16] = v

    to_cmajor(perm[...], dxi_s, put)
    mean, rstd = m_s[...], r_s[...]
    m1 = jnp.zeros_like(mean)
    m2 = jnp.zeros_like(mean)
    for c in range(C):
        dy = dxc_s[c]
        xn = (x[c] - mean) * rstd
        dyx = dy * xn
        gn = lnmid[0, c]
        m1 = m1 + dy * gn
        m2 = m2 + dyx * gn
        acc_mg[c] += fold(dyx[0:8] + dyx[8:16])
        acc_mb[c] += fold(dy[0:8] + dy[8:16])
    m1 = m1 * (1.0 / C)
    m2 = m2 * (1.0 / C)
    for c in range(C):
        xn = (x[c] - mean) * rstd
        v = rstd * (dxc_s[c] * lnmid[0, c] - m1 - xn * m2)
        dx[c] = v.astype(BF16)
        if not second:
            mine, other = split_cols(v, ids[1])
            dxk[c] = mine.astype(BF16)
            dxs[c] = other.astype(BF16)


def post_backward(ids, second, x, z_parts, dz_parts, par, name):
    n = x.shape[-1]
    cspec = pl.BlockSpec((C, RB, n), lambda s: (0, s, 0))
    hspec = pl.BlockSpec((C, RB, 128), lambda s: (0, s, 0))
    rspec = pl.BlockSpec((RB, C, n), lambda s: (s, 0, 0))
    two = [pl.BlockSpec((RB, C, n), peer_map), pl.BlockSpec((RB, C, n), own_map)]
    one = [rspec, pl.BlockSpec((1, 8, 128), lambda s: (0, 0, 0))]
    dummy = jnp.zeros((1, 8, 128), F32)
    zspec, dzspec = (one, two) if second else (two, one)
    z_args = (z_parts[0], dummy) if second else z_parts
    dz_args = dz_parts if second else (dz_parts[0], dummy)
    acc_shapes = [(C, 128), (C, 128), (C, C), (C, 8, 128), (C, 8, 128)]
    accs = [jax.ShapeDtypeStruct(s, F32) for s in acc_shapes]
    acc_specs = [full_spec(s) for s in acc_shapes]
    c_out = jax.ShapeDtypeStruct((C, 128, n), BF16)
    h_out = jax.ShapeDtypeStruct((C, 128, 128), BF16)
    r_out = jax.ShapeDtypeStruct((128, C, n), BF16)
    if second:
        outs = [jax.ShapeDtypeStruct((64, C, n), BF16), c_out, r_out]
        ospecs = [pl.BlockSpec((RB, C, n), own_map), cspec, rspec]
    else:
        outs = [c_out, h_out, h_out, r_out]
        ospecs = [cspec, hspec, hspec, rspec]
    fn = call(
        functools.partial(post_bwd_kernel, second), (8,),
        [SMEM_SPEC, cspec] + zspec + dzspec + [full_spec((C, C)), full_spec((C, n)), full_spec((C, n)), full_spec((C, n)), full_spec((C, C)), full_spec((C, C)), full_spec((C, n)), SMEM_SPEC, full_spec((256, 256))],
        ospecs + acc_specs, outs + accs,
        [pltpu.VMEM((C, RB, n), BF16), pltpu.VMEM((RB, C, n), BF16), pltpu.VMEM((RB, C, n), BF16), pltpu.VMEM((C, RB, n), F32), pltpu.VMEM((RB, n), F32), pltpu.VMEM((RB, n), F32)],
        name, 4 * 10 ** 9, 30 * 2 ** 20)
    return fn(ids, x, *z_args, *dz_args, par["wt_g"], par["bias_g"], par["gain"], par["lbias"], par["wo_t"], par["wo"], par["bo"], par["lnmid"], par["perm"])


def pre_bwd_kernel(two, z, da, db, dpg, drp, dro, mask, wt, bias, w, gain, lbias, perm, dz, acc_w, acc_b, acc_g, acc_lb, dai_s, dbi_s, dp_s):
    step = pl.program_id(0)

    @pl.when(step == 0)
    def _():
        for acc in (acc_w, acc_b, acc_g, acc_lb):
            acc[...] = jnp.zeros_like(acc)

    to_rows(perm[...], da, dai_s)
    to_rows(perm[...], db, dbi_s)

    def row(i, carry):
        zn, rstd = norm_rows(z[i].astype(F32))
        zh = (zn * gain[...] + lbias[...]).astype(BF16)
        p = dot_nn(wt[...], zh) + bias[...]
        m = mask[pl.ds(i, 1), :]
        for side, ref in ((0, dai_s), (1, dbi_s)):
            base = side * 2 * C
            dm = ref[i].astype(F32) * m
            sg = sigm(p[base:base + C])
            dv = dm * sg
            dg = dv * p[base + C:base + 2 * C] * (1.0 - sg)
            acc_b[base:base + C] += fold(dg)
            acc_b[base + C:base + 2 * C] += fold(dv)
            dp_s[i, base:base + C] = dg.astype(BF16)
            dp_s[i, base + C:base + 2 * C] = dv.astype(BF16)
        dp_s[i, 4 * C:5 * C] = dpg[i]
        dp = dp_s[i]
        acc_w[...] += dot_nt(dp, zh)
        dzh = dot_nn(w[...], dp).astype(BF16).astype(F32)
        acc_g[...] += fold(dzh * zn)
        acc_lb[...] += fold(dzh)
        dzn = dzh * gain[...]
        m1 = jnp.mean(dzn, axis=0, keepdims=True)
        m2 = jnp.mean(dzn * zn, axis=0, keepdims=True)
        dzf = rstd * (dzn - m1 - zn * m2)
        if two:
            dr = jnp.where(step < 4, drp[i], dro[i]).astype(F32)
        else:
            dr = drp[i].astype(F32)
        dz[i] = (dr + dzf).astype(BF16)
        return carry

    lax.fori_loop(0, RB, row, 0, unroll=UNROLL)


def pre_backward(z, da, db, dpg, dres_parts, mask2, par, own_only, name):
    n = z.shape[-1]
    steps = da.shape[1] // RB
    off = 4 if own_only else 0
    two = len(dres_parts) == 2
    cspec = pl.BlockSpec((C, RB, n), lambda s: (0, s, 0))
    rspec = pl.BlockSpec((RB, C, n), lambda s: (s, 0, 0))
    hspec = pl.BlockSpec((RB, C, n), lambda s: (s + off, 0, 0))
    if two:
        drspec = [pl.BlockSpec((RB, C, n), peer_map), pl.BlockSpec((RB, C, n), own_map)]
        dr_args = dres_parts
    else:
        drspec = [hspec, pl.BlockSpec((1, 8, 128), lambda s: (0, 0, 0))]
        dr_args = (dres_parts[0], jnp.zeros((1, 8, 128), F32))
    acc_shapes = [(5 * C, C), (4 * C, 128), (C, 128), (C, 128)]
    fn = call(
        functools.partial(pre_bwd_kernel, two), (steps,),
        [rspec, cspec, cspec, hspec] + drspec + [pl.BlockSpec((RB, n), lambda s: (s + off, 0)), full_spec((4 * C, C)), full_spec((4 * C, n)), full_spec((C, 5 * C)), full_spec((C, n)), full_spec((C, n)), full_spec((256, 256))],
        [rspec] + [full_spec(s) for s in acc_shapes],
        [jax.ShapeDtypeStruct((steps * RB, C, n), BF16)] + [jax.ShapeDtypeStruct(s, F32) for s in acc_shapes],
        [pltpu.VMEM((RB, C, n), BF16), pltpu.VMEM((RB, C, n), BF16), pltpu.VMEM((RB, 5 * C, n), BF16)],
        name, 6 * 10 ** 9 * steps // 8, 30 * 2 ** 20 * steps // 8)
    return fn(z, da, db, dpg, *dr_args, mask2, par["wt_ab"], par["bias_ab"], par["w"], par["gain"], par["lbias"], par["perm"])


def make_params(blk, n, perm, ln_in, w_proj, b_proj, ln_mid, w_out, b_out):
    def wide(v):
        return jnp.broadcast_to(v.astype(F32)[:, None], (v.shape[0], n))
    wt = w_proj[blk].T
    return dict(
        wt_ab=wt[:4 * C], wt_g=wt[4 * C:], w=w_proj[blk], bias_ab=wide(b_proj[blk, :4 * C]), bias_g=wide(b_proj[blk, 4 * C:]),
        gain=wide(ln_in[blk, 0]), lbias=wide(ln_in[blk, 1]), wo_t=w_out[blk].T, wo=w_out[blk], bo=wide(b_out[blk]),
        lnmid=ln_mid[blk].astype(F32), perm=perm)


def solution(mesh):
    def local_step(z_pair, pair_mask, dz_out, ln_in, w_proj, b_proj, ln_mid, w_out, b_out):
        n = z_pair.shape[2]
        dap = lax.axis_index("dap")
        ids = jnp.stack([dap // 2, dap % 2]).astype(jnp.int32)
        x_pairs = [(0, 2), (2, 0), (1, 3), (3, 1)]
        c_pairs = [(0, 1), (1, 0), (2, 3), (3, 2)]

        def over_x(v):
            return lax.ppermute(v, "dap", x_pairs)

        def over_c(v):
            return lax.ppermute(v, "dap", c_pairs)

        r_i = jnp.arange(256)
        perm = (r_i[None, :] == (16 * (r_i % 16) + r_i // 16)[:, None]).astype(BF16)
        par = [make_params(k, n, perm, ln_in, w_proj, b_proj, ln_mid, w_out, b_out) for k in range(2)]

        z_own = jnp.transpose(z_pair[0], (0, 2, 1))
        dz_own = jnp.transpose(dz_out[0], (0, 2, 1))
        z_peer = over_x(z_own)
        mask2 = jnp.concatenate([over_x(pair_mask[0]), pair_mask[0]], axis=0).astype(F32)
        dz_peer = over_x(dz_own)

        sds = jax.ShapeDtypeStruct
        a0, b0 = pre_forward(ids, (z_peer, z_own), mask2, par[0], False, "pre_fwd0")
        b0p = over_c(b0)
        a0p = over_c(a0)
        (x0,) = tri_call(tri_out_kernel, ids, (a0, b0, b0p), [sds((C, 128, n), F32)], [pltpu.VMEM((2, n, n), BF16)], "tri_fwd0", 2 * 10 ** 9)
        z_mid = post_forward(x0, z_peer, z_own, par[0])
        a1, b1, a1k, a1s = pre_forward(ids, (z_mid,), mask2, par[1], True, "pre_fwd1")
        a1r = over_c(a1s)
        b1p = over_c(b1)
        (x1,) = tri_call(tri_in_kernel, ids, (a1k, a1r, b1, b1p), [sds((C, 128, n), F32)], [], "tri_fwd1", 2 * 10 ** 9)
        z_new, dx1, dpg1, bg1, bo1, wo1, mg1, mb1 = post_backward(ids, True, x1, (z_mid,), (dz_peer, dz_own), par[1], "post1")
        dx1p = over_c(dx1)
        da1, db1 = tri_call(tri_in_bwd_kernel, ids, (a1, b1, dx1, dx1p), [sds((C, 128, n), BF16)] * 2, [pltpu.VMEM((2, n, n), BF16)], "tri_bwd1", 4 * 10 ** 9)
        dz_mid, w1, b1s, g1, lb1 = pre_backward(z_mid, da1, db1, dpg1, (dz_peer, dz_own), mask2, par[1], False, "pre_bwd1")
        dx0, dx0k, dx0s, dpg0, bg0, bo0, wo0, mg0, mb0 = post_backward(ids, False, x0, (z_peer, z_own), (dz_mid,), par[0], "post0")
        dx0r = over_c(dx0s)
        da0, db0 = tri_call(tri_out_bwd_kernel, ids, (dx0, b0, b0p, dx0k, dx0r, a0, a0p), [sds((C, 64, n), BF16)] * 2, [pltpu.VMEM((2, n, n), BF16), pltpu.VMEM((2, 128, n), F32)], "tri_bwd0", 3 * 10 ** 9)
        dz, w0, b0s, g0, lb0 = pre_backward(z_own, da0, db0, dpg0, (dz_mid,), mask2, par[0], True, "pre_bwd0")

        def lanes(v):
            return jnp.sum(v, axis=tuple(range(1, v.ndim)))

        half = 0.5
        d_w = jnp.stack([w0, half * w1])
        d_wo = half * jnp.stack([wo0, wo1])
        vec = jnp.concatenate([lanes(g0), lanes(lb0), half * lanes(g1), half * lanes(lb1), lanes(b0s), half * lanes(bg0), half * lanes(b1s), half * lanes(bg1), half * lanes(mg0), half * lanes(mb0), half * lanes(mg1), half * lanes(mb1), half * lanes(bo0), half * lanes(bo1)])
        flat = jnp.concatenate([d_w.reshape(-1), d_wo.reshape(-1), vec]).reshape(-1, 128)
        flat = lax.psum(flat, ("dp", "dap")).reshape(-1)
        n_w, n_wo = d_w.size, d_wo.size
        gw = jnp.transpose(flat[:n_w].reshape(2, 5 * C, C), (0, 2, 1))
        gwo = jnp.transpose(flat[n_w:n_w + n_wo].reshape(2, C, C), (0, 2, 1))
        vec = flat[n_w + n_wo:]
        g_ln_in = vec[:4 * C].reshape(2, 2, C)
        g_bp = vec[4 * C:14 * C].reshape(2, 5 * C)
        g_lm = vec[14 * C:18 * C].reshape(2, 2, C)
        g_bo = vec[18 * C:20 * C].reshape(2, C)
        z_res = jnp.transpose(z_new, (0, 2, 1))[None]
        dz_res = jnp.transpose(dz, (0, 2, 1))[None]
        return z_res, dz_res, g_ln_in, gw, g_bp, g_lm, gwo, g_bo

    row_spec = P("dp", "dap")
    return jax.shard_map(local_step, mesh=mesh, in_specs=(row_spec, row_spec, row_spec, P(), P(), P(), P(), P(), P()), out_specs=(row_spec, row_spec, P(), P(), P(), P(), P(), P()), check_vma=False)
```

```python
import functools

import jax
import jax.numpy as jnp
from jax import lax
from jax.experimental import pallas as pl
from jax.experimental.pallas import tpu as pltpu
from jax.sharding import PartitionSpec as P


EPS = 1e-5
F32 = jnp.float32
BF16 = jnp.bfloat16
INTERPRET = False
C = 64
RB = 16
UNROLL = 16
DELAY = 4
LANES = 128
W2 = 256
HALF = 0.5
MEGA = 10 ** 6
GIGA = 10 ** 9
MIB = 2 ** 20
VMEM_LIMIT = 56 * 1024 * 1024


MESH_ID = pl.DeviceIdType.MESH


def dot_nn(a, b):
    return lax.dot_general(a, b, (((1,), (0,)), ((), ())), preferred_element_type=F32)


def dot_nt(a, b):
    return lax.dot_general(a, b, (((1,), (1,)), ((), ())), preferred_element_type=F32)


def dot_tn(a, b):
    return lax.dot_general(a, b, (((0,), (0,)), ((), ())), preferred_element_type=F32)


def norm_rows(zf):
    mean = jnp.mean(zf, axis=0, keepdims=True)
    cen = zf - mean
    var = jnp.mean(cen * cen, axis=0, keepdims=True)
    rstd = lax.rsqrt(var + EPS)
    return cen * rstd, rstd


def staggered(first, second):
    for i in range(RB + DELAY):
        if i < RB:
            first(i)
        if i >= DELAY:
            second(i - DELAY)


def fold(v):
    return v[:, :LANES] + v[:, LANES:]


def to_cmajor(perm, src, dst):
    n = src.shape[-1]
    for grp in range(C // RB):
        blk = src[:, grp * RB:(grp + 1) * RB, :].reshape(W2, n)
        out = dot_nn(perm, blk)
        dst(grp, out.reshape(RB, RB, n))


def to_rows(perm, src, dst):
    n = src.shape[-1]
    for grp in range(C // RB):
        blk = src[grp * RB:(grp + 1) * RB, :, :].reshape(W2, n)
        out = dot_nn(perm, blk)
        dst[:, grp * RB:(grp + 1) * RB, :] = out.reshape(RB, RB, n).astype(BF16)


def split_cols(v, core):
    lo, hi = v[..., :LANES], v[..., LANES:]
    lane = lax.broadcasted_iota(jnp.int32, lo.shape, lo.ndim - 1)
    axis = lo.ndim - 1
    first = jnp.where(lane < C, lo, pltpu.roll(hi, C, axis))
    second = jnp.where(lane < C, pltpu.roll(lo, C, axis), hi)
    mine = jnp.where(core == 0, first, second)
    other = jnp.where(core == 0, second, first)
    return mine, other


KA = C + RB


def prep_kernel(w_proj, b_proj, ln_in, w_out, b_out, wt_aug, wot_aug, gain, lbias, perm, scr):
    n = gain.shape[-1]
    for k in range(2):
        scr[:] = jnp.zeros_like(scr)
        scr[0:C, 0:5 * C] = w_proj[k].astype(F32)
        scr[C:C + 1, 0:5 * C] = b_proj[pl.ds(k, 1), :]
        wt_aug[k] = (HALF * jnp.transpose(scr[:]))[0:5 * C, 0:KA].astype(BF16)
        scr[:] = jnp.zeros_like(scr)
        scr[0:C, 0:C] = w_out[k].astype(F32)
        scr[C:C + 1, 0:C] = b_out[pl.ds(k, 1), :]
        scr[C + 8:C + 10, 0:C] = ln_in[k]
        small = jnp.transpose(scr[:, 0:LANES])
        wot_aug[k] = (HALF * small)[0:C, 0:KA].astype(BF16)
        gain[k] = jnp.broadcast_to(small[0:C, C + 8:C + 9], (C, n))
        lbias[k] = jnp.broadcast_to(small[0:C, C + 9:C + 10], (C, n))
    r = lax.broadcasted_iota(jnp.int32, (W2, W2), 0)
    q = lax.broadcasted_iota(jnp.int32, (W2, W2), 1)
    perm[:] = jnp.where(q == RB * (r % RB) + r // RB, 1.0, 0.0).astype(BF16)


def prepare(n, ln_in, w_proj, b_proj, w_out, b_out):
    sds = jax.ShapeDtypeStruct
    outs = [sds((2, 5 * C, KA), BF16), sds((2, C, KA), BF16), sds((2, C, n), F32), sds((2, C, n), F32), sds((W2, W2), BF16)]
    args = (w_proj, b_proj.astype(F32), ln_in.astype(F32), w_out, b_out.astype(F32))
    return call(prep_kernel, (1,), [full_spec(v.shape) for v in args], [full_spec(o.shape) for o in outs], outs, [pltpu.VMEM((LANES, 384), F32)], MEGA, MIB)(*args)


def with_ones(zh):
    row = lax.broadcasted_iota(jnp.int32, (RB, zh.shape[-1]), 0)
    return jnp.concatenate([zh, jnp.where(row == 0, 1.0, 0.0).astype(BF16)], axis=0)


def pre_fwd_kernel(split, ids, z, *rest):
    n_mask = 2 if split else 1
    masks = rest[:n_mask]
    wt, gain, lbias, perm = rest[n_mask:n_mask + 4]
    outs, (a_s, b_s) = rest[n_mask + 4:-2], rest[-2:]
    step = pl.program_id(0)

    def row(i, carry):
        zn, _ = norm_rows(z[i].astype(F32))
        zh = (zn * gain[:] + lbias[:]).astype(BF16)
        p = dot_nn(wt[0:4 * C], with_ones(zh))
        m = masks[0][pl.ds(i, 1), :]
        if split:
            m = jnp.where(step < 4, m, masks[1][pl.ds(i, 1), :])
        m = m.astype(F32)
        a_s[i] = ((1.0 + jnp.tanh(p[0:C])) * (p[C:2 * C] * m)).astype(BF16)
        b_s[i] = ((1.0 + jnp.tanh(p[2 * C:3 * C])) * (p[3 * C:4 * C] * m)).astype(BF16)
        return carry

    lax.fori_loop(0, RB, row, 0, unroll=UNROLL)

    def put_a(grp, v):
        outs[0][grp * RB:(grp + 1) * RB] = v.astype(BF16)
        if split:
            mine, other = split_cols(v, ids[1])
            outs[2][grp * RB:(grp + 1) * RB] = mine.astype(BF16)
            outs[3][grp * RB:(grp + 1) * RB] = other.astype(BF16)

    def put_b(grp, v):
        outs[1][grp * RB:(grp + 1) * RB] = v.astype(BF16)

    to_cmajor(perm[:], a_s, put_a)
    to_cmajor(perm[:], b_s, put_b)


def full_spec(shape):
    return pl.BlockSpec(shape, lambda s: (0,) * len(shape))


SMEM_SPEC = pl.BlockSpec(memory_space=pltpu.SMEM)


def peer_map(s):
    return (jnp.minimum(s, 3), 0, 0)


def own_map(s):
    return (jnp.maximum(s - 4, 0), 0, 0)


def call(kernel, grid, in_specs, out_specs, out_shape, scratch, flops, bytes_accessed, trans=0):
    return pl.pallas_call(
        kernel,
        grid=grid,
        in_specs=in_specs,
        out_specs=out_specs,
        out_shape=out_shape,
        scratch_shapes=scratch,
        interpret=INTERPRET,
        cost_estimate=pl.CostEstimate(flops=flops, bytes_accessed=bytes_accessed, transcendentals=trans),
        compiler_params=pltpu.CompilerParams(dimension_semantics=("arbitrary",) * len(grid), vmem_limit_bytes=VMEM_LIMIT),
    )


def peer_map2(s):
    return (jnp.minimum(s, 3), 0)


def own_map2(s):
    return (jnp.maximum(s - 4, 0), 0)


def blk_spec(shape, k):
    return pl.BlockSpec((None,) + tuple(shape[1:]), lambda s: (k,) + (0,) * (len(shape) - 1))


def pre_forward(ids, z, masks, par, blk):
    rows, _, n = z.shape
    split = len(masks) == 2
    mspec = [pl.BlockSpec((RB, n), peer_map2), pl.BlockSpec((RB, n), own_map2)] if split else [pl.BlockSpec((RB, n), lambda s: (s, 0))]
    cspec = pl.BlockSpec((C, RB, n), lambda s: (0, s, 0))
    hspec = pl.BlockSpec((C, RB, LANES), lambda s: (0, s, 0))
    out_shape = [jax.ShapeDtypeStruct((C, rows, n), BF16)] * 2
    out_specs = [cspec] * 2
    if split:
        out_shape = out_shape + [jax.ShapeDtypeStruct((C, rows, LANES), BF16)] * 2
        out_specs = out_specs + [hspec] * 2
    wt, _, gain, lbias, perm = par
    fn = call(
        functools.partial(pre_fwd_kernel, split), (rows // RB,),
        [SMEM_SPEC, pl.BlockSpec((RB, C, n), lambda s: (s, 0, 0))] + mspec + [blk_spec(wt.shape, blk), blk_spec(gain.shape, blk), blk_spec(gain.shape, blk), full_spec((W2, W2))],
        out_specs, out_shape, [pltpu.VMEM((RB, C, n), BF16)] * 2, GIGA * rows // LANES, rows * MIB // 8)
    return fn(ids, z, *masks, wt, gain, lbias, perm)


CB = 8


def global_rows(ids, partner):
    x, c = ids[0], ids[1]
    cc = 1 - c if partner else c
    return pl.multiple_of(C * (2 * (1 - x) + cc), C), pl.multiple_of(C * (2 * x + cc), C)


def place(dst, src_mine, src_other, ids):
    for (peer, own), partner in ((src_mine, False), (src_other, True)):
        off_peer, off_own = global_rows(ids, partner)
        dst[pl.ds(off_peer, C), :] = peer
        dst[pl.ds(off_own, C), :] = own


def halves(ref):
    return ref[0:C, :], ref[C:LANES, :]


def tri_out_kernel(ids, ap, ao, bp, bo, qp, qo, x, full):
    for ch in range(CB):
        buf = full.at[ch % 2]
        place(buf, (bp[ch], bo[ch]), (qp[ch], qo[ch]), ids)
        x[ch] = dot_nt(jnp.concatenate([ap[ch], ao[ch]], axis=0), buf[:])


def tri_in_kernel(ids, ak, ar, b, bp, x):
    xx = ids[0]
    for ch in range(CB):
        out = dot_tn(ak[ch], b[ch]) + dot_tn(ar[ch], bp[ch])
        x[ch, pl.ds(pl.multiple_of(C * (1 - xx), C), C), :] = out[0:C]
        x[ch, pl.ds(pl.multiple_of(C * xx, C), C), :] = out[C:LANES]


def tri_in_bwd_kernel(ids, a, b, dx, dxp, da, db, full):
    for ch in range(CB):
        buf = full.at[ch % 2]
        place(buf, halves(dx.at[ch]), halves(dxp.at[ch]), ids)
        da[ch] = dot_nt(b[ch], buf[:]).astype(BF16)
        db[ch] = dot_nn(a[ch], buf[:]).astype(BF16)


def tri_out_bwd_kernel(ids, dx, bp, bo, qp, qo, dxk, dxr, ap, ao, rp, ro, da, db, full, tmp):
    xx = ids[0]
    for ch in range(CB):
        buf = full.at[ch % 2]
        place(buf, (bp[ch], bo[ch]), (qp[ch], qo[ch]), ids)
        da[ch] = dot_nn(dx[ch], buf[:]).astype(BF16)
        tmp[ch % 2] = dot_tn(dxk[ch], jnp.concatenate([ap[ch], ao[ch]], axis=0)) + dot_tn(dxr[ch], jnp.concatenate([rp[ch], ro[ch]], axis=0))
        db[ch] = tmp[ch % 2, pl.ds(pl.multiple_of(C * xx, C), C), :].astype(BF16)


def tri_call(kernel, ids, args, outs, scratch, flops, own_first=False):
    def cspec(shape, row_blk=0):
        return pl.BlockSpec((CB,) + tuple(shape[1:]), lambda s: (s, row_blk, 0))

    nbytes = sum(v.size * v.dtype.itemsize for v in args) + sum(o.size * o.dtype.itemsize for o in outs)
    return call(kernel, (C // CB,), [SMEM_SPEC] + ([cspec((C, C) + args[0].shape[2:], 1)] if own_first else [cspec(args[0].shape)]) + [cspec(v.shape) for v in args[1:]], [cspec(o.shape) for o in outs], outs, scratch, flops, nbytes)(ids, *args)


def mid_norm(x, xh_s, lnmid, blk, xn_s=None, rstd_s=None):
    tot = x[0]
    for c in range(1, C):
        tot = tot + x[c]
    mean = tot * (1.0 / C)
    d = x[0] - mean
    sq = d * d
    for c in range(1, C):
        d = x[c] - mean
        sq = sq + d * d
    rstd = lax.rsqrt(sq * (1.0 / C) + EPS)
    if rstd_s is not None:
        rstd_s[:] = rstd
    for c in range(C):
        xn = (x[c] - mean) * rstd
        if xn_s is not None:
            xn_s[c] = xn
        xh_s[c] = (xn * lnmid[blk, 0, c] + lnmid[blk, 1, c]).astype(BF16)


def gate_of(zf, wt, gain, lbias):
    zn, _ = norm_rows(zf)
    zh = (zn * gain[:] + lbias[:]).astype(BF16)
    return jnp.tanh(dot_nn(wt[4 * C:5 * C], with_ones(zh)))


def post_fwd_kernel(blk, x, zp, zo, wt, gain, lbias, wot, lnmid, perm, zmid, xh_s, xi_s):
    step = pl.program_id(0)
    mid_norm(x, xh_s, lnmid, blk)
    to_rows(perm[:], xh_s, xi_s)

    def row(i, carry):
        zf = jnp.where(step < 4, zp[i], zo[i]).astype(F32)
        t = gate_of(zf, wt, gain, lbias)
        upd = dot_nn(wot[:], with_ones(xi_s[i]))
        zmid[i] = (zf + (1.0 + t) * upd).astype(BF16)
        return carry

    lax.fori_loop(0, RB, row, 0, unroll=UNROLL)


def post_forward(x0, zp, zo, par, lnmid, blk):
    n = zp.shape[-1]
    wt, wot, gain, lbias, perm = par
    fn = call(
        functools.partial(post_fwd_kernel, blk), (8,),
        [pl.BlockSpec((C, RB, n), lambda s: (0, s, 0)), pl.BlockSpec((RB, C, n), peer_map), pl.BlockSpec((RB, C, n), own_map), blk_spec(wt.shape, blk), blk_spec(gain.shape, blk), blk_spec(gain.shape, blk), blk_spec(wot.shape, blk), SMEM_SPEC, full_spec((W2, W2))],
        [pl.BlockSpec((RB, C, n), lambda s: (s, 0, 0))], [jax.ShapeDtypeStruct((LANES, C, n), BF16)],
        [pltpu.VMEM((C, RB, n), BF16), pltpu.VMEM((RB, C, n), BF16)],
        GIGA, 20 * MIB)
    return fn(x0, zp, zo, wt, gain, lbias, wot, lnmid, perm)[0]


def post_bwd_kernel(second, blk, ids, x, zp, zo, dzp, dzo, wt, gain, lbias, wot, wo, lnmid, perm, *rest):
    if second:
        znew, dx, dpg, acc_bg, acc_bo, acc_wo, acc_mg, acc_mb = rest[:8]
    else:
        dx, dxk, dxs, dpg, acc_bg, acc_bo, acc_wo, acc_mg, acc_mb = rest[:9]
    xh_s, xi_s, dxi_s, dub_s, dxc_s, xn_s, r_s = rest[-7:]
    step = pl.program_id(0)

    @pl.when(step == 0)
    def _():
        for acc in (acc_bg, acc_bo, acc_wo, acc_mg, acc_mb):
            acc[:] = jnp.zeros_like(acc)

    mid_norm(x, xh_s, lnmid, blk, xn_s, r_s)
    to_rows(perm[:], xh_s, xi_s)

    sums = [acc_bg[:], acc_bo[:], acc_wo[:]]

    def gates(i):
        if second:
            zf = zp[i].astype(F32)
            dz = jnp.where(step < 4, dzp[i], dzo[i]).astype(F32)
        else:
            zf = jnp.where(step < 4, zp[i], zo[i]).astype(F32)
            dz = dzp[i].astype(F32)
        t = gate_of(zf, wt, gain, lbias)
        upd = dot_nn(wot[:], with_ones(xi_s[i]))
        t1 = 1.0 + t
        if second:
            znew[i] = (zf + t1 * upd).astype(BF16)
        d_upd = (HALF * dz) * t1
        d_pg = d_upd * (upd * (1.0 - t))
        dpg[i] = d_pg.astype(BF16)
        dub_s[i] = d_upd.astype(BF16)
        sums[0] += fold(d_pg)
        sums[1] += fold(d_upd)

    def products(i):
        dxi_s[i] = dot_nn(wo[:], dub_s[i]).astype(BF16)
        sums[2] += dot_nt(dub_s[i], xi_s[i])

    staggered(gates, products)
    acc_bg[:], acc_bo[:], acc_wo[:] = sums

    def put(grp, v):
        dxc_s[grp * RB:(grp + 1) * RB] = v

    to_cmajor(perm[:], dxi_s, put)
    m1 = m2 = None
    for c in range(C):
        dy = dxc_s[c]
        dyx = dy * xn_s[c]
        gn = lnmid[blk, 0, c]
        m1 = dy * gn if m1 is None else m1 + dy * gn
        m2 = dyx * gn if m2 is None else m2 + dyx * gn
        acc_mg[c] += fold(dyx[0:8] + dyx[8:RB])
        acc_mb[c] += fold(dy[0:8] + dy[8:RB])
    m1 = m1 * (1.0 / C)
    m2 = m2 * (1.0 / C)
    rstd = r_s[:]
    for c in range(C):
        v = (rstd * (dxc_s[c] * lnmid[blk, 0, c] - m1 - xn_s[c] * m2))
        dx[c] = v.astype(BF16)
        if not second:
            mine, other = split_cols(v, ids[1])
            dxk[c] = mine.astype(BF16)
            dxs[c] = other.astype(BF16)


def post_backward(ids, second, x, z_parts, dz_parts, par, w_out, lnmid, blk):
    n = x.shape[-1]
    cspec = pl.BlockSpec((C, RB, n), lambda s: (0, s, 0))
    hspec = pl.BlockSpec((C, RB, LANES), lambda s: (0, s, 0))
    rspec = pl.BlockSpec((RB, C, n), lambda s: (s, 0, 0))
    two = [pl.BlockSpec((RB, C, n), peer_map), pl.BlockSpec((RB, C, n), own_map)]
    one = [rspec, SMEM_SPEC]
    zspec, dzspec = (one, two) if second else (two, one)
    z_args = (z_parts[0], ids) if second else z_parts
    dz_args = dz_parts if second else (dz_parts[0], ids)
    acc_shapes = [(C, LANES), (C, LANES), (C, C), (C, 8, LANES), (C, 8, LANES)]
    accs = [jax.ShapeDtypeStruct(s, F32) for s in acc_shapes]
    acc_specs = [full_spec(s) for s in acc_shapes]
    c_out = jax.ShapeDtypeStruct((C, LANES, n), BF16)
    h_out = jax.ShapeDtypeStruct((C, LANES, LANES), BF16)
    r_out = jax.ShapeDtypeStruct((LANES, C, n), BF16)
    if second:
        outs = [jax.ShapeDtypeStruct((C, C, n), BF16), c_out, r_out]
        ospecs = [pl.BlockSpec((RB, C, n), own_map), cspec, rspec]
    else:
        outs = [c_out, h_out, h_out, r_out]
        ospecs = [cspec, hspec, hspec, rspec]
    wt, wot, gain, lbias, perm = par
    fn = call(
        functools.partial(post_bwd_kernel, second, blk), (8,),
        [SMEM_SPEC, cspec] + zspec + dzspec + [blk_spec(wt.shape, blk), blk_spec(gain.shape, blk), blk_spec(gain.shape, blk), blk_spec(wot.shape, blk), blk_spec(w_out.shape, blk), SMEM_SPEC, full_spec((W2, W2))],
        ospecs + acc_specs, outs + accs,
        [pltpu.VMEM((C, RB, n), BF16), pltpu.VMEM((RB, C, n), BF16), pltpu.VMEM((RB, C, n), BF16), pltpu.VMEM((RB, C, n), BF16), pltpu.VMEM((C, RB, n), F32), pltpu.VMEM((C, RB, n), F32), pltpu.VMEM((RB, n), F32)],
        GIGA, 30 * MIB)
    return fn(ids, x, *z_args, *dz_args, wt, gain, lbias, wot, w_out, lnmid, perm)


def pre_bwd_kernel(two, z, da, db, dpg, drp, dro, mp, mo, wt, w, gain, lbias, perm, dz, acc_w, acc_b, acc_g, acc_lb, dai_s, dbi_s, dp_s, zh_s, zn_s, rs_s):
    step = pl.program_id(0)

    @pl.when(step == 0)
    def _():
        for acc in (acc_w, acc_b, acc_g, acc_lb):
            acc[:] = jnp.zeros_like(acc)

    to_rows(perm[:], da, dai_s)
    to_rows(perm[:], db, dbi_s)

    sums = [acc_w[:], acc_g[:], acc_lb[:]]

    def gates(i):
        zn, rstd = norm_rows(z[i].astype(F32))
        zn_s[i] = zn
        rs_s[i] = jnp.broadcast_to(rstd, (8, rstd.shape[-1]))
        zh = (zn * gain[:] + lbias[:]).astype(BF16)
        zh_s[i] = zh
        p = dot_nn(wt[0:4 * C], with_ones(zh))
        m = mp[pl.ds(i, 1), :]
        if two:
            m = jnp.where(step < 4, m, mo[pl.ds(i, 1), :])
        m = HALF * m.astype(F32)
        for side, ref in ((0, dai_s), (1, dbi_s)):
            base = side * 2 * C
            dm = ref[i].astype(F32) * m
            t = jnp.tanh(p[base:base + C])
            dv = dm * (1.0 + t)
            dg = dv * (p[base + C:base + 2 * C] * (1.0 - t))
            for k, d in ((2 * side, dg), (2 * side + 1, dv)):
                acc_b[k * C:(k + 1) * C] += fold(d)
                dp_s[i, k * C:(k + 1) * C] = d.astype(BF16)
        dp_s[i, 4 * C:5 * C] = dpg[i]

    def products(i):
        dp = dp_s[i]
        dzh = dot_nn(w[:], dp).astype(BF16).astype(F32)
        sums[0] += dot_nt(dp, zh_s[i])
        zn, rstd = zn_s[i], rs_s[i, 0:1, :]
        sums[1] += fold(dzh * zn)
        sums[2] += fold(dzh)
        dzn = dzh * gain[:]
        m1 = jnp.mean(dzn, axis=0, keepdims=True)
        m2 = jnp.mean(dzn * zn, axis=0, keepdims=True)
        dzf = rstd * (dzn - m1 - zn * m2)
        if two:
            dr = jnp.where(step < 4, drp[i], dro[i]).astype(F32)
        else:
            dr = drp[i].astype(F32)
        dz[i] = (dr + dzf).astype(BF16)

    staggered(gates, products)
    acc_w[:], acc_g[:], acc_lb[:] = sums


def pre_backward(ids, z, da, db, dpg, dres_parts, masks, par, w_proj, blk, own_only):
    n = z.shape[-1]
    steps = da.shape[1] // RB
    off = 4 if own_only else 0
    two = len(dres_parts) == 2
    cspec = pl.BlockSpec((C, RB, n), lambda s: (0, s, 0))
    rspec = pl.BlockSpec((RB, C, n), lambda s: (s, 0, 0))
    hspec = pl.BlockSpec((RB, C, n), lambda s: (s + off, 0, 0))
    if two:
        drspec = [pl.BlockSpec((RB, C, n), peer_map), pl.BlockSpec((RB, C, n), own_map)]
        mspec = [pl.BlockSpec((RB, n), peer_map2), pl.BlockSpec((RB, n), own_map2)]
        dr_args, m_args = dres_parts, masks
    else:
        drspec = [hspec, SMEM_SPEC]
        mspec = [pl.BlockSpec((RB, n), lambda s: (s, 0)), SMEM_SPEC]
        dr_args, m_args = (dres_parts[0], ids), (masks[0], ids)
    acc_shapes = [(5 * C, C), (4 * C, LANES), (C, LANES), (C, LANES)]
    wt, _, gain, lbias, perm = par
    fn = call(
        functools.partial(pre_bwd_kernel, two), (steps,),
        [rspec, cspec, cspec, hspec] + drspec + mspec + [blk_spec(wt.shape, blk), blk_spec(w_proj.shape, blk), blk_spec(gain.shape, blk), blk_spec(gain.shape, blk), full_spec((W2, W2))],
        [rspec] + [full_spec(s) for s in acc_shapes],
        [jax.ShapeDtypeStruct((steps * RB, C, n), BF16)] + [jax.ShapeDtypeStruct(s, F32) for s in acc_shapes],
        [pltpu.VMEM((RB, C, n), BF16), pltpu.VMEM((RB, C, n), BF16), pltpu.VMEM((RB, 5 * C, n), BF16), pltpu.VMEM((RB, C, n), BF16), pltpu.VMEM((RB, C, n), F32), pltpu.VMEM((RB, 8, n), F32)],
        GIGA * steps // 8, 30 * MIB * steps // 8)
    return fn(z, da, db, dpg, *dr_args, *m_args, wt, w_proj, gain, lbias, perm)


PACK = 512


def grads_kernel(n_dp, n_dap, w0, b0, q0, g0, l0, wo0, o0, mg0, mb0, w1, b1, q1, g1, l1, wo1, o1, mg1, mb1, out, buf, recv_a, red, recv_b, gath, vec, send_a, rcv_a, send_b, rcv_b, send_c, rcv_c, send_d, rcv_d):
    dp, dap = lax.axis_index("dp"), lax.axis_index("dap")
    big, small = PACK // n_dap, PACK // n_dap // n_dp
    bar = pltpu.get_barrier_semaphore()
    for k in range(1, n_dap):
        pl.semaphore_signal(bar, inc=1, device_id=(dp, lax.rem(dap + k, n_dap)), device_id_type=MESH_ID)
    for k in range(1, n_dp):
        pl.semaphore_signal(bar, inc=1, device_id=(lax.rem(dp + k, n_dp), dap), device_id_type=MESH_ID)

    buf[0:5 * C, 0:C] = w0[:]
    buf[0:5 * C, C:2 * C] = HALF * w1[:]
    buf[5 * C:6 * C, 0:C] = HALF * wo0[:]
    buf[5 * C:6 * C, C:2 * C] = HALF * wo1[:]

    def put(k, base, ref, scale):
        v = ref[:]
        if v.ndim == 3:
            v = jnp.sum(v, axis=1)
        rows = v.shape[0]
        tot = scale * jnp.sum(v, axis=1, keepdims=True)
        lane = lax.broadcasted_iota(jnp.int32, (rows, LANES), 1)
        vec[base:base + rows, :] = jnp.where(lane == k, tot, vec[base:base + rows, :])

    vec[:] = jnp.zeros_like(vec)
    put(0, 0, b0, 1.0)
    put(0, 4 * C, q0, HALF)
    put(1, 0, b1, HALF)
    put(1, 4 * C, q1, HALF)
    for k, (ref, scale) in enumerate(((g0, 1.0), (l0, 1.0), (g1, HALF), (l1, HALF), (mg0, HALF), (mb0, HALF), (mg1, HALF), (mb1, HALF), (o0, HALF), (o1, HALF))):
        put(2 + k, 0, ref, scale)
    vt = jnp.transpose(vec[:])
    for t in range(3):
        buf[6 * C + RB * t:6 * C + RB * t + RB, :] = vt[0:RB, LANES * t:LANES * (t + 1)]
    buf[6 * C + 48:PACK, :] = jnp.zeros((PACK - 6 * C - 48, LANES), F32)

    pl.semaphore_wait(bar, n_dap + n_dp - 2)

    def copies(count, make):
        made = [make(k) for k in range(1, count)]
        for cp in made:
            cp.start()
        return made

    def to_dap(k):
        return (dp, lax.rem(dap + k, n_dap))

    def to_dp(k):
        return (lax.rem(dp + k, n_dp), dap)

    def rows_of(idx, size):
        return pl.ds(pl.multiple_of(idx * size, size), size)

    stage = copies(n_dap, lambda k: pltpu.make_async_remote_copy(buf.at[rows_of(lax.rem(dap + k, n_dap), big)], recv_a.at[k - 1], send_a.at[k - 1], rcv_a.at[k - 1], device_id=to_dap(k), device_id_type=MESH_ID))
    tot = buf[rows_of(dap, big), :]
    for k, cp in enumerate(stage):
        cp.wait_recv()
        tot = tot + recv_a[k]
    red[:] = tot
    for cp in stage:
        cp.wait_send()

    stage = copies(n_dp, lambda k: pltpu.make_async_remote_copy(red.at[rows_of(lax.rem(dp + k, n_dp), small)], recv_b.at[k - 1], send_b.at[k - 1], rcv_b.at[k - 1], device_id=to_dp(k), device_id_type=MESH_ID))
    tot = red[rows_of(dp, small), :]
    for k, cp in enumerate(stage):
        cp.wait_recv()
        tot = tot + recv_b[k]
    gath[rows_of(dp, small), :] = tot
    for cp in stage:
        cp.wait_send()

    mine = gath.at[rows_of(dp, small)]
    stage = copies(n_dp, lambda k: pltpu.make_async_remote_copy(mine, mine, send_c.at[k - 1], rcv_c.at[k - 1], device_id=to_dp(k), device_id_type=MESH_ID))
    for cp in stage:
        cp.wait()

    stage = copies(n_dap, lambda k: pltpu.make_async_remote_copy(gath, out.at[rows_of(dap, big)], send_d.at[k - 1], rcv_d.at[k - 1], device_id=to_dap(k), device_id_type=MESH_ID))
    out[rows_of(dap, big), :] = gath[:]
    for cp in stage:
        cp.wait()


def sum_grads(n_dp, n_dap, parts):
    big, small = PACK // n_dap, PACK // n_dap // n_dp
    dma = pltpu.SemaphoreType.DMA
    return pl.pallas_call(
        functools.partial(grads_kernel, n_dp, n_dap),
        out_shape=jax.ShapeDtypeStruct((PACK, LANES), F32),
        in_specs=[pl.BlockSpec(memory_space=pltpu.VMEM)] * len(parts),
        out_specs=pl.BlockSpec(memory_space=pltpu.VMEM),
        scratch_shapes=[pltpu.VMEM((PACK, LANES), F32), pltpu.VMEM((n_dap - 1, big, LANES), F32), pltpu.VMEM((big, LANES), F32), pltpu.VMEM((max(n_dp - 1, 1), small, LANES), F32), pltpu.VMEM((big, LANES), F32), pltpu.VMEM((384, LANES), F32)]
        + [dma((n_dap - 1,))] * 2 + [dma((max(n_dp - 1, 1),))] * 4 + [dma((n_dap - 1,))] * 2,
        name="grad_sum",
        cost_estimate=pl.CostEstimate(flops=MEGA, bytes_accessed=MIB, transcendentals=0),
        compiler_params=pltpu.CompilerParams(collective_id=0, has_side_effects=True),
    )(*parts)


def unpack_kernel(src, ln_in, gw, bp, lm, gwo, bo):
    t = jnp.transpose(src[0:6 * C, :])
    for k in range(2):
        gw[k] = t[k * C:(k + 1) * C, 0:5 * C]
        gwo[k] = t[k * C:(k + 1) * C, 5 * C:6 * C]
    base = 6 * C
    bp[:, 0:LANES] = src[base:base + 2, :]
    bp[:, LANES:W2] = src[base + RB:base + 18, :]
    bp[:, W2:320] = src[base + 32:base + 34, 0:C]
    for k in range(2):
        ln_in[k] = src[base + 2 + 2 * k:base + 4 + 2 * k, 0:C]
        lm[k] = src[base + 6 + 2 * k:base + 8 + 2 * k, 0:C]
    bo[:] = src[base + 10:base + 12, 0:C]


def unpack(flat):
    outs = [jax.ShapeDtypeStruct(s, F32) for s in ((2, 2, C), (2, C, 5 * C), (2, 5 * C), (2, 2, C), (2, C, C), (2, C))]
    return call(unpack_kernel, (1,), [full_spec(flat.shape)], [full_spec(o.shape) for o in outs], outs, [], MEGA, MIB)(flat)


SUM = sum_grads


def solution(mesh):
    def plan(z_pair, pair_mask, dz_out, ln_in, w_proj, b_proj, ln_mid, w_out, b_out):
        n = z_pair.shape[2]
        dap = lax.axis_index("dap")
        ids = jnp.stack([dap // 2, dap % 2]).astype(jnp.int32)
        x_pairs = [(0, 2), (2, 0), (1, 3), (3, 1)]
        c_pairs = [(0, 1), (1, 0), (2, 3), (3, 2)]

        def over_x(v):
            return lax.ppermute(v, "dap", x_pairs)

        def over_c(v):
            return lax.ppermute(v, "dap", c_pairs)

        par = prepare(n, ln_in, w_proj, b_proj, w_out, b_out)
        lnmid = ln_mid.astype(F32)
        m_own = pair_mask[0]
        z_own = jnp.transpose(z_pair[0], (0, 2, 1))
        dz_own = jnp.transpose(dz_out[0], (0, 2, 1))
        m_peer = over_x(m_own)
        z_peer = over_x(z_own)
        z_peer, dz_src = lax.optimization_barrier((z_peer, dz_own))
        dz_peer = over_x(dz_src)
        masks = (m_peer, m_own)

        sds = jax.ShapeDtypeStruct
        full = pltpu.VMEM((2, n, n), BF16)
        ao, bo = pre_forward(ids, z_own, (m_own,), par, 0)
        qo, ro = over_c(bo), over_c(ao)
        ap, bp = pre_forward(ids, z_peer, (m_peer,), par, 0)
        qp, rp = over_c(bp), over_c(ap)
        (x0,) = tri_call(tri_out_kernel, ids, (ap, ao, bp, bo, qp, qo), [sds((C, LANES, n), F32)], [full], GIGA)
        z_mid = post_forward(x0, z_peer, z_own, par, lnmid, 0)
        a1, b1, a1k, a1s = pre_forward(ids, z_mid, masks, par, 1)
        a1r = over_c(a1s)
        b1p = over_c(b1)
        (x1,) = tri_call(tri_in_kernel, ids, (a1k, a1r, b1, b1p), [sds((C, LANES, n), F32)], [], GIGA)
        z_new, dx1, dpg1, bg1, bo1, wo1, mg1, mb1 = post_backward(ids, True, x1, (z_mid,), (dz_peer, dz_own), par, w_out, lnmid, 1)
        dx1p = over_c(dx1)
        da1, db1 = tri_call(tri_in_bwd_kernel, ids, (a1, b1, dx1, dx1p), [sds((C, LANES, n), BF16)] * 2, [full], GIGA)
        dz_mid, w1, b1s, g1, lb1 = pre_backward(ids, z_mid, da1, db1, dpg1, (dz_peer, dz_own), masks, par, w_proj, 1, False)
        dx0, dx0k, dx0s, dpg0, bg0, bo0, wo0, mg0, mb0 = post_backward(ids, False, x0, (z_peer, z_own), (dz_mid,), par, w_out, lnmid, 0)
        dx0r = over_c(dx0s)
        da0, db0 = tri_call(tri_out_bwd_kernel, ids, (dx0, bp, bo, qp, qo, dx0k, dx0r, ap, ao, rp, ro), [sds((C, C, n), BF16)] * 2, [full, pltpu.VMEM((2, LANES, n), F32)], GIGA, own_first=True)
        dz, w0, b0s, g0, lb0 = pre_backward(ids, z_own, da0, db0, dpg0, (dz_mid,), (m_own,), par, w_proj, 0, True)

        flat = SUM(mesh.shape["dp"], mesh.shape["dap"], (w0, b0s, bg0, g0, lb0, wo0, bo0, mg0, mb0, w1, b1s, bg1, g1, lb1, wo1, bo1, mg1, mb1))
        g_ln_in, gw, g_bp, g_lm, gwo, g_bo = unpack(flat)
        z_res = jnp.transpose(z_new, (0, 2, 1))[None]
        dz_res = jnp.transpose(dz, (0, 2, 1))[None]
        return z_res, dz_res, g_ln_in, gw, g_bp, g_lm, gwo, g_bo

    row_spec = P("dp", "dap")
    return jax.shard_map(plan, mesh=mesh, in_specs=(row_spec, row_spec, row_spec, P(), P(), P(), P(), P(), P()), out_specs=(row_spec, row_spec, P(), P(), P(), P(), P(), P()), check_vma=False)
```

```python
import functools

import jax
import jax.numpy as jnp
from jax import lax
from jax.experimental import pallas as pl
from jax.experimental.pallas import tpu as pltpu
from jax.sharding import PartitionSpec as P


EPS = 1e-5
F32 = jnp.float32
BF16 = jnp.bfloat16
INTERPRET = False
C = 64
RB = 16
DELAY = 4
LANES = 128
W2 = 256
HALF = 0.5
MEGA = 10 ** 6
GIGA = 10 ** 9
MIB = 2 ** 20
VMEM_LIMIT = 56 * 1024 * 1024


MESH_ID = pl.DeviceIdType.MESH


def dot_nn(a, b):
    return lax.dot_general(a, b, (((1,), (0,)), ((), ())), preferred_element_type=F32)


def dot_nt(a, b):
    return lax.dot_general(a, b, (((1,), (1,)), ((), ())), preferred_element_type=F32)


def dot_tn(a, b):
    return lax.dot_general(a, b, (((0,), (0,)), ((), ())), preferred_element_type=F32)


def norm_rows(zf):
    mean = jnp.mean(zf, axis=0, keepdims=True)
    cen = zf - mean
    var = jnp.mean(cen * cen, axis=0, keepdims=True)
    rstd = lax.rsqrt(var + EPS)
    return cen * rstd, rstd


def staggered(first, second):
    for i in range(RB + DELAY):
        if i < RB:
            first(i)
        if i >= DELAY:
            second(i - DELAY)


def fold(v):
    return v[:, :LANES] + v[:, LANES:]


def to_cmajor(perm, src, dst):
    n = src.shape[-1]
    for grp in range(C // RB):
        blk = src[:, grp * RB:(grp + 1) * RB, :].reshape(W2, n)
        out = dot_nn(perm, blk)
        dst(grp, out.reshape(RB, RB, n))


def to_rows(perm, src, dst):
    n = src.shape[-1]
    for grp in range(C // RB):
        blk = src[grp * RB:(grp + 1) * RB, :, :].reshape(W2, n)
        out = dot_nn(perm, blk)
        dst[:, grp * RB:(grp + 1) * RB, :] = out.reshape(RB, RB, n).astype(BF16)


def split_cols(v, core):
    lo, hi = v[..., :LANES], v[..., LANES:]
    lane = lax.broadcasted_iota(jnp.int32, lo.shape, lo.ndim - 1)
    axis = lo.ndim - 1
    first = jnp.where(lane < C, lo, pltpu.roll(hi, C, axis))
    second = jnp.where(lane < C, pltpu.roll(lo, C, axis), hi)
    mine = jnp.where(core == 0, first, second)
    other = jnp.where(core == 0, second, first)
    return mine, other


KA = C + RB


def prep_kernel(w_proj, b_proj, ln_in, w_out, b_out, wt_aug, wot_aug, gain, lbias, perm, scr):
    n = gain.shape[-1]
    for k in range(2):
        scr[:] = jnp.zeros_like(scr)
        scr[0:C, 0:5 * C] = w_proj[k].astype(F32)
        scr[C:C + 1, 0:5 * C] = b_proj[pl.ds(k, 1), :]
        wt_aug[k] = (HALF * jnp.transpose(scr[:]))[0:5 * C, 0:KA].astype(BF16)
        scr[:] = jnp.zeros_like(scr)
        scr[0:C, 0:C] = w_out[k].astype(F32)
        scr[C:C + 1, 0:C] = b_out[pl.ds(k, 1), :]
        scr[C + 8:C + 10, 0:C] = ln_in[k]
        small = jnp.transpose(scr[:, 0:LANES])
        wot_aug[k] = (HALF * small)[0:C, 0:KA].astype(BF16)
        gain[k] = jnp.broadcast_to(small[0:C, C + 8:C + 9], (C, n))
        lbias[k] = jnp.broadcast_to(small[0:C, C + 9:C + 10], (C, n))
    r = lax.broadcasted_iota(jnp.int32, (W2, W2), 0)
    q = lax.broadcasted_iota(jnp.int32, (W2, W2), 1)
    perm[:] = jnp.where(q == RB * (r % RB) + r // RB, 1.0, 0.0).astype(BF16)


def prepare(n, ln_in, w_proj, b_proj, w_out, b_out):
    sds = jax.ShapeDtypeStruct
    outs = [sds((2, 5 * C, KA), BF16), sds((2, C, KA), BF16), sds((2, C, n), F32), sds((2, C, n), F32), sds((W2, W2), BF16)]
    args = (w_proj, b_proj.astype(F32), ln_in.astype(F32), w_out, b_out.astype(F32))
    return call(prep_kernel, (1,), [full_spec(v.shape) for v in args], [full_spec(o.shape) for o in outs], outs, [pltpu.VMEM((LANES, 384), F32)], MEGA, MIB)(*args)


def with_ones(zh):
    row = lax.broadcasted_iota(jnp.int32, (RB, zh.shape[-1]), 0)
    return jnp.concatenate([zh, jnp.where(row == 0, 1.0, 0.0).astype(BF16)], axis=0)


def pre_fwd_kernel(z, mask, wt, gain, lbias, perm, a, b, a_s, b_s):
    for i in range(RB):
        a_s[i], b_s[i] = project(z[i].astype(F32), mask[pl.ds(i, 1), :].astype(F32), wt, gain, lbias)

    def put_a(grp, v):
        a[grp * RB:(grp + 1) * RB] = v.astype(BF16)

    def put_b(grp, v):
        b[grp * RB:(grp + 1) * RB] = v.astype(BF16)

    to_cmajor(perm[:], a_s, put_a)
    to_cmajor(perm[:], b_s, put_b)


def full_spec(shape):
    return pl.BlockSpec(shape, lambda s: (0,) * len(shape))


SMEM_SPEC = pl.BlockSpec(memory_space=pltpu.SMEM)


def call(kernel, grid, in_specs, out_specs, out_shape, scratch, flops, bytes_accessed, trans=0):
    return pl.pallas_call(
        kernel,
        grid=grid,
        in_specs=in_specs,
        out_specs=out_specs,
        out_shape=out_shape,
        scratch_shapes=scratch,
        interpret=INTERPRET,
        cost_estimate=pl.CostEstimate(flops=flops, bytes_accessed=bytes_accessed, transcendentals=trans),
        compiler_params=pltpu.CompilerParams(dimension_semantics=("arbitrary",) * len(grid), vmem_limit_bytes=VMEM_LIMIT),
    )


def blk_spec(shape, k):
    return pl.BlockSpec((None,) + tuple(shape[1:]), lambda s: (k,) + (0,) * (len(shape) - 1))


def pre_forward(z, mask, par):
    rows, _, n = z.shape
    specs, args = weights_specs(par, 0, False)
    cspec = pl.BlockSpec((C, RB, n), lambda s: (0, s, 0))
    return call(
        pre_fwd_kernel, (rows // RB,),
        [pl.BlockSpec((RB, C, n), lambda s: (s, 0, 0)), pl.BlockSpec((RB, n), lambda s: (s, 0))] + specs + [full_spec((W2, W2))],
        [cspec] * 2, [jax.ShapeDtypeStruct((C, rows, n), BF16)] * 2, [pltpu.VMEM((RB, C, n), BF16)] * 2, GIGA, 8 * MIB)(z, mask, *args, par[-1])


CB = 8
T_STEPS = C // CB


def global_rows(ids, partner):
    x, c = ids[0], ids[1]
    cc = 1 - c if partner else c
    return pl.multiple_of(C * (2 * (1 - x) + cc), C), pl.multiple_of(C * (2 * x + cc), C)


def place(dst, src_mine, src_other, ids):
    for (peer, own), partner in ((src_mine, False), (src_other, True)):
        off_peer, off_own = global_rows(ids, partner)
        dst[pl.ds(off_peer, C), :] = peer
        dst[pl.ds(off_own, C), :] = own


def halves(ref):
    return ref[0:C, :], ref[C:LANES, :]


def tri_spec(shape, row_blk=0):
    return pl.BlockSpec((CB,) + tuple(shape[1:]), lambda s: (jnp.minimum(s, T_STEPS - 1), row_blk, 0))


def row_blk(s):
    return jnp.maximum(s - T_STEPS, 0)


def r_spec(n, off=0):
    return pl.BlockSpec((RB, C, n), lambda s: (row_blk(s) + off, 0, 0))


def c_spec(n):
    return pl.BlockSpec((C, RB, n), lambda s: (0, row_blk(s), 0))


def two_specs(shape):
    zeros = (0,) * (len(shape) - 1)
    return [pl.BlockSpec(shape, lambda s: (jnp.clip(s - T_STEPS, 0, 3),) + zeros), pl.BlockSpec(shape, lambda s: (jnp.maximum(s - T_STEPS - 4, 0),) + zeros)]


def m_spec(n):
    return pl.BlockSpec((RB, n), lambda s: (row_blk(s), 0))


def pick(r, peer, own):
    return jnp.where(r < 4, peer, own)


def channels(step):
    return [(ch, step * CB + ch) for ch in range(CB)]


def mid_norm(x, xh_s, lnmid, blk, xn_s, rstd_s):
    tot = x[0]
    for c in range(1, C):
        tot = tot + x[c]
    mean = tot * (1.0 / C)
    d = x[0] - mean
    sq = d * d
    for c in range(1, C):
        d = x[c] - mean
        sq = sq + d * d
    rstd = lax.rsqrt(sq * (1.0 / C) + EPS)
    rstd_s[:] = rstd
    for c in range(C):
        xn = (x[c] - mean) * rstd
        xn_s[c] = xn
        xh_s[c] = (xn * lnmid[blk, 0, c] + lnmid[blk, 1, c]).astype(BF16)


def gate_of(zf, wt, gain, lbias):
    zn, _ = norm_rows(zf)
    zh = (zn * gain[:] + lbias[:]).astype(BF16)
    return jnp.tanh(dot_nn(wt[4 * C:5 * C], with_ones(zh)))


def project(zf, m, wt, gain, lbias):
    zn, _ = norm_rows(zf)
    zh = (zn * gain[:] + lbias[:]).astype(BF16)
    p = dot_nn(wt[0:4 * C], with_ones(zh))
    a = ((1.0 + jnp.tanh(p[0:C])) * (p[C:2 * C] * m)).astype(BF16)
    b = ((1.0 + jnp.tanh(p[2 * C:3 * C])) * (p[3 * C:4 * C] * m)).astype(BF16)
    return a, b


def fwd_kernel(ids, ap, ao, bp, bo, qp, qo, zp, zo, mp, mo, wt0, gain0, lbias0, wot0, wt1, gain1, lbias1, lnmid, perm, zmid, xn, rstd, a1, b1, a1k, a1s, x_s, full, xh_s, xi_s, a_s, b_s):
    step = pl.program_id(0)

    @pl.when(step < T_STEPS)
    def _():
        for ch, dst in channels(step):
            buf = full.at[ch % 2]
            place(buf, (bp[ch], bo[ch]), (qp[ch], qo[ch]), ids)
            x_s[dst] = dot_nt(jnp.concatenate([ap[ch], ao[ch]], axis=0), buf[:])

    @pl.when(step >= T_STEPS)
    def _():
        r = step - T_STEPS
        mid_norm(x_s.at[:, pl.ds(pl.multiple_of(r * RB, RB), RB), :], xh_s, lnmid, 0, xn, rstd)
        to_rows(perm[:], xh_s, xi_s)

        def update(i):
            zf = pick(r, zp[i], zo[i]).astype(F32)
            upd = dot_nn(wot0[:], with_ones(xi_s[i]))
            zmid[i] = (zf + (1.0 + gate_of(zf, wt0, gain0, lbias0)) * upd).astype(BF16)

        def sides(i):
            m = pick(r, mp[pl.ds(i, 1), :], mo[pl.ds(i, 1), :]).astype(F32)
            a_s[i], b_s[i] = project(zmid[i].astype(F32), m, wt1, gain1, lbias1)

        staggered(update, sides)

        def put_a(grp, v):
            a1[grp * RB:(grp + 1) * RB] = v.astype(BF16)
            mine, other = split_cols(v, ids[1])
            a1k[grp * RB:(grp + 1) * RB] = mine.astype(BF16)
            a1s[grp * RB:(grp + 1) * RB] = other.astype(BF16)

        def put_b(grp, v):
            b1[grp * RB:(grp + 1) * RB] = v.astype(BF16)

        to_cmajor(perm[:], a_s, put_a)
        to_cmajor(perm[:], b_s, put_b)


def weights_specs(par, blk, with_out):
    wt, wot, gain, lbias, _ = par
    specs = [blk_spec(wt.shape, blk), blk_spec(gain.shape, blk), blk_spec(gain.shape, blk)]
    args = [wt, gain, lbias]
    if with_out:
        specs.append(blk_spec(wot.shape, blk))
        args.append(wot)
    return specs, args


def fwd_fused(ids, sides, zp, zo, masks, par, lnmid):
    n = zp.shape[-1]
    s0, w0 = weights_specs(par, 0, True)
    s1, w1 = weights_specs(par, 1, False)
    sds, vm = jax.ShapeDtypeStruct, pltpu.VMEM
    c_out, h_out = sds((C, LANES, n), BF16), sds((C, LANES, LANES), BF16)
    return call(
        fwd_kernel, (T_STEPS + 8,),
        [SMEM_SPEC] + [tri_spec(v.shape) for v in sides] + two_specs((RB, C, n)) + two_specs((RB, n)) + s0 + s1 + [SMEM_SPEC, full_spec((W2, W2))],
        [r_spec(n), c_spec(n), m_spec(n), c_spec(n), c_spec(n), c_spec(LANES), c_spec(LANES)],
        [sds((LANES, C, n), BF16), sds((C, LANES, n), F32), sds((LANES, n), F32), c_out, c_out, h_out, h_out],
        [vm((C, LANES, n), F32), vm((2, n, n), BF16), vm((C, RB, n), BF16), vm((RB, C, n), BF16), vm((RB, C, n), BF16), vm((RB, C, n), BF16)],
        GIGA, 40 * MIB)(ids, *sides, zp, zo, *masks, *w0, *w1, lnmid, par[-1])


def mid_back(dxc_s, xn, rstd, lnmid, blk, acc_mg, acc_mb, emit):
    m1 = m2 = None
    for c in range(C):
        dy = dxc_s[c]
        dyx = dy * xn[c]
        gn = lnmid[blk, 0, c]
        m1 = dy * gn if m1 is None else m1 + dy * gn
        m2 = dyx * gn if m2 is None else m2 + dyx * gn
        acc_mg[c] += fold(dyx[0:8] + dyx[8:RB])
        acc_mb[c] += fold(dy[0:8] + dy[8:RB])
    m1 = m1 * (1.0 / C)
    m2 = m2 * (1.0 / C)
    for c in range(C):
        emit(c, rstd * (dxc_s[c] * lnmid[blk, 0, c] - m1 - xn[c] * m2))


def clear(step, accs):
    @pl.when(step == 0)
    def _():
        for acc in accs:
            acc[:] = jnp.zeros_like(acc)


def turn_kernel(ids, ak, ar, b, bq, z, dzp, dzo, wt, gain, lbias, wot, wo, lnmid, perm, znew, dx, dpg, acc_bg, acc_bo, acc_wo, acc_mg, acc_mb, x_s, xh_s, xi_s, dxi_s, dub_s, dxc_s, xn_s, r_s):
    step = pl.program_id(0)
    xx = ids[0]
    clear(step, (acc_bg, acc_bo, acc_wo, acc_mg, acc_mb))

    @pl.when(step < T_STEPS)
    def _():
        for ch, dst in channels(step):
            out = dot_tn(ak[ch], b[ch]) + dot_tn(ar[ch], bq[ch])
            x_s[dst, pl.ds(pl.multiple_of(C * (1 - xx), C), C), :] = out[0:C]
            x_s[dst, pl.ds(pl.multiple_of(C * xx, C), C), :] = out[C:LANES]

    @pl.when(step >= T_STEPS)
    def _():
        r = step - T_STEPS
        mid_norm(x_s.at[:, pl.ds(pl.multiple_of(r * RB, RB), RB), :], xh_s, lnmid, 1, xn_s, r_s)
        to_rows(perm[:], xh_s, xi_s)
        sums = [acc_bg[:], acc_bo[:], acc_wo[:]]

        def gates(i):
            zf = z[i].astype(F32)
            dz = pick(r, dzp[i], dzo[i]).astype(F32)
            t = gate_of(zf, wt, gain, lbias)
            upd = dot_nn(wot[:], with_ones(xi_s[i]))
            t1 = 1.0 + t
            znew[i] = (zf + t1 * upd).astype(BF16)
            d_upd = (HALF * dz) * t1
            d_pg = d_upd * (upd * (1.0 - t))
            dpg[i] = d_pg.astype(BF16)
            dub_s[i] = d_upd.astype(BF16)
            sums[0] += fold(d_pg)
            sums[1] += fold(d_upd)

        def products(i):
            dxi_s[i] = dot_nn(wo[:], dub_s[i]).astype(BF16)
            sums[2] += dot_nt(dub_s[i], xi_s[i])

        staggered(gates, products)
        acc_bg[:], acc_bo[:], acc_wo[:] = sums

        def put(grp, v):
            dxc_s[grp * RB:(grp + 1) * RB] = v

        to_cmajor(perm[:], dxi_s, put)

        def emit(c, v):
            dx[c] = v.astype(BF16)

        mid_back(dxc_s, xn_s, r_s[:], lnmid, 1, acc_mg, acc_mb, emit)


ACC_POST = ((C, LANES), (C, LANES), (C, C), (C, 8, LANES), (C, 8, LANES))
ACC_PRE = ((5 * C, C), (4 * C, LANES), (C, LANES), (C, LANES))


def turn_fused(ids, sides, z_mid, dz_parts, par, w_out, lnmid):
    n = z_mid.shape[-1]
    s1, w1 = weights_specs(par, 1, True)
    sds, vm = jax.ShapeDtypeStruct, pltpu.VMEM
    return call(
        turn_kernel, (T_STEPS + 8,),
        [SMEM_SPEC] + [tri_spec(v.shape) for v in sides] + [r_spec(n)] + two_specs((RB, C, n)) + s1 + [blk_spec(w_out.shape, 1), SMEM_SPEC, full_spec((W2, W2))],
        [two_specs((RB, C, n))[1], c_spec(n), r_spec(n)] + [full_spec(s) for s in ACC_POST],
        [sds((C, C, n), BF16), sds((C, LANES, n), BF16), sds((LANES, C, n), BF16)] + [sds(s, F32) for s in ACC_POST],
        [vm((C, LANES, n), F32), vm((C, RB, n), BF16)] + [vm((RB, C, n), BF16)] * 3 + [vm((C, RB, n), F32)] * 2 + [vm((RB, n), F32)],
        GIGA, 40 * MIB)(ids, *sides, z_mid, *dz_parts, *w1, w_out, lnmid, par[-1])


def pre_back_stages(z, dpg, mask_of, res_of, dst, wt, w, gain, lbias, dai_s, dbi_s, dp_s, zh_s, zn_s, rs_s, acc_b, sums):
    def gates(i):
        zn, rstd = norm_rows(z[i].astype(F32))
        zn_s[i] = zn
        rs_s[i] = jnp.broadcast_to(rstd, (8, rstd.shape[-1]))
        zh = (zn * gain[:] + lbias[:]).astype(BF16)
        zh_s[i] = zh
        p = dot_nn(wt[0:4 * C], with_ones(zh))
        m = HALF * mask_of(i).astype(F32)
        for side, ref in ((0, dai_s), (1, dbi_s)):
            base = side * 2 * C
            dm = ref[i].astype(F32) * m
            t = jnp.tanh(p[base:base + C])
            dv = dm * (1.0 + t)
            dg = dv * (p[base + C:base + 2 * C] * (1.0 - t))
            for k, d in ((2 * side, dg), (2 * side + 1, dv)):
                acc_b[k * C:(k + 1) * C] += fold(d)
                dp_s[i, k * C:(k + 1) * C] = d.astype(BF16)
        dp_s[i, 4 * C:5 * C] = dpg[i]

    def products(i):
        dp = dp_s[i]
        dzh = dot_nn(w[:], dp).astype(BF16).astype(F32)
        sums[0] += dot_nt(dp, zh_s[i])
        zn, rstd = zn_s[i], rs_s[i, 0:1, :]
        sums[1] += fold(dzh * zn)
        sums[2] += fold(dzh)
        dzn = dzh * gain[:]
        m1 = jnp.mean(dzn, axis=0, keepdims=True)
        m2 = jnp.mean(dzn * zn, axis=0, keepdims=True)
        dst[i] = (res_of(i).astype(F32) + rstd * (dzn - m1 - zn * m2)).astype(BF16)

    return gates, products


def back_kernel(ids, a, b, dx, dxq, z, dpg1, dzp, dzo, mp, mo, xn, rstd, zp, zo, wt1, gain1, lbias1, w1, wt0, gain0, lbias0, wot0, wo0, lnmid, perm, dzm, dx0, dxk, dxs, dpg0, acc_w, acc_b, acc_g, acc_lb, acc_bg, acc_bo, acc_wo, acc_mg, acc_mb, da_s, db_s, full, dai_s, dbi_s, dp_s, zh_s, zn_s, rs_s, xh_s, xi_s, dxi_s, dub_s, dxc_s):
    step = pl.program_id(0)
    clear(step, (acc_w, acc_b, acc_g, acc_lb, acc_bg, acc_bo, acc_wo, acc_mg, acc_mb))

    @pl.when(step < T_STEPS)
    def _():
        for ch, dst in channels(step):
            buf = full.at[ch % 2]
            place(buf, halves(dx.at[ch]), halves(dxq.at[ch]), ids)
            da_s[dst] = dot_nt(b[ch], buf[:]).astype(BF16)
            db_s[dst] = dot_nn(a[ch], buf[:]).astype(BF16)

    @pl.when(step >= T_STEPS)
    def _():
        r = step - T_STEPS
        rows = pl.ds(pl.multiple_of(r * RB, RB), RB)
        to_rows(perm[:], da_s.at[:, rows, :], dai_s)
        to_rows(perm[:], db_s.at[:, rows, :], dbi_s)
        for c in range(C):
            xh_s[c] = (xn[c] * lnmid[0, 0, c] + lnmid[0, 1, c]).astype(BF16)
        to_rows(perm[:], xh_s, xi_s)
        pre = [acc_w[:], acc_g[:], acc_lb[:]]
        pre_gates, pre_products = pre_back_stages(
            z, dpg1, lambda i: pick(r, mp[pl.ds(i, 1), :], mo[pl.ds(i, 1), :]), lambda i: pick(r, dzp[i], dzo[i]), dzm,
            wt1, w1, gain1, lbias1, dai_s, dbi_s, dp_s, zh_s, zn_s, rs_s, acc_b, pre)
        staggered(pre_gates, pre_products)
        acc_w[:], acc_g[:], acc_lb[:] = pre
        post = [acc_bg[:], acc_bo[:], acc_wo[:]]

        def gates(i):
            t = gate_of(pick(r, zp[i], zo[i]).astype(F32), wt0, gain0, lbias0)
            upd = dot_nn(wot0[:], with_ones(xi_s[i]))
            d_upd = (HALF * dzm[i].astype(F32)) * (1.0 + t)
            d_pg = d_upd * (upd * (1.0 - t))
            dpg0[i] = d_pg.astype(BF16)
            dub_s[i] = d_upd.astype(BF16)
            post[0] += fold(d_pg)
            post[1] += fold(d_upd)

        def products(i):
            dxi_s[i] = dot_nn(wo0[:], dub_s[i]).astype(BF16)
            post[2] += dot_nt(dub_s[i], xi_s[i])

        staggered(gates, products)
        acc_bg[:], acc_bo[:], acc_wo[:] = post

        def put(grp, v):
            dxc_s[grp * RB:(grp + 1) * RB] = v

        to_cmajor(perm[:], dxi_s, put)

        def emit(c, v):
            dx0[c] = v.astype(BF16)
            mine, other = split_cols(v, ids[1])
            dxk[c] = mine.astype(BF16)
            dxs[c] = other.astype(BF16)

        mid_back(dxc_s, xn, rstd[:], lnmid, 0, acc_mg, acc_mb, emit)


def back_fused(ids, sides, z_mid, dpg1, dz_parts, masks, xn, rstd, z_parts, par, w_proj, w_out, lnmid):
    n = z_mid.shape[-1]
    s1, w1 = weights_specs(par, 1, False)
    s0, w0 = weights_specs(par, 0, True)
    sds, vm = jax.ShapeDtypeStruct, pltpu.VMEM
    two = two_specs((RB, C, n))
    rows = vm((RB, C, n), BF16)
    accs = ACC_PRE + ACC_POST
    return call(
        back_kernel, (T_STEPS + 8,),
        [SMEM_SPEC] + [tri_spec(v.shape) for v in sides] + [r_spec(n), r_spec(n)] + two + two_specs((RB, n)) + [c_spec(n), m_spec(n)] + two
        + s1 + [blk_spec(w_proj.shape, 1)] + s0 + [blk_spec(w_out.shape, 0), SMEM_SPEC, full_spec((W2, W2))],
        [two[1], c_spec(n), c_spec(LANES), c_spec(LANES), r_spec(n)] + [full_spec(s) for s in accs],
        [sds((C, C, n), BF16), sds((C, LANES, n), BF16), sds((C, LANES, LANES), BF16), sds((C, LANES, LANES), BF16), sds((LANES, C, n), BF16)] + [sds(s, F32) for s in accs],
        [vm((C, LANES, n), BF16)] * 2 + [vm((2, n, n), BF16), rows, rows, vm((RB, 5 * C, n), BF16), rows, vm((RB, C, n), F32), vm((RB, 8, n), F32), vm((C, RB, n), BF16), rows, rows, rows, vm((C, RB, n), F32)],
        GIGA, 60 * MIB)(ids, *sides, z_mid, dpg1, *dz_parts, *masks, xn, rstd, *z_parts, *w1, w_proj, *w0, w_out, lnmid, par[-1])


def last_kernel(ids, dx, bp, bo, qp, qo, dxk, dxr, ap, ao, rp, ro, z, dpg, dres, mask, wt, gain, lbias, w, perm, dz, acc_w, acc_b, acc_g, acc_lb, da_s, db_s, full, tmp, dai_s, dbi_s, dp_s, zh_s, zn_s, rs_s):
    step = pl.program_id(0)
    xx = ids[0]
    clear(step, (acc_w, acc_b, acc_g, acc_lb))

    @pl.when(step < T_STEPS)
    def _():
        for ch, dst in channels(step):
            buf = full.at[ch % 2]
            place(buf, (bp[ch], bo[ch]), (qp[ch], qo[ch]), ids)
            da_s[dst] = dot_nn(dx[ch], buf[:]).astype(BF16)
            tmp[ch % 2] = dot_tn(dxk[ch], jnp.concatenate([ap[ch], ao[ch]], axis=0)) + dot_tn(dxr[ch], jnp.concatenate([rp[ch], ro[ch]], axis=0))
            db_s[dst] = tmp[ch % 2, pl.ds(pl.multiple_of(C * xx, C), C), :].astype(BF16)

    @pl.when(step >= T_STEPS)
    def _():
        rows = pl.ds(pl.multiple_of((step - T_STEPS) * RB, RB), RB)
        to_rows(perm[:], da_s.at[:, rows, :], dai_s)
        to_rows(perm[:], db_s.at[:, rows, :], dbi_s)
        sums = [acc_w[:], acc_g[:], acc_lb[:]]
        staggered(*pre_back_stages(
            z, dpg, lambda i: mask[pl.ds(i, 1), :], lambda i: dres[i], dz,
            wt, w, gain, lbias, dai_s, dbi_s, dp_s, zh_s, zn_s, rs_s, acc_b, sums))
        acc_w[:], acc_g[:], acc_lb[:] = sums


def last_fused(ids, sides, z, dpg, dres, mask, par, w_proj):
    n = z.shape[-1]
    s0, w0 = weights_specs(par, 0, False)
    sds, vm = jax.ShapeDtypeStruct, pltpu.VMEM
    rows = vm((RB, C, n), BF16)
    return call(
        last_kernel, (T_STEPS + 4,),
        [SMEM_SPEC, tri_spec((C, C, n), 1)] + [tri_spec(v.shape) for v in sides[1:]] + [r_spec(n), r_spec(n, 4), r_spec(n), m_spec(n)] + s0 + [blk_spec(w_proj.shape, 0), full_spec((W2, W2))],
        [r_spec(n)] + [full_spec(s) for s in ACC_PRE],
        [sds((C, C, n), BF16)] + [sds(s, F32) for s in ACC_PRE],
        [vm((C, C, n), BF16)] * 2 + [vm((2, n, n), BF16), vm((2, LANES, n), F32), rows, rows, vm((RB, 5 * C, n), BF16), rows, vm((RB, C, n), F32), vm((RB, 8, n), F32)],
        GIGA, 40 * MIB)(ids, *sides, z, dpg, dres, mask, *w0, w_proj, par[-1])


PACK = 512


def grads_kernel(n_dp, n_dap, w0, b0, q0, g0, l0, wo0, o0, mg0, mb0, w1, b1, q1, g1, l1, wo1, o1, mg1, mb1, out, buf, recv_a, red, recv_b, gath, vec, send_a, rcv_a, send_b, rcv_b, send_c, rcv_c, send_d, rcv_d):
    dp, dap = lax.axis_index("dp"), lax.axis_index("dap")
    big, small = PACK // n_dap, PACK // n_dap // n_dp
    bar = pltpu.get_barrier_semaphore()
    for k in range(1, n_dap):
        pl.semaphore_signal(bar, inc=1, device_id=(dp, lax.rem(dap + k, n_dap)), device_id_type=MESH_ID)
    for k in range(1, n_dp):
        pl.semaphore_signal(bar, inc=1, device_id=(lax.rem(dp + k, n_dp), dap), device_id_type=MESH_ID)

    buf[0:5 * C, 0:C] = w0[:]
    buf[0:5 * C, C:2 * C] = HALF * w1[:]
    buf[5 * C:6 * C, 0:C] = HALF * wo0[:]
    buf[5 * C:6 * C, C:2 * C] = HALF * wo1[:]

    def put(k, base, ref, scale):
        v = ref[:]
        if v.ndim == 3:
            v = jnp.sum(v, axis=1)
        rows = v.shape[0]
        tot = scale * jnp.sum(v, axis=1, keepdims=True)
        lane = lax.broadcasted_iota(jnp.int32, (rows, LANES), 1)
        vec[base:base + rows, :] = jnp.where(lane == k, tot, vec[base:base + rows, :])

    vec[:] = jnp.zeros_like(vec)
    put(0, 0, b0, 1.0)
    put(0, 4 * C, q0, HALF)
    put(1, 0, b1, HALF)
    put(1, 4 * C, q1, HALF)
    for k, (ref, scale) in enumerate(((g0, 1.0), (l0, 1.0), (g1, HALF), (l1, HALF), (mg0, HALF), (mb0, HALF), (mg1, HALF), (mb1, HALF), (o0, HALF), (o1, HALF))):
        put(2 + k, 0, ref, scale)
    vt = jnp.transpose(vec[:])
    for t in range(3):
        buf[6 * C + RB * t:6 * C + RB * t + RB, :] = vt[0:RB, LANES * t:LANES * (t + 1)]
    buf[6 * C + 48:PACK, :] = jnp.zeros((PACK - 6 * C - 48, LANES), F32)

    pl.semaphore_wait(bar, n_dap + n_dp - 2)

    def copies(count, make):
        made = [make(k) for k in range(1, count)]
        for cp in made:
            cp.start()
        return made

    def to_dap(k):
        return (dp, lax.rem(dap + k, n_dap))

    def to_dp(k):
        return (lax.rem(dp + k, n_dp), dap)

    def rows_of(idx, size):
        return pl.ds(pl.multiple_of(idx * size, size), size)

    stage = copies(n_dap, lambda k: pltpu.make_async_remote_copy(buf.at[rows_of(lax.rem(dap + k, n_dap), big)], recv_a.at[k - 1], send_a.at[k - 1], rcv_a.at[k - 1], device_id=to_dap(k), device_id_type=MESH_ID))
    tot = buf[rows_of(dap, big), :]
    for k, cp in enumerate(stage):
        cp.wait_recv()
        tot = tot + recv_a[k]
    red[:] = tot
    for cp in stage:
        cp.wait_send()

    stage = copies(n_dp, lambda k: pltpu.make_async_remote_copy(red.at[rows_of(lax.rem(dp + k, n_dp), small)], recv_b.at[k - 1], send_b.at[k - 1], rcv_b.at[k - 1], device_id=to_dp(k), device_id_type=MESH_ID))
    tot = red[rows_of(dp, small), :]
    for k, cp in enumerate(stage):
        cp.wait_recv()
        tot = tot + recv_b[k]
    gath[rows_of(dp, small), :] = tot
    for cp in stage:
        cp.wait_send()

    mine = gath.at[rows_of(dp, small)]
    stage = copies(n_dp, lambda k: pltpu.make_async_remote_copy(mine, mine, send_c.at[k - 1], rcv_c.at[k - 1], device_id=to_dp(k), device_id_type=MESH_ID))
    for cp in stage:
        cp.wait()

    stage = copies(n_dap, lambda k: pltpu.make_async_remote_copy(gath, out.at[rows_of(dap, big)], send_d.at[k - 1], rcv_d.at[k - 1], device_id=to_dap(k), device_id_type=MESH_ID))
    out[rows_of(dap, big), :] = gath[:]
    for cp in stage:
        cp.wait()


def sum_grads(n_dp, n_dap, parts):
    big, small = PACK // n_dap, PACK // n_dap // n_dp
    dma = pltpu.SemaphoreType.DMA
    return pl.pallas_call(
        functools.partial(grads_kernel, n_dp, n_dap),
        out_shape=jax.ShapeDtypeStruct((PACK, LANES), F32),
        in_specs=[pl.BlockSpec(memory_space=pltpu.VMEM)] * len(parts),
        out_specs=pl.BlockSpec(memory_space=pltpu.VMEM),
        scratch_shapes=[pltpu.VMEM((PACK, LANES), F32), pltpu.VMEM((n_dap - 1, big, LANES), F32), pltpu.VMEM((big, LANES), F32), pltpu.VMEM((max(n_dp - 1, 1), small, LANES), F32), pltpu.VMEM((big, LANES), F32), pltpu.VMEM((384, LANES), F32)]
        + [dma((n_dap - 1,))] * 2 + [dma((max(n_dp - 1, 1),))] * 4 + [dma((n_dap - 1,))] * 2,
        name="grad_sum",
        cost_estimate=pl.CostEstimate(flops=MEGA, bytes_accessed=MIB, transcendentals=0),
        compiler_params=pltpu.CompilerParams(collective_id=0, has_side_effects=True),
    )(*parts)


def unpack_kernel(src, ln_in, gw, bp, lm, gwo, bo):
    t = jnp.transpose(src[0:6 * C, :])
    for k in range(2):
        gw[k] = t[k * C:(k + 1) * C, 0:5 * C]
        gwo[k] = t[k * C:(k + 1) * C, 5 * C:6 * C]
    base = 6 * C
    bp[:, 0:LANES] = src[base:base + 2, :]
    bp[:, LANES:W2] = src[base + RB:base + 18, :]
    bp[:, W2:320] = src[base + 32:base + 34, 0:C]
    for k in range(2):
        ln_in[k] = src[base + 2 + 2 * k:base + 4 + 2 * k, 0:C]
        lm[k] = src[base + 6 + 2 * k:base + 8 + 2 * k, 0:C]
    bo[:] = src[base + 10:base + 12, 0:C]


def unpack(flat):
    outs = [jax.ShapeDtypeStruct(s, F32) for s in ((2, 2, C), (2, C, 5 * C), (2, 5 * C), (2, 2, C), (2, C, C), (2, C))]
    return call(unpack_kernel, (1,), [full_spec(flat.shape)], [full_spec(o.shape) for o in outs], outs, [], MEGA, MIB)(flat)


SUM = sum_grads


def solution(mesh):
    def plan(z_pair, pair_mask, dz_out, ln_in, w_proj, b_proj, ln_mid, w_out, b_out):
        n = z_pair.shape[2]
        dap = lax.axis_index("dap")
        ids = jnp.stack([dap // 2, dap % 2]).astype(jnp.int32)
        x_pairs = [(0, 2), (2, 0), (1, 3), (3, 1)]
        c_pairs = [(0, 1), (1, 0), (2, 3), (3, 2)]

        def over_x(v):
            return lax.ppermute(v, "dap", x_pairs)

        def over_c(v):
            return lax.ppermute(v, "dap", c_pairs)

        par = prepare(n, ln_in, w_proj, b_proj, w_out, b_out)
        lnmid = ln_mid.astype(F32)
        m_own = pair_mask[0]
        z_own = jnp.transpose(z_pair[0], (0, 2, 1))
        dz_own = jnp.transpose(dz_out[0], (0, 2, 1))
        m_peer = over_x(m_own)
        z_peer = over_x(z_own)
        z_peer, dz_src = lax.optimization_barrier((z_peer, dz_own))
        dz_peer = over_x(dz_src)
        masks = (m_peer, m_own)

        ao, bo = pre_forward(z_own, m_own, par)
        qo, ro = over_c(bo), over_c(ao)
        ap, bp = pre_forward(z_peer, m_peer, par)
        qp, rp = over_c(bp), over_c(ap)
        z_mid, xn, rstd, a1, b1, a1k, a1s = fwd_fused(ids, (ap, ao, bp, bo, qp, qo), z_peer, z_own, masks, par, lnmid)
        a1r, b1p = over_c(a1s), over_c(b1)
        z_new, dx1, dpg1, bg1, bo1, wo1, mg1, mb1 = turn_fused(ids, (a1k, a1r, b1, b1p), z_mid, (dz_peer, dz_own), par, w_out, lnmid)
        dx1p = over_c(dx1)
        dz_mid, dx0, dx0k, dx0s, dpg0, w1, b1s, g1, lb1, bg0, bo0, wo0, mg0, mb0 = back_fused(ids, (a1, b1, dx1, dx1p), z_mid, dpg1, (dz_peer, dz_own), masks, xn, rstd, (z_peer, z_own), par, w_proj, w_out, lnmid)
        dx0r = over_c(dx0s)
        dz, w0, b0s, g0, lb0 = last_fused(ids, (dx0, bp, bo, qp, qo, dx0k, dx0r, ap, ao, rp, ro), z_own, dpg0, dz_mid, m_own, par, w_proj)

        flat = SUM(mesh.shape["dp"], mesh.shape["dap"], (w0, b0s, bg0, g0, lb0, wo0, bo0, mg0, mb0, w1, b1s, bg1, g1, lb1, wo1, bo1, mg1, mb1))
        g_ln_in, gw, g_bp, g_lm, gwo, g_bo = unpack(flat)
        z_res = jnp.transpose(z_new, (0, 2, 1))[None]
        dz_res = jnp.transpose(dz, (0, 2, 1))[None]
        return z_res, dz_res, g_ln_in, gw, g_bp, g_lm, gwo, g_bo

    row_spec = P("dp", "dap")
    return jax.shard_map(plan, mesh=mesh, in_specs=(row_spec, row_spec, row_spec, P(), P(), P(), P(), P(), P()), out_specs=(row_spec, row_spec, P(), P(), P(), P(), P(), P()), check_vma=False)
```

```python
import functools

import jax
import jax.numpy as jnp
from jax import lax
from jax.experimental import pallas as pl
from jax.experimental.pallas import tpu as pltpu
from jax.sharding import PartitionSpec as P


EPS = 1e-5
F32 = jnp.float32
BF16 = jnp.bfloat16
INTERPRET = False
C = 64
RB = 16
DELAY = 4
LANES = 128
W2 = 256
HALF = 0.5
MEGA = 10 ** 6
GIGA = 10 ** 9
MIB = 2 ** 20
VMEM_LIMIT = 67043328


MESH_ID = pl.DeviceIdType.MESH


def dot_nn(a, b):
    return lax.dot_general(a, b, (((1,), (0,)), ((), ())), preferred_element_type=F32)


def dot_nt(a, b):
    return lax.dot_general(a, b, (((1,), (1,)), ((), ())), preferred_element_type=F32)


def dot_tn(a, b):
    return lax.dot_general(a, b, (((0,), (0,)), ((), ())), preferred_element_type=F32)


def norm_rows(zf):
    mean = jnp.mean(zf, axis=0, keepdims=True)
    cen = zf - mean
    var = jnp.mean(cen * cen, axis=0, keepdims=True)
    rstd = lax.rsqrt(var + EPS)
    return cen * rstd, rstd


def staggered(first, second):
    for i in range(RB + DELAY):
        if i < RB:
            first(i)
        if i >= DELAY:
            second(i - DELAY)


def fold(v):
    return v[:, :LANES] + v[:, LANES:]


def to_cmajor(perm, src, dst):
    n = src.shape[-1]
    for grp in range(C // RB):
        blk = src[:, grp * RB:(grp + 1) * RB, :].reshape(W2, n)
        out = dot_nn(perm, blk)
        dst(grp, out.reshape(RB, RB, n))


def to_rows(perm, src, dst):
    n = src.shape[-1]
    for grp in range(C // RB):
        blk = src[grp * RB:(grp + 1) * RB, :, :].reshape(W2, n)
        out = dot_nn(perm, blk)
        dst[:, grp * RB:(grp + 1) * RB, :] = out.reshape(RB, RB, n).astype(BF16)


def split_cols(v, core):
    lo, hi = v[..., :LANES], v[..., LANES:]
    lane = lax.broadcasted_iota(jnp.int32, lo.shape, lo.ndim - 1)
    axis = lo.ndim - 1
    first = jnp.where(lane < C, lo, pltpu.roll(hi, C, axis))
    second = jnp.where(lane < C, pltpu.roll(lo, C, axis), hi)
    mine = jnp.where(core == 0, first, second)
    other = jnp.where(core == 0, second, first)
    return mine, other


KA = C + RB


def prep_kernel(ids, lnmid, w_proj, b_proj, ln_in, w_out, b_out, wt_aug, wot_aug, gain, lbias, perm, scr):
    n = gain.shape[-1]
    for k in range(2):
        scr[:] = jnp.zeros_like(scr)
        scr[0:C, 0:5 * C] = w_proj[k].astype(F32)
        scr[C:C + 1, 0:5 * C] = b_proj[pl.ds(k, 1), :]
        wt_aug[k] = (HALF * jnp.transpose(scr[:]))[0:5 * C, 0:KA].astype(BF16)
        scr[:] = jnp.zeros_like(scr)
        scr[0:C, 0:C] = w_out[k].astype(F32)
        scr[C:C + 1, 0:C] = b_out[pl.ds(k, 1), :]
        scr[C + 8:C + 10, 0:C] = ln_in[k]
        small = jnp.transpose(scr[:, 0:LANES])
        wot_aug[k] = (HALF * small)[0:C, 0:KA].astype(BF16)
        gain[k] = jnp.broadcast_to(small[0:C, C + 8:C + 9], (C, n))
        lbias[k] = jnp.broadcast_to(small[0:C, C + 9:C + 10], (C, n))
    r = lax.broadcasted_iota(jnp.int32, (W2, W2), 0)
    q = lax.broadcasted_iota(jnp.int32, (W2, W2), 1)
    perm[:] = jnp.where(q == RB * (r % RB) + r // RB, 1.0, 0.0).astype(BF16)


def prepare(n, ids, lnmid, ln_in, w_proj, b_proj, w_out, b_out):
    sds = jax.ShapeDtypeStruct
    outs = [sds((2, 5 * C, KA), BF16), sds((2, C, KA), BF16), sds((2, C, n), F32), sds((2, C, n), F32), sds((W2, W2), BF16)]
    args = (w_proj, b_proj.astype(F32), ln_in.astype(F32), w_out, b_out.astype(F32))
    return call(prep_kernel, (1,), [SMEM_SPEC, SMEM_SPEC] + [full_spec(v.shape) for v in args], [full_spec(o.shape) for o in outs], outs, [pltpu.VMEM((LANES, 384), F32)], MEGA, MIB)(ids, lnmid, *args)


def with_ones(zh):
    row = lax.broadcasted_iota(jnp.int32, (RB, zh.shape[-1]), 0)
    return jnp.concatenate([zh, jnp.where(row == 0, 1.0, 0.0).astype(BF16)], axis=0)


def pre_fwd_kernel(z, mask, wt, gain, lbias, perm, a, b, a_s, b_s):
    for i in range(RB):
        a_s[i], b_s[i] = project(z[i].astype(F32), mask[pl.ds(i, 1), :].astype(F32), wt, gain, lbias)

    def put_a(grp, v):
        a[grp * RB:(grp + 1) * RB] = v.astype(BF16)

    def put_b(grp, v):
        b[grp * RB:(grp + 1) * RB] = v.astype(BF16)

    to_cmajor(perm[:], a_s, put_a)
    to_cmajor(perm[:], b_s, put_b)


def full_spec(shape):
    return pl.BlockSpec(shape, lambda s: (0,) * len(shape))


SMEM_SPEC = pl.BlockSpec(memory_space=pltpu.SMEM)


def call(kernel, grid, in_specs, out_specs, out_shape, scratch, flops, bytes_accessed, trans=0):
    return pl.pallas_call(
        kernel,
        grid=grid,
        in_specs=in_specs,
        out_specs=out_specs,
        out_shape=out_shape,
        scratch_shapes=scratch,
        interpret=INTERPRET,
        cost_estimate=pl.CostEstimate(flops=flops, bytes_accessed=bytes_accessed, transcendentals=trans),
        compiler_params=pltpu.CompilerParams(dimension_semantics=("arbitrary",) * len(grid), vmem_limit_bytes=VMEM_LIMIT),
    )


def blk_spec(shape, k):
    return pl.BlockSpec((None,) + tuple(shape[1:]), lambda s: (k,) + (0,) * (len(shape) - 1))


def pre_forward(z, mask, par):
    rows, _, n = z.shape
    specs, args = weights_specs(par, 0, False)
    cspec = pl.BlockSpec((C, RB, n), lambda s: (0, s, 0))
    return call(
        pre_fwd_kernel, (rows // RB,),
        [pl.BlockSpec((RB, C, n), lambda s: (s, 0, 0)), pl.BlockSpec((RB, n), lambda s: (s, 0))] + specs + [full_spec((W2, W2))],
        [cspec] * 2, [jax.ShapeDtypeStruct((C, rows, n), BF16)] * 2, [pltpu.VMEM((RB, C, n), BF16)] * 2, GIGA, 8 * MIB)(z, mask, *args, par[-1])


CB = 16
T_STEPS = C // CB


def global_rows(ids, partner):
    x, c = ids[0], ids[1]
    cc = 1 - c if partner else c
    return pl.multiple_of(C * (2 * (1 - x) + cc), C), pl.multiple_of(C * (2 * x + cc), C)


def place(dst, src_mine, src_other, ids):
    for (peer, own), partner in ((src_mine, False), (src_other, True)):
        off_peer, off_own = global_rows(ids, partner)
        dst[pl.ds(off_peer, C), :] = peer
        dst[pl.ds(off_own, C), :] = own


def halves(ref):
    return ref[0:C, :], ref[C:LANES, :]


def tri_spec(shape, row_blk=0):
    return pl.BlockSpec((CB,) + tuple(shape[1:]), lambda s: (jnp.minimum(s, T_STEPS - 1), row_blk, 0))


def row_blk(s):
    return jnp.maximum(s - T_STEPS, 0)


def r_spec(n, off=0):
    return pl.BlockSpec((RB, C, n), lambda s: (row_blk(s) + off, 0, 0))


def c_spec(n):
    return pl.BlockSpec((C, RB, n), lambda s: (0, row_blk(s), 0))


def two_specs(shape):
    zeros = (0,) * (len(shape) - 1)
    return [pl.BlockSpec(shape, lambda s: (jnp.clip(s - T_STEPS, 0, 3),) + zeros), pl.BlockSpec(shape, lambda s: (jnp.maximum(s - T_STEPS - 4, 0),) + zeros)]


def m_spec(n):
    return pl.BlockSpec((RB, n), lambda s: (row_blk(s), 0))


def pick(r, peer, own):
    return jnp.where(r < 4, peer, own)


def channels(step):
    return [(ch, step * CB + ch) for ch in range(CB)]


def mid_norm(x, xh_s, lnmid, blk, xn_s, rstd_s):
    tot = x[0]
    for c in range(1, C):
        tot = tot + x[c]
    mean = tot * (1.0 / C)
    d = x[0] - mean
    sq = d * d
    for c in range(1, C):
        d = x[c] - mean
        sq = sq + d * d
    rstd = lax.rsqrt(sq * (1.0 / C) + EPS)
    rstd_s[:] = rstd
    for c in range(C):
        xn = (x[c] - mean) * rstd
        xn_s[c] = xn
        xh_s[c] = (xn * lnmid[blk, 0, c] + lnmid[blk, 1, c]).astype(BF16)


def gate_of(zf, wt, gain, lbias):
    zn, _ = norm_rows(zf)
    zh = (zn * gain[:] + lbias[:]).astype(BF16)
    return jnp.tanh(dot_nn(wt[4 * C:5 * C], with_ones(zh)))


def project(zf, m, wt, gain, lbias):
    zn, _ = norm_rows(zf)
    zh = (zn * gain[:] + lbias[:]).astype(BF16)
    p = dot_nn(wt[0:4 * C], with_ones(zh))
    a = ((1.0 + jnp.tanh(p[0:C])) * (p[C:2 * C] * m)).astype(BF16)
    b = ((1.0 + jnp.tanh(p[2 * C:3 * C])) * (p[3 * C:4 * C] * m)).astype(BF16)
    return a, b


def fwd_kernel(ids, ap, ao, bp, bo, qp, qo, zp, zo, mp, mo, wt0, gain0, lbias0, wot0, wt1, gain1, lbias1, lnmid, perm, zmid, xn, rstd, a1, b1, a1k, a1s, x_s, full, xh_s, xi_s, a_s, b_s):
    step = pl.program_id(0)

    @pl.when(step < T_STEPS)
    def _():
        for ch, dst in channels(step):
            buf = full.at[ch % 2]
            place(buf, (bp[ch], bo[ch]), (qp[ch], qo[ch]), ids)
            x_s[dst] = dot_nt(jnp.concatenate([ap[ch], ao[ch]], axis=0), buf[:])

    @pl.when(step >= T_STEPS)
    def _():
        r = step - T_STEPS
        mid_norm(x_s.at[:, pl.ds(pl.multiple_of(r * RB, RB), RB), :], xh_s, lnmid, 0, xn, rstd)
        to_rows(perm[:], xh_s, xi_s)

        def update(i):
            zf = pick(r, zp[i], zo[i]).astype(F32)
            upd = dot_nn(wot0[:], with_ones(xi_s[i]))
            zmid[i] = (zf + (1.0 + gate_of(zf, wt0, gain0, lbias0)) * upd).astype(BF16)

        def sides(i):
            m = pick(r, mp[pl.ds(i, 1), :], mo[pl.ds(i, 1), :]).astype(F32)
            a_s[i], b_s[i] = project(zmid[i].astype(F32), m, wt1, gain1, lbias1)

        staggered(update, sides)

        def put_a(grp, v):
            a1[grp * RB:(grp + 1) * RB] = v.astype(BF16)
            mine, other = split_cols(v, ids[1])
            a1k[grp * RB:(grp + 1) * RB] = mine.astype(BF16)
            a1s[grp * RB:(grp + 1) * RB] = other.astype(BF16)

        def put_b(grp, v):
            b1[grp * RB:(grp + 1) * RB] = v.astype(BF16)

        to_cmajor(perm[:], a_s, put_a)
        to_cmajor(perm[:], b_s, put_b)


def weights_specs(par, blk, with_out):
    wt, wot, gain, lbias, _ = par
    specs = [blk_spec(wt.shape, blk), blk_spec(gain.shape, blk), blk_spec(gain.shape, blk)]
    args = [wt, gain, lbias]
    if with_out:
        specs.append(blk_spec(wot.shape, blk))
        args.append(wot)
    return specs, args


def fwd_fused(ids, sides, zp, zo, masks, par, lnmid):
    n = zp.shape[-1]
    s0, w0 = weights_specs(par, 0, True)
    s1, w1 = weights_specs(par, 1, False)
    sds, vm = jax.ShapeDtypeStruct, pltpu.VMEM
    c_out, h_out = sds((C, LANES, n), BF16), sds((C, LANES, LANES), BF16)
    return call(
        fwd_kernel, (T_STEPS + 8,),
        [SMEM_SPEC] + [tri_spec(v.shape) for v in sides] + two_specs((RB, C, n)) + two_specs((RB, n)) + s0 + s1 + [SMEM_SPEC, full_spec((W2, W2))],
        [r_spec(n), c_spec(n), m_spec(n), c_spec(n), c_spec(n), c_spec(LANES), c_spec(LANES)],
        [sds((LANES, C, n), BF16), sds((C, LANES, n), F32), sds((LANES, n), F32), c_out, c_out, h_out, h_out],
        [vm((C, LANES, n), F32), vm((2, n, n), BF16), vm((C, RB, n), BF16), vm((RB, C, n), BF16), vm((RB, C, n), BF16), vm((RB, C, n), BF16)],
        GIGA, 40 * MIB)(ids, *sides, zp, zo, *masks, *w0, *w1, lnmid, par[-1])


def mid_back(dxc_s, xn, rstd, lnmid, blk, acc_mg, acc_mb, emit):
    m1 = m2 = None
    for c in range(C):
        dy = dxc_s[c]
        dyx = dy * xn[c]
        gn = lnmid[blk, 0, c]
        m1 = dy * gn if m1 is None else m1 + dy * gn
        m2 = dyx * gn if m2 is None else m2 + dyx * gn
        acc_mg[c] += fold(dyx[0:8] + dyx[8:RB])
        acc_mb[c] += fold(dy[0:8] + dy[8:RB])
    m1 = m1 * (1.0 / C)
    m2 = m2 * (1.0 / C)
    for c in range(C):
        emit(c, rstd * (dxc_s[c] * lnmid[blk, 0, c] - m1 - xn[c] * m2))


def clear(step, accs):
    @pl.when(step == 0)
    def _():
        for acc in accs:
            acc[:] = jnp.zeros_like(acc)


def turn_kernel(ids, ak, ar, b, bq, z, dzp, dzo, wt, gain, lbias, wot, wo, lnmid, perm, znew, dx, dpg, acc_bg, acc_bo, acc_wo, acc_mg, acc_mb, x_s, xh_s, xi_s, dxi_s, dub_s, dxc_s, xn_s, r_s):
    step = pl.program_id(0)
    xx = ids[0]
    clear(step, (acc_bg, acc_bo, acc_wo, acc_mg, acc_mb))

    @pl.when(step < T_STEPS)
    def _():
        for ch, dst in channels(step):
            out = dot_tn(ak[ch], b[ch]) + dot_tn(ar[ch], bq[ch])
            x_s[dst, pl.ds(pl.multiple_of(C * (1 - xx), C), C), :] = out[0:C]
            x_s[dst, pl.ds(pl.multiple_of(C * xx, C), C), :] = out[C:LANES]

    @pl.when(step >= T_STEPS)
    def _():
        r = step - T_STEPS
        mid_norm(x_s.at[:, pl.ds(pl.multiple_of(r * RB, RB), RB), :], xh_s, lnmid, 1, xn_s, r_s)
        to_rows(perm[:], xh_s, xi_s)
        sums = [acc_bg[:], acc_bo[:], acc_wo[:]]

        def gates(i):
            zf = z[i].astype(F32)
            dz = pick(r, dzp[i], dzo[i]).astype(F32)
            t = gate_of(zf, wt, gain, lbias)
            upd = dot_nn(wot[:], with_ones(xi_s[i]))
            t1 = 1.0 + t
            znew[i] = (zf + t1 * upd).astype(BF16)
            d_upd = (HALF * dz) * t1
            d_pg = d_upd * (upd * (1.0 - t))
            dpg[i] = d_pg.astype(BF16)
            dub_s[i] = d_upd.astype(BF16)
            sums[0] += fold(d_pg)
            sums[1] += fold(d_upd)

        def products(i):
            dxi_s[i] = dot_nn(wo[:], dub_s[i]).astype(BF16)
            sums[2] += dot_nt(dub_s[i], xi_s[i])

        staggered(gates, products)
        acc_bg[:], acc_bo[:], acc_wo[:] = sums

        def put(grp, v):
            dxc_s[grp * RB:(grp + 1) * RB] = v

        to_cmajor(perm[:], dxi_s, put)

        def emit(c, v):
            dx[c] = v.astype(BF16)

        mid_back(dxc_s, xn_s, r_s[:], lnmid, 1, acc_mg, acc_mb, emit)


ACC_POST = ((C, LANES), (C, LANES), (C, C), (C, 8, LANES), (C, 8, LANES))
ACC_PRE = ((5 * C, C), (4 * C, LANES), (C, LANES), (C, LANES))


def turn_fused(ids, sides, z_mid, dz_parts, par, w_out, lnmid):
    n = z_mid.shape[-1]
    s1, w1 = weights_specs(par, 1, True)
    sds, vm = jax.ShapeDtypeStruct, pltpu.VMEM
    return call(
        turn_kernel, (T_STEPS + 8,),
        [SMEM_SPEC] + [tri_spec(v.shape) for v in sides] + [r_spec(n)] + two_specs((RB, C, n)) + s1 + [blk_spec(w_out.shape, 1), SMEM_SPEC, full_spec((W2, W2))],
        [two_specs((RB, C, n))[1], c_spec(n), r_spec(n)] + [full_spec(s) for s in ACC_POST],
        [sds((C, C, n), BF16), sds((C, LANES, n), BF16), sds((LANES, C, n), BF16)] + [sds(s, F32) for s in ACC_POST],
        [vm((C, LANES, n), F32), vm((C, RB, n), BF16)] + [vm((RB, C, n), BF16)] * 3 + [vm((C, RB, n), F32)] * 2 + [vm((RB, n), F32)],
        GIGA, 40 * MIB)(ids, *sides, z_mid, *dz_parts, *w1, w_out, lnmid, par[-1])


def pre_back_stages(z, dpg, mask_of, res_of, dst, wt, w, gain, lbias, dai_s, dbi_s, dp_s, zh_s, zn_s, rs_s, acc_b, sums):
    def gates(i):
        zn, rstd = norm_rows(z[i].astype(F32))
        zn_s[i] = zn
        rs_s[i] = jnp.broadcast_to(rstd, (8, rstd.shape[-1]))
        zh = (zn * gain[:] + lbias[:]).astype(BF16)
        zh_s[i] = zh
        p = dot_nn(wt[0:4 * C], with_ones(zh))
        m = HALF * mask_of(i).astype(F32)
        for side, ref in ((0, dai_s), (1, dbi_s)):
            base = side * 2 * C
            dm = ref[i].astype(F32) * m
            t = jnp.tanh(p[base:base + C])
            dv = dm * (1.0 + t)
            dg = dv * (p[base + C:base + 2 * C] * (1.0 - t))
            for k, d in ((2 * side, dg), (2 * side + 1, dv)):
                acc_b[k * C:(k + 1) * C] += fold(d)
                dp_s[i, k * C:(k + 1) * C] = d.astype(BF16)
        dp_s[i, 4 * C:5 * C] = dpg[i]

    def products(i):
        dp = dp_s[i]
        dzh = dot_nn(w[:], dp).astype(BF16).astype(F32)
        sums[0] += dot_nt(dp, zh_s[i])
        zn, rstd = zn_s[i], rs_s[i, 0:1, :]
        sums[1] += fold(dzh * zn)
        sums[2] += fold(dzh)
        dzn = dzh * gain[:]
        m1 = jnp.mean(dzn, axis=0, keepdims=True)
        m2 = jnp.mean(dzn * zn, axis=0, keepdims=True)
        dst[i] = (res_of(i).astype(F32) + rstd * (dzn - m1 - zn * m2)).astype(BF16)

    return gates, products


def back_kernel(ids, a, b, dx, dxq, z, dpg1, dzp, dzo, mp, mo, xn, rstd, zp, zo, wt1, gain1, lbias1, w1, wt0, gain0, lbias0, wot0, wo0, lnmid, perm, dzm, dx0, dxk, dxs, dpg0, acc_w, acc_b, acc_g, acc_lb, acc_bg, acc_bo, acc_wo, acc_mg, acc_mb, da_s, db_s, full, dai_s, dbi_s, dp_s, zh_s, zn_s, rs_s, xh_s, xi_s, dxi_s, dub_s, dxc_s):
    step = pl.program_id(0)
    clear(step, (acc_w, acc_b, acc_g, acc_lb, acc_bg, acc_bo, acc_wo, acc_mg, acc_mb))

    @pl.when(step < T_STEPS)
    def _():
        for ch, dst in channels(step):
            buf = full.at[ch % 2]
            place(buf, halves(dx.at[ch]), halves(dxq.at[ch]), ids)
            da_s[dst] = dot_nt(b[ch], buf[:]).astype(BF16)
            db_s[dst] = dot_nn(a[ch], buf[:]).astype(BF16)

    @pl.when(step >= T_STEPS)
    def _():
        r = step - T_STEPS
        rows = pl.ds(pl.multiple_of(r * RB, RB), RB)
        to_rows(perm[:], da_s.at[:, rows, :], dai_s)
        to_rows(perm[:], db_s.at[:, rows, :], dbi_s)
        for c in range(C):
            xh_s[c] = (xn[c] * lnmid[0, 0, c] + lnmid[0, 1, c]).astype(BF16)
        to_rows(perm[:], xh_s, xi_s)
        pre = [acc_w[:], acc_g[:], acc_lb[:]]
        pre_gates, pre_products = pre_back_stages(
            z, dpg1, lambda i: pick(r, mp[pl.ds(i, 1), :], mo[pl.ds(i, 1), :]), lambda i: pick(r, dzp[i], dzo[i]), dzm,
            wt1, w1, gain1, lbias1, dai_s, dbi_s, dp_s, zh_s, zn_s, rs_s, acc_b, pre)
        staggered(pre_gates, pre_products)
        acc_w[:], acc_g[:], acc_lb[:] = pre
        post = [acc_bg[:], acc_bo[:], acc_wo[:]]

        def gates(i):
            t = gate_of(pick(r, zp[i], zo[i]).astype(F32), wt0, gain0, lbias0)
            upd = dot_nn(wot0[:], with_ones(xi_s[i]))
            d_upd = (HALF * dzm[i].astype(F32)) * (1.0 + t)
            d_pg = d_upd * (upd * (1.0 - t))
            dpg0[i] = d_pg.astype(BF16)
            dub_s[i] = d_upd.astype(BF16)
            post[0] += fold(d_pg)
            post[1] += fold(d_upd)

        def products(i):
            dxi_s[i] = dot_nn(wo0[:], dub_s[i]).astype(BF16)
            post[2] += dot_nt(dub_s[i], xi_s[i])

        staggered(gates, products)
        acc_bg[:], acc_bo[:], acc_wo[:] = post

        def put(grp, v):
            dxc_s[grp * RB:(grp + 1) * RB] = v

        to_cmajor(perm[:], dxi_s, put)

        def emit(c, v):
            dx0[c] = v.astype(BF16)
            mine, other = split_cols(v, ids[1])
            dxk[c] = mine.astype(BF16)
            dxs[c] = other.astype(BF16)

        mid_back(dxc_s, xn, rstd[:], lnmid, 0, acc_mg, acc_mb, emit)


def back_fused(ids, sides, z_mid, dpg1, dz_parts, masks, xn, rstd, z_parts, par, w_proj, w_out, lnmid):
    n = z_mid.shape[-1]
    s1, w1 = weights_specs(par, 1, False)
    s0, w0 = weights_specs(par, 0, True)
    sds, vm = jax.ShapeDtypeStruct, pltpu.VMEM
    two = two_specs((RB, C, n))
    rows = vm((RB, C, n), BF16)
    accs = ACC_PRE + ACC_POST
    return call(
        back_kernel, (T_STEPS + 8,),
        [SMEM_SPEC] + [tri_spec(v.shape) for v in sides] + [r_spec(n), r_spec(n)] + two + two_specs((RB, n)) + [c_spec(n), m_spec(n)] + two
        + s1 + [blk_spec(w_proj.shape, 1)] + s0 + [blk_spec(w_out.shape, 0), SMEM_SPEC, full_spec((W2, W2))],
        [two[1], c_spec(n), c_spec(LANES), c_spec(LANES), r_spec(n)] + [full_spec(s) for s in accs],
        [sds((C, C, n), BF16), sds((C, LANES, n), BF16), sds((C, LANES, LANES), BF16), sds((C, LANES, LANES), BF16), sds((LANES, C, n), BF16)] + [sds(s, F32) for s in accs],
        [vm((C, LANES, n), BF16)] * 2 + [vm((2, n, n), BF16), rows, rows, vm((RB, 5 * C, n), BF16), rows, vm((RB, C, n), F32), vm((RB, 8, n), F32), vm((C, RB, n), BF16), rows, rows, rows, vm((C, RB, n), F32)],
        GIGA, 60 * MIB)(ids, *sides, z_mid, dpg1, *dz_parts, *masks, xn, rstd, *z_parts, *w1, w_proj, *w0, w_out, lnmid, par[-1])


def last_kernel(ids, dx, bp, bo, qp, qo, dxk, dxr, ap, ao, rp, ro, z, dpg, dres, mask, wt, gain, lbias, w, perm, dz, acc_w, acc_b, acc_g, acc_lb, da_s, db_s, full, tmp, dai_s, dbi_s, dp_s, zh_s, zn_s, rs_s):
    step = pl.program_id(0)
    xx = ids[0]
    clear(step, (acc_w, acc_b, acc_g, acc_lb))

    @pl.when(step < T_STEPS)
    def _():
        for ch, dst in channels(step):
            buf = full.at[ch % 2]
            place(buf, (bp[ch], bo[ch]), (qp[ch], qo[ch]), ids)
            da_s[dst] = dot_nn(dx[ch], buf[:]).astype(BF16)
            tmp[ch % 2] = dot_tn(dxk[ch], jnp.concatenate([ap[ch], ao[ch]], axis=0)) + dot_tn(dxr[ch], jnp.concatenate([rp[ch], ro[ch]], axis=0))
            db_s[dst] = tmp[ch % 2, pl.ds(pl.multiple_of(C * xx, C), C), :].astype(BF16)

    @pl.when(step >= T_STEPS)
    def _():
        rows = pl.ds(pl.multiple_of((step - T_STEPS) * RB, RB), RB)
        to_rows(perm[:], da_s.at[:, rows, :], dai_s)
        to_rows(perm[:], db_s.at[:, rows, :], dbi_s)
        sums = [acc_w[:], acc_g[:], acc_lb[:]]
        staggered(*pre_back_stages(
            z, dpg, lambda i: mask[pl.ds(i, 1), :], lambda i: dres[i], dz,
            wt, w, gain, lbias, dai_s, dbi_s, dp_s, zh_s, zn_s, rs_s, acc_b, sums))
        acc_w[:], acc_g[:], acc_lb[:] = sums


def last_fused(ids, sides, z, dpg, dres, mask, par, w_proj):
    n = z.shape[-1]
    s0, w0 = weights_specs(par, 0, False)
    sds, vm = jax.ShapeDtypeStruct, pltpu.VMEM
    rows = vm((RB, C, n), BF16)
    return call(
        last_kernel, (T_STEPS + 4,),
        [SMEM_SPEC, tri_spec((C, C, n), 1)] + [tri_spec(v.shape) for v in sides[1:]] + [r_spec(n), r_spec(n, 4), r_spec(n), m_spec(n)] + s0 + [blk_spec(w_proj.shape, 0), full_spec((W2, W2))],
        [r_spec(n)] + [full_spec(s) for s in ACC_PRE],
        [sds((C, C, n), BF16)] + [sds(s, F32) for s in ACC_PRE],
        [vm((C, C, n), BF16)] * 2 + [vm((2, n, n), BF16), vm((2, LANES, n), F32), rows, rows, vm((RB, 5 * C, n), BF16), rows, vm((RB, C, n), F32), vm((RB, 8, n), F32)],
        GIGA, 40 * MIB)(ids, *sides, z, dpg, dres, mask, *w0, w_proj, par[-1])


PACK = 512


def grads_kernel(n_dp, n_dap, w0, b0, q0, g0, l0, wo0, o0, mg0, mb0, w1, b1, q1, g1, l1, wo1, o1, mg1, mb1, out, buf, recv_a, red, recv_b, gath, vec, send_a, rcv_a, send_b, rcv_b, send_c, rcv_c, send_d, rcv_d):
    dp, dap = lax.axis_index("dp"), lax.axis_index("dap")
    big, small = PACK // n_dap, PACK // n_dap // n_dp
    bar = pltpu.get_barrier_semaphore()
    for k in range(1, n_dap):
        pl.semaphore_signal(bar, inc=1, device_id=(dp, lax.rem(dap + k, n_dap)), device_id_type=MESH_ID)
    for k in range(1, n_dp):
        pl.semaphore_signal(bar, inc=1, device_id=(lax.rem(dp + k, n_dp), dap), device_id_type=MESH_ID)

    buf[0:5 * C, 0:C] = w0[:]
    buf[0:5 * C, C:2 * C] = HALF * w1[:]
    buf[5 * C:6 * C, 0:C] = HALF * wo0[:]
    buf[5 * C:6 * C, C:2 * C] = HALF * wo1[:]

    def put(k, base, ref, scale):
        v = ref[:]
        if v.ndim == 3:
            v = jnp.sum(v, axis=1)
        rows = v.shape[0]
        tot = scale * jnp.sum(v, axis=1, keepdims=True)
        lane = lax.broadcasted_iota(jnp.int32, (rows, LANES), 1)
        vec[base:base + rows, :] = jnp.where(lane == k, tot, vec[base:base + rows, :])

    vec[:] = jnp.zeros_like(vec)
    put(0, 0, b0, 1.0)
    put(0, 4 * C, q0, HALF)
    put(1, 0, b1, HALF)
    put(1, 4 * C, q1, HALF)
    for k, (ref, scale) in enumerate(((g0, 1.0), (l0, 1.0), (g1, HALF), (l1, HALF), (mg0, HALF), (mb0, HALF), (mg1, HALF), (mb1, HALF), (o0, HALF), (o1, HALF))):
        put(2 + k, 0, ref, scale)
    vt = jnp.transpose(vec[:])
    for t in range(3):
        buf[6 * C + RB * t:6 * C + RB * t + RB, :] = vt[0:RB, LANES * t:LANES * (t + 1)]
    buf[6 * C + 48:PACK, :] = jnp.zeros((PACK - 6 * C - 48, LANES), F32)

    pl.semaphore_wait(bar, n_dap + n_dp - 2)

    def copies(count, make):
        made = [make(k) for k in range(1, count)]
        for cp in made:
            cp.start()
        return made

    def to_dap(k):
        return (dp, lax.rem(dap + k, n_dap))

    def to_dp(k):
        return (lax.rem(dp + k, n_dp), dap)

    def rows_of(idx, size):
        return pl.ds(pl.multiple_of(idx * size, size), size)

    stage = copies(n_dap, lambda k: pltpu.make_async_remote_copy(buf.at[rows_of(lax.rem(dap + k, n_dap), big)], recv_a.at[k - 1], send_a.at[k - 1], rcv_a.at[k - 1], device_id=to_dap(k), device_id_type=MESH_ID))
    tot = buf[rows_of(dap, big), :]
    for k, cp in enumerate(stage):
        cp.wait_recv()
        tot = tot + recv_a[k]
    red[:] = tot
    for cp in stage:
        cp.wait_send()

    stage = copies(n_dp, lambda k: pltpu.make_async_remote_copy(red.at[rows_of(lax.rem(dp + k, n_dp), small)], recv_b.at[k - 1], send_b.at[k - 1], rcv_b.at[k - 1], device_id=to_dp(k), device_id_type=MESH_ID))
    tot = red[rows_of(dp, small), :]
    for k, cp in enumerate(stage):
        cp.wait_recv()
        tot = tot + recv_b[k]
    gath[rows_of(dp, small), :] = tot
    for cp in stage:
        cp.wait_send()

    mine = gath.at[rows_of(dp, small)]
    stage = copies(n_dp, lambda k: pltpu.make_async_remote_copy(mine, mine, send_c.at[k - 1], rcv_c.at[k - 1], device_id=to_dp(k), device_id_type=MESH_ID))
    for cp in stage:
        cp.wait()

    stage = copies(n_dap, lambda k: pltpu.make_async_remote_copy(gath, out.at[rows_of(dap, big)], send_d.at[k - 1], rcv_d.at[k - 1], device_id=to_dap(k), device_id_type=MESH_ID))
    out[rows_of(dap, big), :] = gath[:]
    for cp in stage:
        cp.wait()


def sum_grads(n_dp, n_dap, parts):
    big, small = PACK // n_dap, PACK // n_dap // n_dp
    dma = pltpu.SemaphoreType.DMA
    return pl.pallas_call(
        functools.partial(grads_kernel, n_dp, n_dap),
        out_shape=jax.ShapeDtypeStruct((PACK, LANES), F32),
        in_specs=[pl.BlockSpec(memory_space=pltpu.VMEM)] * len(parts),
        out_specs=pl.BlockSpec(memory_space=pltpu.VMEM),
        scratch_shapes=[pltpu.VMEM((PACK, LANES), F32), pltpu.VMEM((n_dap - 1, big, LANES), F32), pltpu.VMEM((big, LANES), F32), pltpu.VMEM((max(n_dp - 1, 1), small, LANES), F32), pltpu.VMEM((big, LANES), F32), pltpu.VMEM((384, LANES), F32)]
        + [dma((n_dap - 1,))] * 2 + [dma((max(n_dp - 1, 1),))] * 4 + [dma((n_dap - 1,))] * 2,
        name="grad_sum",
        cost_estimate=pl.CostEstimate(flops=MEGA, bytes_accessed=MIB, transcendentals=0),
        compiler_params=pltpu.CompilerParams(collective_id=0, has_side_effects=True),
    )(*parts)


def unpack_kernel(src, ln_in, gw, bp, lm, gwo, bo):
    t = jnp.transpose(src[0:6 * C, :])
    for k in range(2):
        gw[k] = t[k * C:(k + 1) * C, 0:5 * C]
        gwo[k] = t[k * C:(k + 1) * C, 5 * C:6 * C]
    base = 6 * C
    bp[:, 0:LANES] = src[base:base + 2, :]
    bp[:, LANES:W2] = src[base + RB:base + 18, :]
    bp[:, W2:320] = src[base + 32:base + 34, 0:C]
    for k in range(2):
        ln_in[k] = src[base + 2 + 2 * k:base + 4 + 2 * k, 0:C]
        lm[k] = src[base + 6 + 2 * k:base + 8 + 2 * k, 0:C]
    bo[:] = src[base + 10:base + 12, 0:C]


def unpack(flat):
    outs = [jax.ShapeDtypeStruct(s, F32) for s in ((2, 2, C), (2, C, 5 * C), (2, 5 * C), (2, 2, C), (2, C, C), (2, C))]
    return call(unpack_kernel, (1,), [full_spec(flat.shape)], [full_spec(o.shape) for o in outs], outs, [], MEGA, MIB)(flat)


SUM = sum_grads


def solution(mesh):
    def plan(z_pair, pair_mask, dz_out, ln_in, w_proj, b_proj, ln_mid, w_out, b_out):
        n = z_pair.shape[2]
        dap = lax.axis_index("dap")
        ids = jnp.stack([dap // 2, dap % 2]).astype(jnp.int32)
        x_pairs = [(0, 2), (2, 0), (1, 3), (3, 1)]
        c_pairs = [(0, 1), (1, 0), (2, 3), (3, 2)]

        def over_x(v):
            return lax.ppermute(v, "dap", x_pairs)

        def over_c(v):
            return lax.ppermute(v, "dap", c_pairs)

        lnmid = ln_mid.astype(F32)
        par = prepare(n, ids, lnmid, ln_in, w_proj, b_proj, w_out, b_out)
        m_own = pair_mask[0]
        z_own = jnp.transpose(z_pair[0], (0, 2, 1))
        dz_own = jnp.transpose(dz_out[0], (0, 2, 1))
        m_peer = over_x(m_own)
        z_peer = over_x(z_own)
        z_peer, dz_src = lax.optimization_barrier((z_peer, dz_own))
        dz_peer = over_x(dz_src)
        masks = (m_peer, m_own)

        ao, bo = pre_forward(z_own, m_own, par)
        qo, ro = over_c(bo), over_c(ao)
        ap, bp = pre_forward(z_peer, m_peer, par)
        qp, rp = over_c(bp), over_c(ap)
        z_mid, xn, rstd, a1, b1, a1k, a1s = fwd_fused(ids, (ap, ao, bp, bo, qp, qo), z_peer, z_own, masks, par, lnmid)
        a1r, b1p = over_c(a1s), over_c(b1)
        z_new, dx1, dpg1, bg1, bo1, wo1, mg1, mb1 = turn_fused(ids, (a1k, a1r, b1, b1p), z_mid, (dz_peer, dz_own), par, w_out, lnmid)
        dx1p = over_c(dx1)
        dz_mid, dx0, dx0k, dx0s, dpg0, w1, b1s, g1, lb1, bg0, bo0, wo0, mg0, mb0 = back_fused(ids, (a1, b1, dx1, dx1p), z_mid, dpg1, (dz_peer, dz_own), masks, xn, rstd, (z_peer, z_own), par, w_proj, w_out, lnmid)
        dx0r = over_c(dx0s)
        dz, w0, b0s, g0, lb0 = last_fused(ids, (dx0, bp, bo, qp, qo, dx0k, dx0r, ap, ao, rp, ro), z_own, dpg0, dz_mid, m_own, par, w_proj)

        flat = SUM(mesh.shape["dp"], mesh.shape["dap"], (w0, b0s, bg0, g0, lb0, wo0, bo0, mg0, mb0, w1, b1s, bg1, g1, lb1, wo1, bo1, mg1, mb1))
        g_ln_in, gw, g_bp, g_lm, gwo, g_bo = unpack(flat)
        z_res = jnp.transpose(z_new, (0, 2, 1))[None]
        dz_res = jnp.transpose(dz, (0, 2, 1))[None]
        return z_res, dz_res, g_ln_in, gw, g_bp, g_lm, gwo, g_bo

    row_spec = P("dp", "dap")
    return jax.shard_map(plan, mesh=mesh, in_specs=(row_spec, row_spec, row_spec, P(), P(), P(), P(), P(), P()), out_specs=(row_spec, row_spec, P(), P(), P(), P(), P(), P()), check_vma=False)
```

```python
import functools

import jax
import jax.numpy as jnp
from jax import lax
from jax.experimental import pallas as pl
from jax.experimental.pallas import tpu as pltpu
from jax.sharding import PartitionSpec as P


EPS = 1e-5
F32 = jnp.float32
BF16 = jnp.bfloat16
INTERPRET = False
C = 64
RB = 16
DELAY = 4
LANES = 128
W2 = 256
HALF = 0.5
MEGA = 10 ** 6
GIGA = 10 ** 9
MIB = 2 ** 20
VMEM_LIMIT = 67043328


MESH_ID = pl.DeviceIdType.MESH


def dot_nn(a, b):
    return lax.dot_general(a, b, (((1,), (0,)), ((), ())), preferred_element_type=F32)


def dot_nt(a, b):
    return lax.dot_general(a, b, (((1,), (1,)), ((), ())), preferred_element_type=F32)


def dot_tn(a, b):
    return lax.dot_general(a, b, (((0,), (0,)), ((), ())), preferred_element_type=F32)


def norm_rows(zf):
    mean = jnp.mean(zf, axis=0, keepdims=True)
    cen = zf - mean
    var = jnp.mean(cen * cen, axis=0, keepdims=True)
    rstd = lax.rsqrt(var + EPS)
    return cen * rstd, rstd


def staggered(first, second):
    for i in range(RB + DELAY):
        if i < RB:
            first(i)
        if i >= DELAY:
            second(i - DELAY)


def fold(v):
    return v[:, :LANES] + v[:, LANES:]


def to_cmajor(perm, src, dst):
    n = src.shape[-1]
    for grp in range(C // RB):
        blk = src[:, grp * RB:(grp + 1) * RB, :].reshape(W2, n)
        out = dot_nn(perm, blk)
        dst(grp, out.reshape(RB, RB, n))


def to_rows(perm, src, dst):
    n = src.shape[-1]
    for grp in range(C // RB):
        blk = src[grp * RB:(grp + 1) * RB, :, :].reshape(W2, n)
        out = dot_nn(perm, blk)
        dst[:, grp * RB:(grp + 1) * RB, :] = out.reshape(RB, RB, n).astype(BF16)


def split_cols(v, core):
    lo, hi = v[..., :LANES], v[..., LANES:]
    lane = lax.broadcasted_iota(jnp.int32, lo.shape, lo.ndim - 1)
    axis = lo.ndim - 1
    first = jnp.where(lane < C, lo, pltpu.roll(hi, C, axis))
    second = jnp.where(lane < C, pltpu.roll(lo, C, axis), hi)
    mine = jnp.where(core == 0, first, second)
    other = jnp.where(core == 0, second, first)
    return mine, other


KA = C + RB


def prep_kernel(ids, lnmid, w_proj, b_proj, ln_in, w_out, b_out, wt_aug, wot_aug, gain, lbias, perm, scr):
    n = gain.shape[-1]
    for k in range(2):
        scr[:] = jnp.zeros_like(scr)
        scr[0:C, 0:5 * C] = w_proj[k].astype(F32)
        scr[C:C + 1, 0:5 * C] = b_proj[pl.ds(k, 1), :]
        wt_aug[k] = (HALF * jnp.transpose(scr[:]))[0:5 * C, 0:KA].astype(BF16)
        scr[:] = jnp.zeros_like(scr)
        scr[0:C, 0:C] = w_out[k].astype(F32)
        scr[C:C + 1, 0:C] = b_out[pl.ds(k, 1), :]
        scr[C + 8:C + 10, 0:C] = ln_in[k]
        small = jnp.transpose(scr[:, 0:LANES])
        wot_aug[k] = (HALF * small)[0:C, 0:KA].astype(BF16)
        gain[k] = jnp.broadcast_to(small[0:C, C + 8:C + 9], (C, n))
        lbias[k] = jnp.broadcast_to(small[0:C, C + 9:C + 10], (C, n))
    r = lax.broadcasted_iota(jnp.int32, (W2, W2), 0)
    q = lax.broadcasted_iota(jnp.int32, (W2, W2), 1)
    perm[:] = jnp.where(q == RB * (r % RB) + r // RB, 1.0, 0.0).astype(BF16)


def prepare(n, ids, lnmid, ln_in, w_proj, b_proj, w_out, b_out):
    sds = jax.ShapeDtypeStruct
    outs = [sds((2, 5 * C, KA), BF16), sds((2, C, KA), BF16), sds((2, C, n), F32), sds((2, C, n), F32), sds((W2, W2), BF16)]
    args = (w_proj, b_proj.astype(F32), ln_in.astype(F32), w_out, b_out.astype(F32))
    return call(prep_kernel, (1,), [SMEM_SPEC, SMEM_SPEC] + [full_spec(v.shape) for v in args], [full_spec(o.shape) for o in outs], outs, [pltpu.VMEM((LANES, 384), F32)], MEGA, MIB)(ids, lnmid, *args)


def with_ones(zh):
    row = lax.broadcasted_iota(jnp.int32, (RB, zh.shape[-1]), 0)
    return jnp.concatenate([zh, jnp.where(row == 0, 1.0, 0.0).astype(BF16)], axis=0)


def pre_fwd_kernel(z, mask, wt, gain, lbias, perm, a, b, a_s, b_s):
    for i in range(RB):
        a_s[i], b_s[i] = project(z[i].astype(F32), mask[pl.ds(i, 1), :].astype(F32), wt, gain, lbias)

    def put_a(grp, v):
        a[grp * RB:(grp + 1) * RB] = v.astype(BF16)

    def put_b(grp, v):
        b[grp * RB:(grp + 1) * RB] = v.astype(BF16)

    to_cmajor(perm[:], a_s, put_a)
    to_cmajor(perm[:], b_s, put_b)


def full_spec(shape):
    return pl.BlockSpec(shape, lambda s: (0,) * len(shape))


SMEM_SPEC = pl.BlockSpec(memory_space=pltpu.SMEM)


def call(kernel, grid, in_specs, out_specs, out_shape, scratch, flops, bytes_accessed, trans=0):
    return pl.pallas_call(
        kernel,
        grid=grid,
        in_specs=in_specs,
        out_specs=out_specs,
        out_shape=out_shape,
        scratch_shapes=scratch,
        interpret=INTERPRET,
        cost_estimate=pl.CostEstimate(flops=flops, bytes_accessed=bytes_accessed, transcendentals=trans),
        compiler_params=pltpu.CompilerParams(dimension_semantics=("arbitrary",) * len(grid), vmem_limit_bytes=VMEM_LIMIT),
    )


def blk_spec(shape, k):
    return pl.BlockSpec((None,) + tuple(shape[1:]), lambda s: (k,) + (0,) * (len(shape) - 1))


def pre_forward(z, mask, par):
    rows, _, n = z.shape
    specs, args = weights_specs(par, 0, False)
    cspec = pl.BlockSpec((C, RB, n), lambda s: (0, s, 0))
    return call(
        pre_fwd_kernel, (rows // RB,),
        [pl.BlockSpec((RB, C, n), lambda s: (s, 0, 0)), pl.BlockSpec((RB, n), lambda s: (s, 0))] + specs + [full_spec((W2, W2))],
        [cspec] * 2, [jax.ShapeDtypeStruct((C, rows, n), BF16)] * 2, [pltpu.VMEM((RB, C, n), BF16)] * 2, GIGA, 8 * MIB)(z, mask, *args, par[-1])


CB = 16
T_STEPS = C // CB


def global_rows(ids, partner):
    x, c = ids[0], ids[1]
    cc = 1 - c if partner else c
    return pl.multiple_of(C * (2 * (1 - x) + cc), C), pl.multiple_of(C * (2 * x + cc), C)


def place(dst, src_mine, src_other, ids):
    for (peer, own), partner in ((src_mine, False), (src_other, True)):
        off_peer, off_own = global_rows(ids, partner)
        dst[pl.ds(off_peer, C), :] = peer
        dst[pl.ds(off_own, C), :] = own


def halves(ref):
    return ref[0:C, :], ref[C:LANES, :]


def tri_spec(shape, row_blk=0):
    return pl.BlockSpec((CB,) + tuple(shape[1:]), lambda s: (jnp.minimum(s, T_STEPS - 1), row_blk, 0))


def row_blk(s):
    return jnp.maximum(s - T_STEPS, 0)


def r_spec(n, off=0):
    return pl.BlockSpec((RB, C, n), lambda s: (row_blk(s) + off, 0, 0))


def c_spec(n):
    return pl.BlockSpec((C, RB, n), lambda s: (0, row_blk(s), 0))


def two_specs(shape):
    zeros = (0,) * (len(shape) - 1)
    return [pl.BlockSpec(shape, lambda s: (jnp.clip(s - T_STEPS, 0, 3),) + zeros), pl.BlockSpec(shape, lambda s: (jnp.maximum(s - T_STEPS - 4, 0),) + zeros)]


def m_spec(n):
    return pl.BlockSpec((RB, n), lambda s: (row_blk(s), 0))


def pick(own, peer_ref, own_ref, at):
    return (own_ref if own else peer_ref)[at]


def each_half(step, body):
    r = step - T_STEPS
    pl.when((r >= 0) & (r < 4))(lambda: body(r, False))
    pl.when(r >= 4)(lambda: body(r, True))


def channels(step):
    return [(ch, step * CB + ch) for ch in range(CB)]


def mid_norm(x, xh_s, lnmid, blk, xn_s, rstd_s):
    tot = x[0]
    for c in range(1, C):
        tot = tot + x[c]
    mean = tot * (1.0 / C)
    d = x[0] - mean
    sq = d * d
    for c in range(1, C):
        d = x[c] - mean
        sq = sq + d * d
    rstd = lax.rsqrt(sq * (1.0 / C) + EPS)
    rstd_s[:] = rstd
    for c in range(C):
        xn = (x[c] - mean) * rstd
        xn_s[c] = xn
        xh_s[c] = (xn * lnmid[blk, 0, c] + lnmid[blk, 1, c]).astype(BF16)


def gate_of(zf, wt, gain, lbias):
    zn, _ = norm_rows(zf)
    zh = (zn * gain[:] + lbias[:]).astype(BF16)
    return jnp.tanh(dot_nn(wt[4 * C:5 * C], with_ones(zh)))


def project(zf, m, wt, gain, lbias):
    zn, _ = norm_rows(zf)
    zh = (zn * gain[:] + lbias[:]).astype(BF16)
    p = dot_nn(wt[0:4 * C], with_ones(zh))
    a = ((1.0 + jnp.tanh(p[0:C])) * (p[C:2 * C] * m)).astype(BF16)
    b = ((1.0 + jnp.tanh(p[2 * C:3 * C])) * (p[3 * C:4 * C] * m)).astype(BF16)
    return a, b


def fwd_kernel(ids, ap, ao, bp, bo, qp, qo, zp, zo, mp, mo, wt0, gain0, lbias0, wot0, wt1, gain1, lbias1, lnmid, perm, zmid, xn, rstd, a1, b1, a1k, a1s, x_s, full, xh_s, xi_s, a_s, b_s):
    step = pl.program_id(0)

    @pl.when(step < T_STEPS)
    def _():
        for ch, dst in channels(step):
            buf = full.at[ch % 2]
            place(buf, (bp[ch], bo[ch]), (qp[ch], qo[ch]), ids)
            x_s[dst] = dot_nt(jnp.concatenate([ap[ch], ao[ch]], axis=0), buf[:])

    def body(r, own):
        mid_norm(x_s.at[:, pl.ds(pl.multiple_of(r * RB, RB), RB), :], xh_s, lnmid, 0, xn, rstd)
        to_rows(perm[:], xh_s, xi_s)

        def update(i):
            zf = pick(own, zp, zo, i).astype(F32)
            upd = dot_nn(wot0[:], with_ones(xi_s[i]))
            zmid[i] = (zf + (1.0 + gate_of(zf, wt0, gain0, lbias0)) * upd).astype(BF16)

        def sides(i):
            m = pick(own, mp, mo, (pl.ds(i, 1), slice(None))).astype(F32)
            a_s[i], b_s[i] = project(zmid[i].astype(F32), m, wt1, gain1, lbias1)

        staggered(update, sides)

        def put_a(grp, v):
            a1[grp * RB:(grp + 1) * RB] = v.astype(BF16)
            mine, other = split_cols(v, ids[1])
            a1k[grp * RB:(grp + 1) * RB] = mine.astype(BF16)
            a1s[grp * RB:(grp + 1) * RB] = other.astype(BF16)

        def put_b(grp, v):
            b1[grp * RB:(grp + 1) * RB] = v.astype(BF16)

        to_cmajor(perm[:], a_s, put_a)
        to_cmajor(perm[:], b_s, put_b)

    each_half(step, body)


def weights_specs(par, blk, with_out):
    wt, wot, gain, lbias, _ = par
    specs = [blk_spec(wt.shape, blk), blk_spec(gain.shape, blk), blk_spec(gain.shape, blk)]
    args = [wt, gain, lbias]
    if with_out:
        specs.append(blk_spec(wot.shape, blk))
        args.append(wot)
    return specs, args


def fwd_fused(ids, sides, zp, zo, masks, par, lnmid):
    n = zp.shape[-1]
    s0, w0 = weights_specs(par, 0, True)
    s1, w1 = weights_specs(par, 1, False)
    sds, vm = jax.ShapeDtypeStruct, pltpu.VMEM
    c_out, h_out = sds((C, LANES, n), BF16), sds((C, LANES, LANES), BF16)
    return call(
        fwd_kernel, (T_STEPS + 8,),
        [SMEM_SPEC] + [tri_spec(v.shape) for v in sides] + two_specs((RB, C, n)) + two_specs((RB, n)) + s0 + s1 + [SMEM_SPEC, full_spec((W2, W2))],
        [r_spec(n), c_spec(n), m_spec(n), c_spec(n), c_spec(n), c_spec(LANES), c_spec(LANES)],
        [sds((LANES, C, n), BF16), sds((C, LANES, n), F32), sds((LANES, n), F32), c_out, c_out, h_out, h_out],
        [vm((C, LANES, n), F32), vm((2, n, n), BF16), vm((C, RB, n), BF16), vm((RB, C, n), BF16), vm((RB, C, n), BF16), vm((RB, C, n), BF16)],
        GIGA, 40 * MIB)(ids, *sides, zp, zo, *masks, *w0, *w1, lnmid, par[-1])


def mid_back(own, dxc_s, xn, rstd, lnmid, blk, acc_mg, acc_mb, emit):
    m1 = m2 = None
    for c in range(C):
        dy = dxc_s[c]
        dyx = dy * xn[c]
        gn = lnmid[blk, 0, c]
        m1 = dy * gn if m1 is None else m1 + dy * gn
        m2 = dyx * gn if m2 is None else m2 + dyx * gn
        if own:
            acc_mg[c] += fold(dyx[0:8] + dyx[8:RB])
            acc_mb[c] += fold(dy[0:8] + dy[8:RB])
    m1 = m1 * (1.0 / C)
    m2 = m2 * (1.0 / C)
    for c in range(C):
        emit(c, rstd * (dxc_s[c] * lnmid[blk, 0, c] - m1 - xn[c] * m2))


def clear(step, accs):
    @pl.when(step == 0)
    def _():
        for acc in accs:
            acc[:] = jnp.zeros_like(acc)


def turn_kernel(ids, ak, ar, b, bq, z, dzp, dzo, wt, gain, lbias, wot, wo, lnmid, perm, znew, dx, dpg, acc_bg, acc_bo, acc_wo, acc_mg, acc_mb, x_s, xh_s, xi_s, dxi_s, dub_s, dxc_s, xn_s, r_s):
    step = pl.program_id(0)
    xx = ids[0]
    clear(step, (acc_bg, acc_bo, acc_wo, acc_mg, acc_mb))

    @pl.when(step < T_STEPS)
    def _():
        for ch, dst in channels(step):
            out = dot_tn(ak[ch], b[ch]) + dot_tn(ar[ch], bq[ch])
            x_s[dst, pl.ds(pl.multiple_of(C * (1 - xx), C), C), :] = out[0:C]
            x_s[dst, pl.ds(pl.multiple_of(C * xx, C), C), :] = out[C:LANES]

    def body(r, own):
        mid_norm(x_s.at[:, pl.ds(pl.multiple_of(r * RB, RB), RB), :], xh_s, lnmid, 1, xn_s, r_s)
        to_rows(perm[:], xh_s, xi_s)
        sums = [acc_bg[:], acc_bo[:], acc_wo[:]]

        def gates(i):
            zf = z[i].astype(F32)
            dz = pick(own, dzp, dzo, i).astype(F32)
            t = gate_of(zf, wt, gain, lbias)
            upd = dot_nn(wot[:], with_ones(xi_s[i]))
            t1 = 1.0 + t
            if own:
                znew[i] = (zf + t1 * upd).astype(BF16)
            d_upd = (HALF * dz) * t1
            d_pg = d_upd * (upd * (1.0 - t))
            dpg[i] = d_pg.astype(BF16)
            dub_s[i] = d_upd.astype(BF16)
            if own:
                sums[0] += fold(d_pg)
                sums[1] += fold(d_upd)

        def products(i):
            dxi_s[i] = dot_nn(wo[:], dub_s[i]).astype(BF16)
            if own:
                sums[2] += dot_nt(dub_s[i], xi_s[i])

        staggered(gates, products)
        if own:
            acc_bg[:], acc_bo[:], acc_wo[:] = sums

        def put(grp, v):
            dxc_s[grp * RB:(grp + 1) * RB] = v

        to_cmajor(perm[:], dxi_s, put)

        def emit(c, v):
            dx[c] = v.astype(BF16)

        mid_back(own, dxc_s, xn_s, r_s[:], lnmid, 1, acc_mg, acc_mb, emit)

    each_half(step, body)


ACC_POST = ((C, LANES), (C, LANES), (C, C), (C, 8, LANES), (C, 8, LANES))
ACC_PRE = ((5 * C, C), (4 * C, LANES), (C, LANES), (C, LANES))


def turn_fused(ids, sides, z_mid, dz_parts, par, w_out, lnmid):
    n = z_mid.shape[-1]
    s1, w1 = weights_specs(par, 1, True)
    sds, vm = jax.ShapeDtypeStruct, pltpu.VMEM
    return call(
        turn_kernel, (T_STEPS + 8,),
        [SMEM_SPEC] + [tri_spec(v.shape) for v in sides] + [r_spec(n)] + two_specs((RB, C, n)) + s1 + [blk_spec(w_out.shape, 1), SMEM_SPEC, full_spec((W2, W2))],
        [two_specs((RB, C, n))[1], c_spec(n), r_spec(n)] + [full_spec(s) for s in ACC_POST],
        [sds((C, C, n), BF16), sds((C, LANES, n), BF16), sds((LANES, C, n), BF16)] + [sds(s, F32) for s in ACC_POST],
        [vm((C, LANES, n), F32), vm((C, RB, n), BF16)] + [vm((RB, C, n), BF16)] * 3 + [vm((C, RB, n), F32)] * 2 + [vm((RB, n), F32)],
        GIGA, 40 * MIB)(ids, *sides, z_mid, *dz_parts, *w1, w_out, lnmid, par[-1])


def pre_back_stages(own, z, dpg, mask_of, res_of, dst, wt, w, gain, lbias, dai_s, dbi_s, dp_s, zh_s, zn_s, rs_s, acc_b, sums):
    def gates(i):
        zn, rstd = norm_rows(z[i].astype(F32))
        zn_s[i] = zn
        rs_s[i] = jnp.broadcast_to(rstd, (8, rstd.shape[-1]))
        zh = (zn * gain[:] + lbias[:]).astype(BF16)
        zh_s[i] = zh
        p = dot_nn(wt[0:4 * C], with_ones(zh))
        m = HALF * mask_of(i).astype(F32)
        for side, ref in ((0, dai_s), (1, dbi_s)):
            base = side * 2 * C
            dm = ref[i].astype(F32) * m
            t = jnp.tanh(p[base:base + C])
            dv = dm * (1.0 + t)
            dg = dv * (p[base + C:base + 2 * C] * (1.0 - t))
            for k, d in ((2 * side, dg), (2 * side + 1, dv)):
                if own:
                    acc_b[k * C:(k + 1) * C] += fold(d)
                dp_s[i, k * C:(k + 1) * C] = d.astype(BF16)
        dp_s[i, 4 * C:5 * C] = dpg[i]

    def products(i):
        dp = dp_s[i]
        dzh = dot_nn(w[:], dp).astype(BF16).astype(F32)
        zn, rstd = zn_s[i], rs_s[i, 0:1, :]
        if own:
            sums[0] += dot_nt(dp, zh_s[i])
            sums[1] += fold(dzh * zn)
            sums[2] += fold(dzh)
        dzn = dzh * gain[:]
        m1 = jnp.mean(dzn, axis=0, keepdims=True)
        m2 = jnp.mean(dzn * zn, axis=0, keepdims=True)
        dst[i] = (res_of(i).astype(F32) + rstd * (dzn - m1 - zn * m2)).astype(BF16)

    return gates, products


def back_kernel(ids, a, b, dx, dxq, z, dpg1, dzp, dzo, mp, mo, xn, rstd, zp, zo, wt1, gain1, lbias1, w1, wt0, gain0, lbias0, wot0, wo0, lnmid, perm, dzm, dx0, dxk, dxs, dpg0, acc_w, acc_b, acc_g, acc_lb, acc_bg, acc_bo, acc_wo, acc_mg, acc_mb, da_s, db_s, full, dai_s, dbi_s, dp_s, zh_s, zn_s, rs_s, xh_s, xi_s, dxi_s, dub_s, dxc_s):
    step = pl.program_id(0)
    clear(step, (acc_w, acc_b, acc_g, acc_lb, acc_bg, acc_bo, acc_wo, acc_mg, acc_mb))

    @pl.when(step < T_STEPS)
    def _():
        for ch, dst in channels(step):
            buf = full.at[ch % 2]
            place(buf, halves(dx.at[ch]), halves(dxq.at[ch]), ids)
            da_s[dst] = dot_nt(b[ch], buf[:]).astype(BF16)
            db_s[dst] = dot_nn(a[ch], buf[:]).astype(BF16)

    def body(r, own):
        rows = pl.ds(pl.multiple_of(r * RB, RB), RB)
        to_rows(perm[:], da_s.at[:, rows, :], dai_s)
        to_rows(perm[:], db_s.at[:, rows, :], dbi_s)
        for c in range(C):
            xh_s[c] = (xn[c] * lnmid[0, 0, c] + lnmid[0, 1, c]).astype(BF16)
        to_rows(perm[:], xh_s, xi_s)
        pre = [acc_w[:], acc_g[:], acc_lb[:]]
        pre_gates, pre_products = pre_back_stages(
            own, z, dpg1, lambda i: pick(own, mp, mo, (pl.ds(i, 1), slice(None))), lambda i: pick(own, dzp, dzo, i), dzm,
            wt1, w1, gain1, lbias1, dai_s, dbi_s, dp_s, zh_s, zn_s, rs_s, acc_b, pre)
        staggered(pre_gates, pre_products)
        if own:
            acc_w[:], acc_g[:], acc_lb[:] = pre
        post = [acc_bg[:], acc_bo[:], acc_wo[:]]

        def gates(i):
            t = gate_of(pick(own, zp, zo, i).astype(F32), wt0, gain0, lbias0)
            upd = dot_nn(wot0[:], with_ones(xi_s[i]))
            d_upd = (HALF * dzm[i].astype(F32)) * (1.0 + t)
            d_pg = d_upd * (upd * (1.0 - t))
            dpg0[i] = d_pg.astype(BF16)
            dub_s[i] = d_upd.astype(BF16)
            if own:
                post[0] += fold(d_pg)
                post[1] += fold(d_upd)

        def products(i):
            dxi_s[i] = dot_nn(wo0[:], dub_s[i]).astype(BF16)
            if own:
                post[2] += dot_nt(dub_s[i], xi_s[i])

        staggered(gates, products)
        if own:
            acc_bg[:], acc_bo[:], acc_wo[:] = post

        def put(grp, v):
            dxc_s[grp * RB:(grp + 1) * RB] = v

        to_cmajor(perm[:], dxi_s, put)

        def emit(c, v):
            dx0[c] = v.astype(BF16)
            mine, other = split_cols(v, ids[1])
            dxk[c] = mine.astype(BF16)
            dxs[c] = other.astype(BF16)

        mid_back(own, dxc_s, xn, rstd[:], lnmid, 0, acc_mg, acc_mb, emit)

    each_half(step, body)


def back_fused(ids, sides, z_mid, dpg1, dz_parts, masks, xn, rstd, z_parts, par, w_proj, w_out, lnmid):
    n = z_mid.shape[-1]
    s1, w1 = weights_specs(par, 1, False)
    s0, w0 = weights_specs(par, 0, True)
    sds, vm = jax.ShapeDtypeStruct, pltpu.VMEM
    two = two_specs((RB, C, n))
    rows = vm((RB, C, n), BF16)
    accs = ACC_PRE + ACC_POST
    return call(
        back_kernel, (T_STEPS + 8,),
        [SMEM_SPEC] + [tri_spec(v.shape) for v in sides] + [r_spec(n), r_spec(n)] + two + two_specs((RB, n)) + [c_spec(n), m_spec(n)] + two
        + s1 + [blk_spec(w_proj.shape, 1)] + s0 + [blk_spec(w_out.shape, 0), SMEM_SPEC, full_spec((W2, W2))],
        [two[1], c_spec(n), c_spec(LANES), c_spec(LANES), r_spec(n)] + [full_spec(s) for s in accs],
        [sds((C, C, n), BF16), sds((C, LANES, n), BF16), sds((C, LANES, LANES), BF16), sds((C, LANES, LANES), BF16), sds((LANES, C, n), BF16)] + [sds(s, F32) for s in accs],
        [vm((C, LANES, n), BF16)] * 2 + [vm((2, n, n), BF16), rows, rows, vm((RB, 5 * C, n), BF16), rows, vm((RB, C, n), F32), vm((RB, 8, n), F32), vm((C, RB, n), BF16), rows, rows, rows, vm((C, RB, n), F32)],
        GIGA, 60 * MIB)(ids, *sides, z_mid, dpg1, *dz_parts, *masks, xn, rstd, *z_parts, *w1, w_proj, *w0, w_out, lnmid, par[-1])


def last_kernel(ids, dx, bp, bo, qp, qo, dxk, dxr, ap, ao, rp, ro, z, dpg, dres, mask, wt, gain, lbias, w, perm, dz, acc_w, acc_b, acc_g, acc_lb, da_s, db_s, full, tmp, dai_s, dbi_s, dp_s, zh_s, zn_s, rs_s):
    step = pl.program_id(0)
    xx = ids[0]
    clear(step, (acc_w, acc_b, acc_g, acc_lb))

    @pl.when(step < T_STEPS)
    def _():
        for ch, dst in channels(step):
            buf = full.at[ch % 2]
            place(buf, (bp[ch], bo[ch]), (qp[ch], qo[ch]), ids)
            da_s[dst] = dot_nn(dx[ch], buf[:]).astype(BF16)
            tmp[ch % 2] = dot_tn(dxk[ch], jnp.concatenate([ap[ch], ao[ch]], axis=0)) + dot_tn(dxr[ch], jnp.concatenate([rp[ch], ro[ch]], axis=0))
            db_s[dst] = tmp[ch % 2, pl.ds(pl.multiple_of(C * xx, C), C), :].astype(BF16)

    @pl.when(step >= T_STEPS)
    def _():
        rows = pl.ds(pl.multiple_of((step - T_STEPS) * RB, RB), RB)
        to_rows(perm[:], da_s.at[:, rows, :], dai_s)
        to_rows(perm[:], db_s.at[:, rows, :], dbi_s)
        sums = [acc_w[:], acc_g[:], acc_lb[:]]
        staggered(*pre_back_stages(
            True, z, dpg, lambda i: mask[pl.ds(i, 1), :], lambda i: dres[i], dz,
            wt, w, gain, lbias, dai_s, dbi_s, dp_s, zh_s, zn_s, rs_s, acc_b, sums))
        acc_w[:], acc_g[:], acc_lb[:] = sums


def last_fused(ids, sides, z, dpg, dres, mask, par, w_proj):
    n = z.shape[-1]
    s0, w0 = weights_specs(par, 0, False)
    sds, vm = jax.ShapeDtypeStruct, pltpu.VMEM
    rows = vm((RB, C, n), BF16)
    return call(
        last_kernel, (T_STEPS + 4,),
        [SMEM_SPEC, tri_spec((C, C, n), 1)] + [tri_spec(v.shape) for v in sides[1:]] + [r_spec(n), r_spec(n, 4), r_spec(n), m_spec(n)] + s0 + [blk_spec(w_proj.shape, 0), full_spec((W2, W2))],
        [r_spec(n)] + [full_spec(s) for s in ACC_PRE],
        [sds((C, C, n), BF16)] + [sds(s, F32) for s in ACC_PRE],
        [vm((C, C, n), BF16)] * 2 + [vm((2, n, n), BF16), vm((2, LANES, n), F32), rows, rows, vm((RB, 5 * C, n), BF16), rows, vm((RB, C, n), F32), vm((RB, 8, n), F32)],
        GIGA, 40 * MIB)(ids, *sides, z, dpg, dres, mask, *w0, w_proj, par[-1])


PACK = 512


def grads_kernel(n_dp, n_dap, w0, b0, q0, g0, l0, wo0, o0, mg0, mb0, w1, b1, q1, g1, l1, wo1, o1, mg1, mb1, out, buf, recv_a, red, recv_b, gath, vec, send_a, rcv_a, send_b, rcv_b, send_c, rcv_c, send_d, rcv_d):
    dp, dap = lax.axis_index("dp"), lax.axis_index("dap")
    big, small = PACK // n_dap, PACK // n_dap // n_dp
    bar = pltpu.get_barrier_semaphore()
    for k in range(1, n_dap):
        pl.semaphore_signal(bar, inc=1, device_id=(dp, lax.rem(dap + k, n_dap)), device_id_type=MESH_ID)
    for k in range(1, n_dp):
        pl.semaphore_signal(bar, inc=1, device_id=(lax.rem(dp + k, n_dp), dap), device_id_type=MESH_ID)

    buf[0:5 * C, 0:C] = w0[:]
    buf[0:5 * C, C:2 * C] = w1[:]
    buf[5 * C:6 * C, 0:C] = wo0[:]
    buf[5 * C:6 * C, C:2 * C] = wo1[:]

    def put(k, base, ref):
        v = ref[:]
        if v.ndim == 3:
            v = jnp.sum(v, axis=1)
        rows = v.shape[0]
        tot = jnp.sum(v, axis=1, keepdims=True)
        lane = lax.broadcasted_iota(jnp.int32, (rows, LANES), 1)
        vec[base:base + rows, :] = jnp.where(lane == k, tot, vec[base:base + rows, :])

    vec[:] = jnp.zeros_like(vec)
    put(0, 0, b0)
    put(0, 4 * C, q0)
    put(1, 0, b1)
    put(1, 4 * C, q1)
    for k, ref in enumerate((g0, l0, g1, l1, mg0, mb0, mg1, mb1, o0, o1)):
        put(2 + k, 0, ref)
    vt = jnp.transpose(vec[:])
    for t in range(3):
        buf[6 * C + RB * t:6 * C + RB * t + RB, :] = vt[0:RB, LANES * t:LANES * (t + 1)]
    buf[6 * C + 48:PACK, :] = jnp.zeros((PACK - 6 * C - 48, LANES), F32)

    pl.semaphore_wait(bar, n_dap + n_dp - 2)

    def copies(count, make):
        made = [make(k) for k in range(1, count)]
        for cp in made:
            cp.start()
        return made

    def to_dap(k):
        return (dp, lax.rem(dap + k, n_dap))

    def to_dp(k):
        return (lax.rem(dp + k, n_dp), dap)

    def rows_of(idx, size):
        return pl.ds(pl.multiple_of(idx * size, size), size)

    stage = copies(n_dap, lambda k: pltpu.make_async_remote_copy(buf.at[rows_of(lax.rem(dap + k, n_dap), big)], recv_a.at[k - 1], send_a.at[k - 1], rcv_a.at[k - 1], device_id=to_dap(k), device_id_type=MESH_ID))
    tot = buf[rows_of(dap, big), :]
    for k, cp in enumerate(stage):
        cp.wait_recv()
        tot = tot + recv_a[k]
    red[:] = tot
    for cp in stage:
        cp.wait_send()

    stage = copies(n_dp, lambda k: pltpu.make_async_remote_copy(red.at[rows_of(lax.rem(dp + k, n_dp), small)], recv_b.at[k - 1], send_b.at[k - 1], rcv_b.at[k - 1], device_id=to_dp(k), device_id_type=MESH_ID))
    tot = red[rows_of(dp, small), :]
    for k, cp in enumerate(stage):
        cp.wait_recv()
        tot = tot + recv_b[k]
    gath[rows_of(dp, small), :] = tot
    for cp in stage:
        cp.wait_send()

    mine = gath.at[rows_of(dp, small)]
    stage = copies(n_dp, lambda k: pltpu.make_async_remote_copy(mine, mine, send_c.at[k - 1], rcv_c.at[k - 1], device_id=to_dp(k), device_id_type=MESH_ID))
    for cp in stage:
        cp.wait()

    stage = copies(n_dap, lambda k: pltpu.make_async_remote_copy(gath, out.at[rows_of(dap, big)], send_d.at[k - 1], rcv_d.at[k - 1], device_id=to_dap(k), device_id_type=MESH_ID))
    out[rows_of(dap, big), :] = gath[:]
    for cp in stage:
        cp.wait()


def sum_grads(n_dp, n_dap, parts):
    big, small = PACK // n_dap, PACK // n_dap // n_dp
    dma = pltpu.SemaphoreType.DMA
    return pl.pallas_call(
        functools.partial(grads_kernel, n_dp, n_dap),
        out_shape=jax.ShapeDtypeStruct((PACK, LANES), F32),
        in_specs=[pl.BlockSpec(memory_space=pltpu.VMEM)] * len(parts),
        out_specs=pl.BlockSpec(memory_space=pltpu.VMEM),
        scratch_shapes=[pltpu.VMEM((PACK, LANES), F32), pltpu.VMEM((n_dap - 1, big, LANES), F32), pltpu.VMEM((big, LANES), F32), pltpu.VMEM((max(n_dp - 1, 1), small, LANES), F32), pltpu.VMEM((big, LANES), F32), pltpu.VMEM((384, LANES), F32)]
        + [dma((n_dap - 1,))] * 2 + [dma((max(n_dp - 1, 1),))] * 4 + [dma((n_dap - 1,))] * 2,
        name="grad_sum",
        cost_estimate=pl.CostEstimate(flops=MEGA, bytes_accessed=MIB, transcendentals=0),
        compiler_params=pltpu.CompilerParams(collective_id=0, has_side_effects=True),
    )(*parts)


def unpack_kernel(src, ln_in, gw, bp, lm, gwo, bo):
    t = jnp.transpose(src[0:6 * C, :])
    for k in range(2):
        gw[k] = t[k * C:(k + 1) * C, 0:5 * C]
        gwo[k] = t[k * C:(k + 1) * C, 5 * C:6 * C]
    base = 6 * C
    bp[:, 0:LANES] = src[base:base + 2, :]
    bp[:, LANES:W2] = src[base + RB:base + 18, :]
    bp[:, W2:320] = src[base + 32:base + 34, 0:C]
    for k in range(2):
        ln_in[k] = src[base + 2 + 2 * k:base + 4 + 2 * k, 0:C]
        lm[k] = src[base + 6 + 2 * k:base + 8 + 2 * k, 0:C]
    bo[:] = src[base + 10:base + 12, 0:C]


def unpack(flat):
    outs = [jax.ShapeDtypeStruct(s, F32) for s in ((2, 2, C), (2, C, 5 * C), (2, 5 * C), (2, 2, C), (2, C, C), (2, C))]
    return call(unpack_kernel, (1,), [full_spec(flat.shape)], [full_spec(o.shape) for o in outs], outs, [], MEGA, MIB)(flat)


SUM = sum_grads


def solution(mesh):
    def plan(z_pair, pair_mask, dz_out, ln_in, w_proj, b_proj, ln_mid, w_out, b_out):
        n = z_pair.shape[2]
        dap = lax.axis_index("dap")
        ids = jnp.stack([dap // 2, dap % 2]).astype(jnp.int32)
        x_pairs = [(0, 2), (2, 0), (1, 3), (3, 1)]
        c_pairs = [(0, 1), (1, 0), (2, 3), (3, 2)]

        def over_x(v):
            return lax.ppermute(v, "dap", x_pairs)

        def over_c(v):
            return lax.ppermute(v, "dap", c_pairs)

        lnmid = ln_mid.astype(F32)
        par = prepare(n, ids, lnmid, ln_in, w_proj, b_proj, w_out, b_out)
        m_own = pair_mask[0]
        z_own = jnp.transpose(z_pair[0], (0, 2, 1))
        dz_own = jnp.transpose(dz_out[0], (0, 2, 1))
        m_peer = over_x(m_own)
        z_peer = over_x(z_own)
        z_peer, dz_src = lax.optimization_barrier((z_peer, dz_own))
        dz_peer = over_x(dz_src)
        masks = (m_peer, m_own)

        ao, bo = pre_forward(z_own, m_own, par)
        qo, ro = over_c(bo), over_c(ao)
        ap, bp = pre_forward(z_peer, m_peer, par)
        qp, rp = over_c(bp), over_c(ap)
        z_mid, xn, rstd, a1, b1, a1k, a1s = fwd_fused(ids, (ap, ao, bp, bo, qp, qo), z_peer, z_own, masks, par, lnmid)
        a1r, b1p = over_c(a1s), over_c(b1)
        z_new, dx1, dpg1, bg1, bo1, wo1, mg1, mb1 = turn_fused(ids, (a1k, a1r, b1, b1p), z_mid, (dz_peer, dz_own), par, w_out, lnmid)
        dx1p = over_c(dx1)
        dz_mid, dx0, dx0k, dx0s, dpg0, w1, b1s, g1, lb1, bg0, bo0, wo0, mg0, mb0 = back_fused(ids, (a1, b1, dx1, dx1p), z_mid, dpg1, (dz_peer, dz_own), masks, xn, rstd, (z_peer, z_own), par, w_proj, w_out, lnmid)
        dx0r = over_c(dx0s)
        dz, w0, b0s, g0, lb0 = last_fused(ids, (dx0, bp, bo, qp, qo, dx0k, dx0r, ap, ao, rp, ro), z_own, dpg0, dz_mid, m_own, par, w_proj)

        flat = SUM(mesh.shape["dp"], mesh.shape["dap"], (w0, b0s, bg0, g0, lb0, wo0, bo0, mg0, mb0, w1, b1s, bg1, g1, lb1, wo1, bo1, mg1, mb1))
        g_ln_in, gw, g_bp, g_lm, gwo, g_bo = unpack(flat)
        z_res = jnp.transpose(z_new, (0, 2, 1))[None]
        dz_res = jnp.transpose(dz, (0, 2, 1))[None]
        return z_res, dz_res, g_ln_in, gw, g_bp, g_lm, gwo, g_bo

    row_spec = P("dp", "dap")
    return jax.shard_map(plan, mesh=mesh, in_specs=(row_spec, row_spec, row_spec, P(), P(), P(), P(), P(), P()), out_specs=(row_spec, row_spec, P(), P(), P(), P(), P(), P()), check_vma=False)
```

```python
import functools

import jax
import jax.numpy as jnp
from jax import lax
from jax.experimental import pallas as pl
from jax.experimental.pallas import tpu as pltpu
from jax.sharding import PartitionSpec as P


EPS = 1e-5
F32 = jnp.float32
BF16 = jnp.bfloat16
INTERPRET = False
C = 64
RB = 16
DELAY = 4
LANES = 128
W2 = 256
HALF = 0.5
MEGA = 10 ** 6
GIGA = 10 ** 9
MIB = 2 ** 20
VMEM_LIMIT = 67043328


MESH_ID = pl.DeviceIdType.MESH


def dot_nn(a, b):
    return lax.dot_general(a, b, (((1,), (0,)), ((), ())), preferred_element_type=F32)


def dot_nt(a, b):
    return lax.dot_general(a, b, (((1,), (1,)), ((), ())), preferred_element_type=F32)


def dot_tn(a, b):
    return lax.dot_general(a, b, (((0,), (0,)), ((), ())), preferred_element_type=F32)


def norm_rows(zf):
    mean = jnp.mean(zf, axis=0, keepdims=True)
    cen = zf - mean
    var = jnp.mean(cen * cen, axis=0, keepdims=True)
    rstd = lax.rsqrt(var + EPS)
    return cen * rstd, rstd


def staggered(first, second):
    for i in range(RB + DELAY):
        if i < RB:
            first(i)
        if i >= DELAY:
            second(i - DELAY)


def fold(v):
    return v[:, :LANES] + v[:, LANES:]


def to_cmajor(perm, src, dst):
    n = src.shape[-1]
    for grp in range(C // RB):
        blk = src[:, grp * RB:(grp + 1) * RB, :].reshape(W2, n)
        out = dot_nn(perm, blk)
        dst(grp, out.reshape(RB, RB, n))


def to_rows(perm, src, dst):
    n = src.shape[-1]
    for grp in range(C // RB):
        blk = src[grp * RB:(grp + 1) * RB, :, :].reshape(W2, n)
        out = dot_nn(perm, blk)
        dst[:, grp * RB:(grp + 1) * RB, :] = out.reshape(RB, RB, n).astype(BF16)


def split_cols(v, core):
    lo, hi = v[..., :LANES], v[..., LANES:]
    lane = lax.broadcasted_iota(jnp.int32, lo.shape, lo.ndim - 1)
    axis = lo.ndim - 1
    first = jnp.where(lane < C, lo, pltpu.roll(hi, C, axis))
    second = jnp.where(lane < C, pltpu.roll(lo, C, axis), hi)
    mine = jnp.where(core == 0, first, second)
    other = jnp.where(core == 0, second, first)
    return mine, other


KA = C + RB


def prep_kernel(ids, lnmid, w_proj, b_proj, ln_in, w_out, b_out, wt_aug, wot_aug, gain, lbias, perm, scr):
    n = gain.shape[-1]
    for k in range(2):
        scr[:] = jnp.zeros_like(scr)
        scr[0:C, 0:5 * C] = w_proj[k].astype(F32)
        scr[C:C + 1, 0:5 * C] = b_proj[pl.ds(k, 1), :]
        wt_aug[k] = (HALF * jnp.transpose(scr[:]))[0:5 * C, 0:KA].astype(BF16)
        scr[:] = jnp.zeros_like(scr)
        scr[0:C, 0:C] = w_out[k].astype(F32)
        scr[C:C + 1, 0:C] = b_out[pl.ds(k, 1), :]
        scr[C + 8:C + 10, 0:C] = ln_in[k]
        small = jnp.transpose(scr[:, 0:LANES])
        wot_aug[k] = (HALF * small)[0:C, 0:KA].astype(BF16)
        gain[k] = jnp.broadcast_to(small[0:C, C + 8:C + 9], (C, n))
        lbias[k] = jnp.broadcast_to(small[0:C, C + 9:C + 10], (C, n))
    r = lax.broadcasted_iota(jnp.int32, (W2, W2), 0)
    q = lax.broadcasted_iota(jnp.int32, (W2, W2), 1)
    perm[:] = jnp.where(q == RB * (r % RB) + r // RB, 1.0, 0.0).astype(BF16)


def prepare(n, ids, lnmid, ln_in, w_proj, b_proj, w_out, b_out):
    sds = jax.ShapeDtypeStruct
    outs = [sds((2, 5 * C, KA), BF16), sds((2, C, KA), BF16), sds((2, C, n), F32), sds((2, C, n), F32), sds((W2, W2), BF16)]
    args = (w_proj, b_proj.astype(F32), ln_in.astype(F32), w_out, b_out.astype(F32))
    return call(prep_kernel, (1,), [SMEM_SPEC, SMEM_SPEC] + [full_spec(v.shape) for v in args], [full_spec(o.shape) for o in outs], outs, [pltpu.VMEM((LANES, 384), F32)], MEGA, MIB)(ids, lnmid, *args)


def with_ones(zh):
    row = lax.broadcasted_iota(jnp.int32, (RB, zh.shape[-1]), 0)
    return jnp.concatenate([zh, jnp.where(row == 0, 1.0, 0.0).astype(BF16)], axis=0)


def pre_fwd_kernel(z, mask, wt, gain, lbias, perm, a, b, a_s, b_s):
    for i in range(RB):
        a_s[i], b_s[i] = project(z[i].astype(F32), mask[pl.ds(i, 1), :].astype(F32), wt, gain, lbias)

    def put_a(grp, v):
        a[grp * RB:(grp + 1) * RB] = v.astype(BF16)

    def put_b(grp, v):
        b[grp * RB:(grp + 1) * RB] = v.astype(BF16)

    to_cmajor(perm[:], a_s, put_a)
    to_cmajor(perm[:], b_s, put_b)


def full_spec(shape):
    return pl.BlockSpec(shape, lambda s: (0,) * len(shape))


SMEM_SPEC = pl.BlockSpec(memory_space=pltpu.SMEM)


def call(kernel, grid, in_specs, out_specs, out_shape, scratch, flops, bytes_accessed, remote=None):
    return pl.pallas_call(
        kernel,
        grid=grid,
        in_specs=in_specs,
        out_specs=out_specs,
        out_shape=out_shape,
        scratch_shapes=scratch,
        interpret=INTERPRET,
        cost_estimate=pl.CostEstimate(flops=flops, bytes_accessed=bytes_accessed, transcendentals=0),
        compiler_params=pltpu.CompilerParams(dimension_semantics=("arbitrary",) * len(grid), vmem_limit_bytes=VMEM_LIMIT, collective_id=remote, has_side_effects=remote is not None),
    )


def blk_spec(shape, k):
    return pl.BlockSpec((None,) + tuple(shape[1:]), lambda s: (k,) + (0,) * (len(shape) - 1))


def pre_forward(z, mask, par):
    rows, _, n = z.shape
    specs, args = weights_specs(par, 0, False)
    cspec = pl.BlockSpec((C, RB, n), lambda s: (0, s, 0))
    return call(
        pre_fwd_kernel, (rows // RB,),
        [pl.BlockSpec((RB, C, n), lambda s: (s, 0, 0)), pl.BlockSpec((RB, n), lambda s: (s, 0))] + specs + [full_spec((W2, W2))],
        [cspec] * 2, [jax.ShapeDtypeStruct((C, rows, n), BF16)] * 2, [pltpu.VMEM((RB, C, n), BF16)] * 2, GIGA, 8 * MIB)(z, mask, *args, par[-1])


CB = 16
T_STEPS = C // CB


def global_rows(ids, partner):
    x, c = ids[0], ids[1]
    cc = 1 - c if partner else c
    return pl.multiple_of(C * (2 * (1 - x) + cc), C), pl.multiple_of(C * (2 * x + cc), C)


def place(dst, src_mine, src_other, ids):
    for (peer, own), partner in ((src_mine, False), (src_other, True)):
        off_peer, off_own = global_rows(ids, partner)
        dst[pl.ds(off_peer, C), :] = peer
        dst[pl.ds(off_own, C), :] = own


def halves(ref):
    return ref[0:C, :], ref[C:LANES, :]


def tri_spec(shape, row_blk=0):
    return pl.BlockSpec((CB,) + tuple(shape[1:]), lambda s: (jnp.minimum(s, T_STEPS - 1), row_blk, 0))


def row_blk(s):
    return jnp.maximum(s - T_STEPS, 0)


def r_spec(n, off=0):
    return pl.BlockSpec((RB, C, n), lambda s: (row_blk(s) + off, 0, 0))


def c_spec(n):
    return pl.BlockSpec((C, RB, n), lambda s: (0, row_blk(s), 0))


def two_specs(shape):
    zeros = (0,) * (len(shape) - 1)
    return [pl.BlockSpec(shape, lambda s: (jnp.clip(s - T_STEPS, 0, 3),) + zeros), pl.BlockSpec(shape, lambda s: (jnp.maximum(s - T_STEPS - 4, 0),) + zeros)]


def m_spec(n):
    return pl.BlockSpec((RB, n), lambda s: (row_blk(s), 0))


def pick(own, peer_ref, own_ref, at):
    return (own_ref if own else peer_ref)[at]


def each_half(step, body):
    r = step - T_STEPS
    pl.when((r >= 0) & (r < 4))(lambda: body(r, False))
    pl.when(r >= 4)(lambda: body(r, True))


def here():
    dap = lax.axis_index("dap")
    return dap // 2, dap % 2


def from_partner(step, pairs, send, recv):
    dp, dap = lax.axis_index("dp"), lax.axis_index("dap")
    other = (dp, dap + 1 - 2 * (dap % 2))

    def copy(k, t):
        src, dst = pairs[k]
        blk = pl.ds(pl.multiple_of(t * CB, CB), CB)
        return pltpu.make_async_remote_copy(src.at[blk], dst.at[blk], send.at[k, t], recv.at[k, t], device_id=other, device_id_type=MESH_ID)

    @pl.when(step == 0)
    def _():
        bar = pltpu.get_barrier_semaphore()
        pl.semaphore_signal(bar, inc=1, device_id=other, device_id_type=MESH_ID)
        pl.semaphore_wait(bar, 1)
        for t in range(T_STEPS):
            for k in range(len(pairs)):
                copy(k, t).start()

    @pl.when(step < T_STEPS)
    def _():
        for k in range(len(pairs)):
            copy(k, step).wait_recv()

    @pl.when(step == T_STEPS)
    def _():
        for t in range(T_STEPS):
            for k in range(len(pairs)):
                copy(k, t).wait_send()


def channels(step):
    return [(ch, step * CB + ch) for ch in range(CB)]


def mid_norm(x, xh_s, lnmid, blk, xn_s, rstd_s):
    tot = x[0]
    for c in range(1, C):
        tot = tot + x[c]
    mean = tot * (1.0 / C)
    d = x[0] - mean
    sq = d * d
    for c in range(1, C):
        d = x[c] - mean
        sq = sq + d * d
    rstd = lax.rsqrt(sq * (1.0 / C) + EPS)
    rstd_s[:] = rstd
    for c in range(C):
        xn = (x[c] - mean) * rstd
        xn_s[c] = xn
        xh_s[c] = (xn * lnmid[blk, 0, c] + lnmid[blk, 1, c]).astype(BF16)


def gate_of(zf, wt, gain, lbias):
    zn, _ = norm_rows(zf)
    zh = (zn * gain[:] + lbias[:]).astype(BF16)
    return jnp.tanh(dot_nn(wt[4 * C:5 * C], with_ones(zh)))


def project(zf, m, wt, gain, lbias):
    zn, _ = norm_rows(zf)
    zh = (zn * gain[:] + lbias[:]).astype(BF16)
    p = dot_nn(wt[0:4 * C], with_ones(zh))
    a = ((1.0 + jnp.tanh(p[0:C])) * (p[C:2 * C] * m)).astype(BF16)
    b = ((1.0 + jnp.tanh(p[2 * C:3 * C])) * (p[3 * C:4 * C] * m)).astype(BF16)
    return a, b


def fwd_kernel(ids, ap, ao, bp, bo, qp, qo, zp, zo, mp, mo, wt0, gain0, lbias0, wot0, wt1, gain1, lbias1, lnmid, perm, zmid, xn, rstd, a1, b1, a1k, a1s, x_s, full, xh_s, xi_s, a_s, b_s):
    step = pl.program_id(0)

    @pl.when(step < T_STEPS)
    def _():
        for ch, dst in channels(step):
            buf = full.at[ch % 2]
            place(buf, (bp[ch], bo[ch]), (qp[ch], qo[ch]), ids)
            x_s[dst] = dot_nt(jnp.concatenate([ap[ch], ao[ch]], axis=0), buf[:])

    def body(r, own):
        mid_norm(x_s.at[:, pl.ds(pl.multiple_of(r * RB, RB), RB), :], xh_s, lnmid, 0, xn, rstd)
        to_rows(perm[:], xh_s, xi_s)

        def update(i):
            zf = pick(own, zp, zo, i).astype(F32)
            upd = dot_nn(wot0[:], with_ones(xi_s[i]))
            zmid[i] = (zf + (1.0 + gate_of(zf, wt0, gain0, lbias0)) * upd).astype(BF16)

        def sides(i):
            m = pick(own, mp, mo, (pl.ds(i, 1), slice(None))).astype(F32)
            a_s[i], b_s[i] = project(zmid[i].astype(F32), m, wt1, gain1, lbias1)

        staggered(update, sides)

        def put_a(grp, v):
            a1[grp * RB:(grp + 1) * RB] = v.astype(BF16)
            mine, other = split_cols(v, ids[1])
            a1k[grp * RB:(grp + 1) * RB] = mine.astype(BF16)
            a1s[grp * RB:(grp + 1) * RB] = other.astype(BF16)

        def put_b(grp, v):
            b1[grp * RB:(grp + 1) * RB] = v.astype(BF16)

        to_cmajor(perm[:], a_s, put_a)
        to_cmajor(perm[:], b_s, put_b)

    each_half(step, body)


def weights_specs(par, blk, with_out):
    wt, wot, gain, lbias, _ = par
    specs = [blk_spec(wt.shape, blk), blk_spec(gain.shape, blk), blk_spec(gain.shape, blk)]
    args = [wt, gain, lbias]
    if with_out:
        specs.append(blk_spec(wot.shape, blk))
        args.append(wot)
    return specs, args


def fwd_fused(ids, sides, zp, zo, masks, par, lnmid):
    n = zp.shape[-1]
    s0, w0 = weights_specs(par, 0, True)
    s1, w1 = weights_specs(par, 1, False)
    sds, vm = jax.ShapeDtypeStruct, pltpu.VMEM
    c_out, h_out = sds((C, LANES, n), BF16), sds((C, LANES, LANES), BF16)
    return call(
        fwd_kernel, (T_STEPS + 8,),
        [SMEM_SPEC] + [tri_spec(v.shape) for v in sides] + two_specs((RB, C, n)) + two_specs((RB, n)) + s0 + s1 + [SMEM_SPEC, full_spec((W2, W2))],
        [r_spec(n), c_spec(n), m_spec(n), c_spec(n), c_spec(n), c_spec(LANES), c_spec(LANES)],
        [sds((LANES, C, n), BF16), sds((C, LANES, n), F32), sds((LANES, n), F32), c_out, c_out, h_out, h_out],
        [vm((C, LANES, n), F32), vm((2, n, n), BF16), vm((C, RB, n), BF16), vm((RB, C, n), BF16), vm((RB, C, n), BF16), vm((RB, C, n), BF16)],
        GIGA, 40 * MIB)(ids, *sides, zp, zo, *masks, *w0, *w1, lnmid, par[-1])


def mid_back(own, dxc_s, xn, rstd, lnmid, blk, acc_mg, acc_mb, emit):
    m1 = m2 = None
    for c in range(C):
        dy = dxc_s[c]
        dyx = dy * xn[c]
        gn = lnmid[blk, 0, c]
        m1 = dy * gn if m1 is None else m1 + dy * gn
        m2 = dyx * gn if m2 is None else m2 + dyx * gn
        if own:
            acc_mg[c] += fold(dyx[0:8] + dyx[8:RB])
            acc_mb[c] += fold(dy[0:8] + dy[8:RB])
    m1 = m1 * (1.0 / C)
    m2 = m2 * (1.0 / C)
    for c in range(C):
        emit(c, rstd * (dxc_s[c] * lnmid[blk, 0, c] - m1 - xn[c] * m2))


def clear(step, accs):
    @pl.when(step == 0)
    def _():
        for acc in accs:
            acc[:] = jnp.zeros_like(acc)


def turn_kernel(ak, b, a_send, b_send, z, dzp, dzo, wt, gain, lbias, wot, wo, lnmid, perm, znew, dx, dpg, acc_bg, acc_bo, acc_wo, acc_mg, acc_mb, x_s, xh_s, xi_s, dxi_s, dub_s, dxc_s, xn_s, r_s, ar_s, bq_s, send, recv):
    step = pl.program_id(0)
    xx, _ = here()
    from_partner(step, ((a_send, ar_s), (b_send, bq_s)), send, recv)
    clear(step, (acc_bg, acc_bo, acc_wo, acc_mg, acc_mb))

    @pl.when(step < T_STEPS)
    def _():
        for ch, dst in channels(step):
            out = dot_tn(ak[ch], b[ch]) + dot_tn(ar_s[dst], bq_s[dst])
            x_s[dst, pl.ds(pl.multiple_of(C * (1 - xx), C), C), :] = out[0:C]
            x_s[dst, pl.ds(pl.multiple_of(C * xx, C), C), :] = out[C:LANES]

    def body(r, own):
        mid_norm(x_s.at[:, pl.ds(pl.multiple_of(r * RB, RB), RB), :], xh_s, lnmid, 1, xn_s, r_s)
        to_rows(perm[:], xh_s, xi_s)
        sums = [acc_bg[:], acc_bo[:], acc_wo[:]]

        def gates(i):
            zf = z[i].astype(F32)
            dz = pick(own, dzp, dzo, i).astype(F32)
            t = gate_of(zf, wt, gain, lbias)
            upd = dot_nn(wot[:], with_ones(xi_s[i]))
            t1 = 1.0 + t
            if own:
                znew[i] = (zf + t1 * upd).astype(BF16)
            d_upd = (HALF * dz) * t1
            d_pg = d_upd * (upd * (1.0 - t))
            dpg[i] = d_pg.astype(BF16)
            dub_s[i] = d_upd.astype(BF16)
            if own:
                sums[0] += fold(d_pg)
                sums[1] += fold(d_upd)

        def products(i):
            dxi_s[i] = dot_nn(wo[:], dub_s[i]).astype(BF16)
            if own:
                sums[2] += dot_nt(dub_s[i], xi_s[i])

        staggered(gates, products)
        if own:
            acc_bg[:], acc_bo[:], acc_wo[:] = sums

        def put(grp, v):
            dxc_s[grp * RB:(grp + 1) * RB] = v

        to_cmajor(perm[:], dxi_s, put)

        def emit(c, v):
            dx[c] = v.astype(BF16)

        mid_back(own, dxc_s, xn_s, r_s[:], lnmid, 1, acc_mg, acc_mb, emit)

    each_half(step, body)


ACC_POST = ((C, LANES), (C, LANES), (C, C), (C, 8, LANES), (C, 8, LANES))
ACC_PRE = ((5 * C, C), (4 * C, LANES), (C, LANES), (C, LANES))


def turn_fused(sides, z_mid, dz_parts, par, w_out, lnmid):
    n = z_mid.shape[-1]
    s1, w1 = weights_specs(par, 1, True)
    sds, vm = jax.ShapeDtypeStruct, pltpu.VMEM
    return call(
        turn_kernel, (T_STEPS + 8,),
        [tri_spec(v.shape) for v in sides[:2]] + [pl.BlockSpec(memory_space=pl.ANY)] * 2 + [r_spec(n)] + two_specs((RB, C, n)) + s1 + [blk_spec(w_out.shape, 1), SMEM_SPEC, full_spec((W2, W2))],
        [two_specs((RB, C, n))[1], c_spec(n), r_spec(n)] + [full_spec(s) for s in ACC_POST],
        [sds((C, C, n), BF16), sds((C, LANES, n), BF16), sds((LANES, C, n), BF16)] + [sds(s, F32) for s in ACC_POST],
        [vm((C, LANES, n), F32), vm((C, RB, n), BF16)] + [vm((RB, C, n), BF16)] * 3 + [vm((C, RB, n), F32)] * 2 + [vm((RB, n), F32), vm((C, LANES, LANES), BF16), vm((C, LANES, n), BF16)] + [pltpu.SemaphoreType.DMA((2, T_STEPS))] * 2,
        GIGA, 40 * MIB, 1)(*sides, z_mid, *dz_parts, *w1, w_out, lnmid, par[-1])


def pre_back_stages(own, z, dpg, mask_of, res_of, dst, wt, w, gain, lbias, dai_s, dbi_s, dp_s, zh_s, zn_s, rs_s, acc_b, sums):
    def gates(i):
        zn, rstd = norm_rows(z[i].astype(F32))
        zn_s[i] = zn
        rs_s[i] = jnp.broadcast_to(rstd, (8, rstd.shape[-1]))
        zh = (zn * gain[:] + lbias[:]).astype(BF16)
        zh_s[i] = zh
        p = dot_nn(wt[0:4 * C], with_ones(zh))
        m = HALF * mask_of(i).astype(F32)
        for side, ref in ((0, dai_s), (1, dbi_s)):
            base = side * 2 * C
            dm = ref[i].astype(F32) * m
            t = jnp.tanh(p[base:base + C])
            dv = dm * (1.0 + t)
            dg = dv * (p[base + C:base + 2 * C] * (1.0 - t))
            for k, d in ((2 * side, dg), (2 * side + 1, dv)):
                if own:
                    acc_b[k * C:(k + 1) * C] += fold(d)
                dp_s[i, k * C:(k + 1) * C] = d.astype(BF16)
        dp_s[i, 4 * C:5 * C] = dpg[i]

    def products(i):
        dp = dp_s[i]
        dzh = dot_nn(w[:], dp).astype(BF16).astype(F32)
        zn, rstd = zn_s[i], rs_s[i, 0:1, :]
        if own:
            sums[0] += dot_nt(dp, zh_s[i])
            sums[1] += fold(dzh * zn)
            sums[2] += fold(dzh)
        dzn = dzh * gain[:]
        m1 = jnp.mean(dzn, axis=0, keepdims=True)
        m2 = jnp.mean(dzn * zn, axis=0, keepdims=True)
        dst[i] = (res_of(i).astype(F32) + rstd * (dzn - m1 - zn * m2)).astype(BF16)

    return gates, products


def back_kernel(a, b, dx, dx_send, z, dpg1, dzp, dzo, mp, mo, xn, rstd, zp, zo, wt1, gain1, lbias1, w1, wt0, gain0, lbias0, wot0, wo0, lnmid, perm, dzm, dx0, dxk, dxs, dpg0, acc_w, acc_b, acc_g, acc_lb, acc_bg, acc_bo, acc_wo, acc_mg, acc_mb, da_s, db_s, full, dai_s, dbi_s, dp_s, zh_s, zn_s, rs_s, xh_s, xi_s, dxi_s, dub_s, dxc_s, dxq_s, send, recv):
    step = pl.program_id(0)
    ids = here()
    from_partner(step, ((dx_send, dxq_s),), send, recv)
    clear(step, (acc_w, acc_b, acc_g, acc_lb, acc_bg, acc_bo, acc_wo, acc_mg, acc_mb))

    @pl.when(step < T_STEPS)
    def _():
        for ch, dst in channels(step):
            buf = full.at[ch % 2]
            place(buf, halves(dx.at[ch]), halves(dxq_s.at[dst]), ids)
            da_s[dst] = dot_nt(b[ch], buf[:]).astype(BF16)
            db_s[dst] = dot_nn(a[ch], buf[:]).astype(BF16)

    def body(r, own):
        rows = pl.ds(pl.multiple_of(r * RB, RB), RB)
        to_rows(perm[:], da_s.at[:, rows, :], dai_s)
        to_rows(perm[:], db_s.at[:, rows, :], dbi_s)
        for c in range(C):
            xh_s[c] = (xn[c] * lnmid[0, 0, c] + lnmid[0, 1, c]).astype(BF16)
        to_rows(perm[:], xh_s, xi_s)
        pre = [acc_w[:], acc_g[:], acc_lb[:]]
        pre_gates, pre_products = pre_back_stages(
            own, z, dpg1, lambda i: pick(own, mp, mo, (pl.ds(i, 1), slice(None))), lambda i: pick(own, dzp, dzo, i), dzm,
            wt1, w1, gain1, lbias1, dai_s, dbi_s, dp_s, zh_s, zn_s, rs_s, acc_b, pre)
        staggered(pre_gates, pre_products)
        if own:
            acc_w[:], acc_g[:], acc_lb[:] = pre
        post = [acc_bg[:], acc_bo[:], acc_wo[:]]

        def gates(i):
            t = gate_of(pick(own, zp, zo, i).astype(F32), wt0, gain0, lbias0)
            upd = dot_nn(wot0[:], with_ones(xi_s[i]))
            d_upd = (HALF * dzm[i].astype(F32)) * (1.0 + t)
            d_pg = d_upd * (upd * (1.0 - t))
            dpg0[i] = d_pg.astype(BF16)
            dub_s[i] = d_upd.astype(BF16)
            if own:
                post[0] += fold(d_pg)
                post[1] += fold(d_upd)

        def products(i):
            dxi_s[i] = dot_nn(wo0[:], dub_s[i]).astype(BF16)
            if own:
                post[2] += dot_nt(dub_s[i], xi_s[i])

        staggered(gates, products)
        if own:
            acc_bg[:], acc_bo[:], acc_wo[:] = post

        def put(grp, v):
            dxc_s[grp * RB:(grp + 1) * RB] = v

        to_cmajor(perm[:], dxi_s, put)

        def emit(c, v):
            dx0[c] = v.astype(BF16)
            mine, other = split_cols(v, ids[1])
            dxk[c] = mine.astype(BF16)
            dxs[c] = other.astype(BF16)

        mid_back(own, dxc_s, xn, rstd[:], lnmid, 0, acc_mg, acc_mb, emit)

    each_half(step, body)


def back_fused(sides, z_mid, dpg1, dz_parts, masks, xn, rstd, z_parts, par, w_proj, w_out, lnmid):
    n = z_mid.shape[-1]
    s1, w1 = weights_specs(par, 1, False)
    s0, w0 = weights_specs(par, 0, True)
    sds, vm = jax.ShapeDtypeStruct, pltpu.VMEM
    two = two_specs((RB, C, n))
    rows = vm((RB, C, n), BF16)
    accs = ACC_PRE + ACC_POST
    return call(
        back_kernel, (T_STEPS + 8,),
        [tri_spec(v.shape) for v in sides[:3]] + [pl.BlockSpec(memory_space=pl.ANY)] + [r_spec(n), r_spec(n)] + two + two_specs((RB, n)) + [c_spec(n), m_spec(n)] + two
        + s1 + [blk_spec(w_proj.shape, 1)] + s0 + [blk_spec(w_out.shape, 0), SMEM_SPEC, full_spec((W2, W2))],
        [two[1], c_spec(n), c_spec(LANES), c_spec(LANES), r_spec(n)] + [full_spec(s) for s in accs],
        [sds((C, C, n), BF16), sds((C, LANES, n), BF16), sds((C, LANES, LANES), BF16), sds((C, LANES, LANES), BF16), sds((LANES, C, n), BF16)] + [sds(s, F32) for s in accs],
        [vm((C, LANES, n), BF16)] * 2 + [vm((2, n, n), BF16), rows, rows, vm((RB, 5 * C, n), BF16), rows, vm((RB, C, n), F32), vm((RB, 8, n), F32), vm((C, RB, n), BF16), rows, rows, rows, vm((C, RB, n), F32), vm((C, LANES, n), BF16)] + [pltpu.SemaphoreType.DMA((1, T_STEPS))] * 2,
        GIGA, 60 * MIB, 2)(*sides, z_mid, dpg1, *dz_parts, *masks, xn, rstd, *z_parts, *w1, w_proj, *w0, w_out, lnmid, par[-1])


def last_kernel(ids, dx, bp, bo, qp, qo, dxk, dxr, ap, ao, rp, ro, z, dpg, dres, mask, wt, gain, lbias, w, perm, dz, acc_w, acc_b, acc_g, acc_lb, da_s, db_s, full, tmp, dai_s, dbi_s, dp_s, zh_s, zn_s, rs_s):
    step = pl.program_id(0)
    xx = ids[0]
    clear(step, (acc_w, acc_b, acc_g, acc_lb))

    @pl.when(step < T_STEPS)
    def _():
        for ch, dst in channels(step):
            buf = full.at[ch % 2]
            place(buf, (bp[ch], bo[ch]), (qp[ch], qo[ch]), ids)
            da_s[dst] = dot_nn(dx[ch], buf[:]).astype(BF16)
            tmp[ch % 2] = dot_tn(dxk[ch], jnp.concatenate([ap[ch], ao[ch]], axis=0)) + dot_tn(dxr[ch], jnp.concatenate([rp[ch], ro[ch]], axis=0))
            db_s[dst] = tmp[ch % 2, pl.ds(pl.multiple_of(C * xx, C), C), :].astype(BF16)

    @pl.when(step >= T_STEPS)
    def _():
        rows = pl.ds(pl.multiple_of((step - T_STEPS) * RB, RB), RB)
        to_rows(perm[:], da_s.at[:, rows, :], dai_s)
        to_rows(perm[:], db_s.at[:, rows, :], dbi_s)
        sums = [acc_w[:], acc_g[:], acc_lb[:]]
        staggered(*pre_back_stages(
            True, z, dpg, lambda i: mask[pl.ds(i, 1), :], lambda i: dres[i], dz,
            wt, w, gain, lbias, dai_s, dbi_s, dp_s, zh_s, zn_s, rs_s, acc_b, sums))
        acc_w[:], acc_g[:], acc_lb[:] = sums


def last_fused(ids, sides, z, dpg, dres, mask, par, w_proj):
    n = z.shape[-1]
    s0, w0 = weights_specs(par, 0, False)
    sds, vm = jax.ShapeDtypeStruct, pltpu.VMEM
    rows = vm((RB, C, n), BF16)
    return call(
        last_kernel, (T_STEPS + 4,),
        [SMEM_SPEC, tri_spec((C, C, n), 1)] + [tri_spec(v.shape) for v in sides[1:]] + [r_spec(n), r_spec(n, 4), r_spec(n), m_spec(n)] + s0 + [blk_spec(w_proj.shape, 0), full_spec((W2, W2))],
        [r_spec(n)] + [full_spec(s) for s in ACC_PRE],
        [sds((C, C, n), BF16)] + [sds(s, F32) for s in ACC_PRE],
        [vm((C, C, n), BF16)] * 2 + [vm((2, n, n), BF16), vm((2, LANES, n), F32), rows, rows, vm((RB, 5 * C, n), BF16), rows, vm((RB, C, n), F32), vm((RB, 8, n), F32)],
        GIGA, 40 * MIB)(ids, *sides, z, dpg, dres, mask, *w0, w_proj, par[-1])


PACK = 512


def grads_kernel(n_dp, n_dap, w0, b0, q0, g0, l0, wo0, o0, mg0, mb0, w1, b1, q1, g1, l1, wo1, o1, mg1, mb1, out, buf, recv_a, red, recv_b, gath, vec, send_a, rcv_a, send_b, rcv_b, send_c, rcv_c, send_d, rcv_d):
    dp, dap = lax.axis_index("dp"), lax.axis_index("dap")
    big, small = PACK // n_dap, PACK // n_dap // n_dp
    bar = pltpu.get_barrier_semaphore()
    for k in range(1, n_dap):
        pl.semaphore_signal(bar, inc=1, device_id=(dp, lax.rem(dap + k, n_dap)), device_id_type=MESH_ID)
    for k in range(1, n_dp):
        pl.semaphore_signal(bar, inc=1, device_id=(lax.rem(dp + k, n_dp), dap), device_id_type=MESH_ID)

    buf[0:5 * C, 0:C] = w0[:]
    buf[0:5 * C, C:2 * C] = w1[:]
    buf[5 * C:6 * C, 0:C] = wo0[:]
    buf[5 * C:6 * C, C:2 * C] = wo1[:]

    def put(k, base, ref):
        v = ref[:]
        if v.ndim == 3:
            v = jnp.sum(v, axis=1)
        rows = v.shape[0]
        tot = jnp.sum(v, axis=1, keepdims=True)
        lane = lax.broadcasted_iota(jnp.int32, (rows, LANES), 1)
        vec[base:base + rows, :] = jnp.where(lane == k, tot, vec[base:base + rows, :])

    vec[:] = jnp.zeros_like(vec)
    put(0, 0, b0)
    put(0, 4 * C, q0)
    put(1, 0, b1)
    put(1, 4 * C, q1)
    for k, ref in enumerate((g0, l0, g1, l1, mg0, mb0, mg1, mb1, o0, o1)):
        put(2 + k, 0, ref)
    vt = jnp.transpose(vec[:])
    for t in range(3):
        buf[6 * C + RB * t:6 * C + RB * t + RB, :] = vt[0:RB, LANES * t:LANES * (t + 1)]
    buf[6 * C + 48:PACK, :] = jnp.zeros((PACK - 6 * C - 48, LANES), F32)

    pl.semaphore_wait(bar, n_dap + n_dp - 2)

    def copies(count, make):
        made = [make(k) for k in range(1, count)]
        for cp in made:
            cp.start()
        return made

    def to_dap(k):
        return (dp, lax.rem(dap + k, n_dap))

    def to_dp(k):
        return (lax.rem(dp + k, n_dp), dap)

    def rows_of(idx, size):
        return pl.ds(pl.multiple_of(idx * size, size), size)

    stage = copies(n_dap, lambda k: pltpu.make_async_remote_copy(buf.at[rows_of(lax.rem(dap + k, n_dap), big)], recv_a.at[k - 1], send_a.at[k - 1], rcv_a.at[k - 1], device_id=to_dap(k), device_id_type=MESH_ID))
    tot = buf[rows_of(dap, big), :]
    for k, cp in enumerate(stage):
        cp.wait_recv()
        tot = tot + recv_a[k]
    red[:] = tot
    for cp in stage:
        cp.wait_send()

    stage = copies(n_dp, lambda k: pltpu.make_async_remote_copy(red.at[rows_of(lax.rem(dp + k, n_dp), small)], recv_b.at[k - 1], send_b.at[k - 1], rcv_b.at[k - 1], device_id=to_dp(k), device_id_type=MESH_ID))
    tot = red[rows_of(dp, small), :]
    for k, cp in enumerate(stage):
        cp.wait_recv()
        tot = tot + recv_b[k]
    gath[rows_of(dp, small), :] = tot
    for cp in stage:
        cp.wait_send()

    mine = gath.at[rows_of(dp, small)]
    stage = copies(n_dp, lambda k: pltpu.make_async_remote_copy(mine, mine, send_c.at[k - 1], rcv_c.at[k - 1], device_id=to_dp(k), device_id_type=MESH_ID))
    for cp in stage:
        cp.wait()

    stage = copies(n_dap, lambda k: pltpu.make_async_remote_copy(gath, out.at[rows_of(dap, big)], send_d.at[k - 1], rcv_d.at[k - 1], device_id=to_dap(k), device_id_type=MESH_ID))
    out[rows_of(dap, big), :] = gath[:]
    for cp in stage:
        cp.wait()


def sum_grads(n_dp, n_dap, parts):
    big, small = PACK // n_dap, PACK // n_dap // n_dp
    dma = pltpu.SemaphoreType.DMA
    return pl.pallas_call(
        functools.partial(grads_kernel, n_dp, n_dap),
        out_shape=jax.ShapeDtypeStruct((PACK, LANES), F32),
        in_specs=[pl.BlockSpec(memory_space=pltpu.VMEM)] * len(parts),
        out_specs=pl.BlockSpec(memory_space=pltpu.VMEM),
        scratch_shapes=[pltpu.VMEM((PACK, LANES), F32), pltpu.VMEM((n_dap - 1, big, LANES), F32), pltpu.VMEM((big, LANES), F32), pltpu.VMEM((max(n_dp - 1, 1), small, LANES), F32), pltpu.VMEM((big, LANES), F32), pltpu.VMEM((384, LANES), F32)]
        + [dma((n_dap - 1,))] * 2 + [dma((max(n_dp - 1, 1),))] * 4 + [dma((n_dap - 1,))] * 2,
        name="grad_sum",
        cost_estimate=pl.CostEstimate(flops=MEGA, bytes_accessed=MIB, transcendentals=0),
        compiler_params=pltpu.CompilerParams(collective_id=0, has_side_effects=True),
    )(*parts)


def unpack_kernel(src, ln_in, gw, bp, lm, gwo, bo):
    t = jnp.transpose(src[0:6 * C, :])
    for k in range(2):
        gw[k] = t[k * C:(k + 1) * C, 0:5 * C]
        gwo[k] = t[k * C:(k + 1) * C, 5 * C:6 * C]
    base = 6 * C
    bp[:, 0:LANES] = src[base:base + 2, :]
    bp[:, LANES:W2] = src[base + RB:base + 18, :]
    bp[:, W2:320] = src[base + 32:base + 34, 0:C]
    for k in range(2):
        ln_in[k] = src[base + 2 + 2 * k:base + 4 + 2 * k, 0:C]
        lm[k] = src[base + 6 + 2 * k:base + 8 + 2 * k, 0:C]
    bo[:] = src[base + 10:base + 12, 0:C]


def unpack(flat):
    outs = [jax.ShapeDtypeStruct(s, F32) for s in ((2, 2, C), (2, C, 5 * C), (2, 5 * C), (2, 2, C), (2, C, C), (2, C))]
    return call(unpack_kernel, (1,), [full_spec(flat.shape)], [full_spec(o.shape) for o in outs], outs, [], MEGA, MIB)(flat)


SUM = sum_grads


def solution(mesh):
    def plan(z_pair, pair_mask, dz_out, ln_in, w_proj, b_proj, ln_mid, w_out, b_out):
        n = z_pair.shape[2]
        dap = lax.axis_index("dap")
        ids = jnp.stack([dap // 2, dap % 2]).astype(jnp.int32)
        x_pairs = [(0, 2), (2, 0), (1, 3), (3, 1)]
        c_pairs = [(0, 1), (1, 0), (2, 3), (3, 2)]

        def over_x(v):
            return lax.ppermute(v, "dap", x_pairs)

        def over_c(v):
            return lax.ppermute(v, "dap", c_pairs)

        lnmid = ln_mid.astype(F32)
        par = prepare(n, ids, lnmid, ln_in, w_proj, b_proj, w_out, b_out)
        m_own = pair_mask[0]
        z_own = jnp.transpose(z_pair[0], (0, 2, 1))
        dz_own = jnp.transpose(dz_out[0], (0, 2, 1))
        m_peer = over_x(m_own)
        z_peer = over_x(z_own)
        z_peer, dz_src = lax.optimization_barrier((z_peer, dz_own))
        dz_peer = over_x(dz_src)
        masks = (m_peer, m_own)

        ao, bo = pre_forward(z_own, m_own, par)
        qo, ro = over_c(bo), over_c(ao)
        ap, bp = pre_forward(z_peer, m_peer, par)
        qp, rp = over_c(bp), over_c(ap)
        z_mid, xn, rstd, a1, b1, a1k, a1s = fwd_fused(ids, (ap, ao, bp, bo, qp, qo), z_peer, z_own, masks, par, lnmid)
        z_new, dx1, dpg1, bg1, bo1, wo1, mg1, mb1 = turn_fused((a1k, b1, a1s, b1), z_mid, (dz_peer, dz_own), par, w_out, lnmid)
        dz_mid, dx0, dx0k, dx0s, dpg0, w1, b1s, g1, lb1, bg0, bo0, wo0, mg0, mb0 = back_fused((a1, b1, dx1, dx1), z_mid, dpg1, (dz_peer, dz_own), masks, xn, rstd, (z_peer, z_own), par, w_proj, w_out, lnmid)
        dx0r = over_c(dx0s)
        dz, w0, b0s, g0, lb0 = last_fused(ids, (dx0, bp, bo, qp, qo, dx0k, dx0r, ap, ao, rp, ro), z_own, dpg0, dz_mid, m_own, par, w_proj)

        flat = SUM(mesh.shape["dp"], mesh.shape["dap"], (w0, b0s, bg0, g0, lb0, wo0, bo0, mg0, mb0, w1, b1s, bg1, g1, lb1, wo1, bo1, mg1, mb1))
        g_ln_in, gw, g_bp, g_lm, gwo, g_bo = unpack(flat)
        z_res = jnp.transpose(z_new, (0, 2, 1))[None]
        dz_res = jnp.transpose(dz, (0, 2, 1))[None]
        return z_res, dz_res, g_ln_in, gw, g_bp, g_lm, gwo, g_bo

    row_spec = P("dp", "dap")
    return jax.shard_map(plan, mesh=mesh, in_specs=(row_spec, row_spec, row_spec, P(), P(), P(), P(), P(), P()), out_specs=(row_spec, row_spec, P(), P(), P(), P(), P(), P()), check_vma=False)
```
